256 devices in a mesh: grp: 2 (over y), seq: 16 (over z), ch: 4 (over x), col: 2 (over core).
Axes of the slice: x: 4, y: 2, z: 16, core: 2. Of those that a mesh axis runs over, the one named last changes fastest.
The devices are a block of a 4x16x16 slice.
Arguments:
- latent: bfloat16 [32, 16, 16, 512], P('grp', 'seq', 'col', 'ch'), parts along dimension 0, may hold values from -8 to 8, as said below
- mid_gain: float32 [512], P('ch'), may hold values from 0.25 to 1.75
- mid_bias: float32 [512], P('ch'), may hold values from -3 to 3
- mid_weight: bfloat16 [3, 3, 3, 512, 512], P(None, None, None, None, 'ch'), may hold values from -0.0546875 to 0.0546875
- mid_conv_bias: float32 [512], P('ch'), may hold values from -2 to 2
- first_gain: float32 [512], P('ch'), may hold values from 0.25 to 1.75
- first_bias: float32 [512], P('ch'), may hold values from -3 to 3
- first_weight: bfloat16 [3, 3, 3, 512, 512], P(None, None, None, None, 'ch'), may hold values from -0.0546875 to 0.0546875
- first_conv_bias: float32 [512], P('ch'), may hold values from -2 to 2
- second_gain: float32 [512], P('ch'), may hold values from 0.25 to 1.75
- second_bias: float32 [512], P('ch'), may hold values from -3 to 3
- second_weight: bfloat16 [3, 3, 3, 512, 512], P(None, None, None, None, 'ch'), may hold values from -0.0546875 to 0.0546875
- second_conv_bias: float32 [512], P('ch'), may hold values from -2 to 2
Outputs:
- decoded: bfloat16 [64, 16, 16, 512], P(('grp', 'seq'), None, 'col', 'ch'), parts along dimension 0
The draws below stay inside these ranges and needn't reach their ends.
There are 2 independent parts, one for each index of `grp`. The reference program is written for one: setup_inputs(seed, part) draws one part's arguments, and reference() takes and returns one part's arrays. A program takes and returns all parts, laid end to end along the dimension named above; an argument that names none is the same for every part. Nothing has to cross between parts.
Inputs may be any that keep to these rules, and one draw needn't show every extreme that they name: `latent`: each row has its own scale and each row and channel its own offset; values are clipped to the range.
All inputs are finite; a program needn't handle non-finite values.
Results may differ from the reference program's by a relative error of at most 0.0095.
Values may be sent and summed in bfloat16 or wider, within the bound.
A program may use at most 64 MiB of HBM per device.

```python
import jax
import jax.numpy as jnp
from jax import lax

C = 512
GROUPS = 32
FRAMES = 16
HEIGHT = 16
WIDTH = 16


def draw_latent(key, part):
    first_key, second_key, third_key = jax.random.split(jax.random.fold_in(key, 17), 3)
    gauss_noise = jax.random.normal(first_key, (FRAMES, HEIGHT, WIDTH, C), jnp.float32)
    row_scale = jnp.exp(jax.random.uniform(second_key, (1, HEIGHT, 1, 1), jnp.float32, -0.7, 0.7))
    offset = 0.5 * jax.random.normal(third_key, (1, HEIGHT, 1, C), jnp.float32)
    return jnp.clip(gauss_noise * row_scale + offset, -8.0, 8.0).astype(jnp.bfloat16)


def block_scale(key, extent, shards, least, largest):
    level, own = 1.0, jax.random.fold_in(key, 6)
    for dim, blocks in shards:
        steps = jnp.exp(jax.random.uniform(jax.random.fold_in(own, dim), (blocks,), jnp.float32, least / len(shards), largest / len(shards)))
        level = level * jnp.repeat(steps, extent[dim] // blocks).reshape([-1 if axis == dim else 1 for axis in range(len(extent))])
    return level


def noise(rng, dims, scale, limit, cuts=(), kind=jnp.bfloat16):
    level = block_scale(rng, dims, cuts, -0.22, 0.18) if cuts else 1.0
    drawn = jax.random.normal(rng, dims, jnp.float32) * scale * level
    return jnp.minimum(jnp.maximum(drawn, -limit), limit).astype(kind)


def setup_inputs(seed: int = 0, part: int = 0) -> dict:
    seeds = jax.random.split(jax.random.key(seed), 14)
    own_keys = jax.random.split(jax.random.fold_in(seeds[13], part), 14)
    return {
        "latent": draw_latent(jax.random.fold_in(jax.random.fold_in(seeds[13], part), 71), part),
        "mid_gain": jnp.clip(1.0 + 0.15 * jax.random.normal(seeds[1], (C,), jnp.float32), 0.25, 1.75),
        "mid_bias": noise(seeds[2], (C,), 0.5, 3.0, ((0, 4),), jnp.float32),
        "mid_weight": noise(seeds[3], (3, 3, 3, C, C), (27 * C) ** -0.5, 0.0546875, ((4, 4),)),
        "mid_conv_bias": noise(seeds[4], (C,), 0.3, 2.0, ((0, 4),), jnp.float32),
        "first_gain": jnp.clip(1.0 + 0.15 * jax.random.normal(seeds[5], (C,), jnp.float32), 0.25, 1.75),
        "first_bias": noise(seeds[6], (C,), 0.5, 3.0, ((0, 4),), jnp.float32),
        "first_weight": noise(seeds[7], (3, 3, 3, C, C), (27 * C) ** -0.5, 0.0546875, ((4, 4),)),
        "first_conv_bias": noise(seeds[8], (C,), 0.3, 2.0, ((0, 4),), jnp.float32),
        "second_gain": jnp.clip(1.0 + 0.15 * jax.random.normal(seeds[9], (C,), jnp.float32), 0.25, 1.75),
        "second_bias": noise(seeds[10], (C,), 0.5, 3.0, ((0, 4),), jnp.float32),
        "second_weight": noise(seeds[11], (3, 3, 3, C, C), (27 * C) ** -0.5, 0.0546875, ((4, 4),)),
        "second_conv_bias": noise(seeds[12], (C,), 0.3, 2.0, ((0, 4),), jnp.float32),
    }


def group_norm(field, gain, shift_term):
    values = field.astype(jnp.float32)
    group_size = C // GROUPS
    totals = lax.optimization_barrier(jnp.sum(values, axis=(0, 1, 2))).reshape(GROUPS, group_size).sum(axis=1)
    squares = lax.optimization_barrier(jnp.sum(values * values, axis=(0, 1, 2))).reshape(GROUPS, group_size).sum(axis=1)
    samples = values.shape[0] * values.shape[1] * values.shape[2] * group_size
    group_mean = totals / samples
    spread = squares / samples - group_mean * group_mean
    inverse = 1.0 / jnp.sqrt(spread + 0.01)
    scaled = (values - jnp.repeat(group_mean, group_size)) * jnp.repeat(inverse, group_size) * gain + shift_term
    return jax.nn.silu(scaled).astype(jnp.bfloat16)

def convolve(field, weight):
    result = lax.conv_general_dilated(field[None].astype(jnp.float32), weight.astype(jnp.float32), (1, 1, 1), ((2, 0), (1, 1), (1, 1)), dimension_numbers=('NDHWC', 'DHWIO', 'NDHWC'), precision=lax.Precision.HIGHEST)
    return result[0]

def reference(latent, mid_gain, mid_bias, mid_weight, mid_conv_bias, first_gain, first_bias, first_weight, first_conv_bias, second_gain, second_bias, second_weight, second_conv_bias):
    mid_act = group_norm(latent, mid_gain, mid_bias)
    middle = (latent.astype(jnp.float32) + convolve(mid_act, mid_weight) + mid_conv_bias).astype(jnp.bfloat16)
    doubled = jnp.repeat(middle, 2, axis=0)
    first_act = group_norm(doubled, first_gain, first_bias)
    hidden = (convolve(first_act, first_weight) + first_conv_bias).astype(jnp.bfloat16)
    second_act = group_norm(hidden, second_gain, second_bias)
    return (doubled.astype(jnp.float32) + convolve(second_act, second_weight) + second_conv_bias).astype(jnp.bfloat16)
```

```python
import functools

import jax
import jax.numpy as jnp
from jax import lax
from jax.experimental import pallas as pl
from jax.experimental.pallas import tpu as pltpu
from jax.sharding import PartitionSpec as P

MESH = pl.DeviceIdType.MESH
GROUP = 16
LANES = 128
EPS = 0.01
BF = jnp.bfloat16
F32 = jnp.float32


def lane_ids():
    return lax.broadcasted_iota(jnp.int32, (8, LANES), 1)


def row_ids():
    return lax.broadcasted_iota(jnp.int32, (8, LANES), 0)


def group_total(v):
    lane = lane_ids()
    step = GROUP // 2
    while step:
        from_below = pltpu.roll(v, step, 1)
        from_above = pltpu.roll(v, LANES - step, 1)
        v = v + jnp.where((lane & step) != 0, from_below, from_above)
        step //= 2
    return v


def packed_sums(values, x):
    total = jnp.sum(values, axis=0, keepdims=True)
    square = jnp.sum(values * values, axis=0, keepdims=True)
    total = group_total(jnp.broadcast_to(total, (8, LANES)))
    square = group_total(jnp.broadcast_to(square, (8, LANES)))
    slot = lane_ids() & 7
    row = jnp.where(slot == 2 * x, total, jnp.where(slot == 2 * x + 1, square, 0.0))
    return row[0:1]


def affine(row, samples, params, which, nx):
    spread_rows = jnp.broadcast_to(row, (8, LANES))
    picked = jnp.where((lane_ids() & (GROUP - 1)) == row_ids(), spread_rows, 0.0)
    sums = group_total(picked) * (1.0 / samples)
    out = []
    for block in range(nx):
        mean = sums[2 * block : 2 * block + 1]
        square = sums[2 * block + 1 : 2 * block + 2]
        inverse = 1.0 / jnp.sqrt(square - mean * mean + EPS)
        gain = params[block, 2 * which : 2 * which + 1]
        bias = params[block, 2 * which + 1 : 2 * which + 2]
        scale = inverse * gain
        out.append((scale, bias - mean * scale))
    return out


def activate(values, scale, shift):
    u = values * scale.reshape((1,) * (values.ndim - 1) + (LANES,)) + shift.reshape(
        (1,) * (values.ndim - 1) + (LANES,)
    )
    half = 0.5 * u
    return (half + half * jnp.tanh(half)).astype(BF)


def column_sum(y):
    n, cols = y.shape[0], y.shape[1]
    left, mid, right = (y[:, :, i * LANES : (i + 1) * LANES] for i in range(3))
    col = lax.broadcasted_iota(jnp.int32, (n, cols, LANES), 1)
    left = jnp.where(col == 0, 0.0, pltpu.roll(left, 1, 1))
    right = jnp.where(col == cols - 1, 0.0, pltpu.roll(right, cols - 1, 1))
    return left + mid + right


def taps(weight, dt, di):
    base = dt * 9 + di * 3
    return jnp.concatenate([weight[base + dj] for dj in range(3)], axis=1)


def dot(a, b):
    return jnp.dot(a, b, preferred_element_type=F32)


def flat(v):
    return v.reshape(-1, v.shape[-1])


def kernel(
    nz,
    nx,
    lat,
    g0,
    b0,
    w0_hbm,
    c0,
    g1,
    b1,
    w1_hbm,
    c1,
    g2,
    b2,
    w2_hbm,
    c2,
    out,
    w0,
    w1,
    w2,
    params,
    r0,
    x1,
    x2,
    act0,
    act1,
    act2,
    middle,
    hidden,
    give,
    take,
    plane_src,
    plane_in,
    line_src,
    line_in,
    w_sem,
    par_s,
    par_r,
    plane_s,
    plane_r,
    line_s,
    line_r,
    x0_s,
    x0_r,
    z0_s,
    z0_r,
    a_s,
    a_r,
    x1_s,
    x1_r,
    x2_s,
    x2_r,
    e2_s,
    e2_r,
    o_s,
    o_r,
):
    z = lax.axis_index("seq")
    x = lax.axis_index("ch")
    c = lax.axis_index("col")
    half = nz // 2
    samples = float(nz * nz * 16 * GROUP)

    def peer(dz, dx, col):
        return {"seq": lax.rem(z + dz + nz, nz), "ch": lax.rem(x + dx, nx), "col": col}

    def remote(src, dst, s_sem, r_sem, to):
        return pltpu.make_async_remote_copy(
            src_ref=src,
            dst_ref=dst,
            send_sem=s_sem,
            recv_sem=r_sem,
            device_id=to,
            device_id_type=MESH,
        )

    def landed(ref, sem):
        pltpu.make_async_copy(ref, ref, sem).wait()

    loads = [
        pltpu.make_async_copy(a, b, w_sem.at[i])
        for i, (a, b) in enumerate(((w0_hbm, w0), (w1_hbm, w1), (w2_hbm, w2)))
    ]
    for load in loads:
        load.start()

    barrier = pltpu.get_barrier_semaphore()
    greeted = []
    for dz in range(nz):
        greeted.append((dz, 0, 1 - c))
        if dz:
            greeted.append((dz, 0, c))
    for dz in (0, 1, nz - 1):
        for dx in range(1, nx):
            greeted.append((dz, dx, c))
            greeted.append((dz, dx, 1 - c))
    greeted.sort(key=lambda g: -min(g[0], nz - g[0]))
    for dz, dx, col in greeted:
        pl.semaphore_signal(barrier, inc=1, device_id=peer(dz, dx, col), device_id_type=MESH)

    mine = pl.multiple_of(x * 8, 8)
    for i, ref in enumerate((g0, b0, g1, b1, g2, b2)):
        params[x, i : i + 1, :] = ref[...]
    own = lat[...].astype(F32)
    plane_src[0] = packed_sums(flat(own), x)
    own_at = ((nx + x) * 2 + c) * 6
    r0[pl.ds(own_at + 1 - c, 5)] = lat[pl.ds(3 * c, 5)]

    pl.semaphore_wait(barrier, len(greeted))

    def plane_start(stage):
        place = 8 * stage + 2 * x + c
        plane_in[place] = plane_src[stage]
        for dx in range(nx):
            for other in (0, 1):
                if dx == 0 and other == 0:
                    continue
                remote(
                    plane_src.at[stage],
                    plane_in.at[place],
                    plane_s.at[stage],
                    plane_r.at[stage],
                    peer(0, dx, c if other == 0 else 1 - c),
                ).start()

    def line_start(stage):
        landed(plane_in.at[pl.ds(8 * stage, 2 * nx - 1)], plane_r.at[stage])
        row = jnp.sum(plane_in[8 * stage : 8 * stage + 2 * nx], axis=0)
        line_src[stage] = row
        line_in[stage * nz + z] = row
        order = sorted(range(1, nz), key=lambda dz: -min(dz, nz - dz))
        for dz in order:
            remote(
                line_src.at[stage],
                line_in.at[stage * nz + z],
                line_s.at[stage],
                line_r.at[stage],
                peer(dz, 0, c),
            ).start()

    def line_total(stage):
        landed(line_in.at[pl.ds(stage * nz, nz - 1)], line_r.at[stage])
        return jnp.sum(line_in[stage * nz : (stage + 1) * nz], axis=0)

    plane_start(0)
    for dx in range(1, nx):
        remote(params.at[x], params.at[x], par_s, par_r, peer(0, dx, c)).start()

    for dx in (2, 1, 3, 0):
        for other in (0, 1):
            if dx == 0 and other == 0:
                continue
            to_col = c if other == 0 else 1 - c
            remote(
                lat.at[pl.ds(3 * to_col, 5)],
                r0.at[pl.ds(own_at + 1 - to_col, 5)],
                x0_s,
                x0_r.at[x * 2 + c],
                peer(0, dx, to_col),
            ).start()

    line_start(0)

    for dx in (0, 1, 3, 2):
        for other in (0, 1):
            from_x = lax.rem(x + dx, nx)
            from_c = c if other == 0 else 1 - c
            at = (from_x * 2 + from_c) * 6
            if not (dx == 0 and other == 0):
                landed(r0.at[pl.ds(nx * 12 + at + 1 - c, 5)], x0_r.at[from_x * 2 + from_c])
            for row, dz in ((0, 1), (2, nz - 1)):
                remote(
                    r0.at[pl.ds(nx * 12 + at, 5)],
                    r0.at[pl.ds(row * nx * 12 + at, 5)],
                    z0_s,
                    z0_r.at[(row // 2) * 8 + from_x * 2 + from_c],
                    peer(dz, 0, c),
                ).start()

    landed(params.at[pl.ds(0, nx - 1)], par_r)
    norm = affine(line_total(0), samples, params, 0, nx)

    def frames_of(row, block):
        at = (row * nx + block) * 12
        parts = []
        for col in range(2):
            v = r0[pl.ds(at + 6 * col, 5)].astype(F32)
            parts.append(v.reshape(10, 8, LANES))
        return jnp.concatenate(parts, axis=1)

    for row in (1, 0, 2):
        for block in range(nx):
            if row != 1:
                for col in range(2):
                    at = (row * nx + block) * 12 + 6 * col
                    landed(r0.at[pl.ds(at, 5)], z0_r.at[(row // 2) * 8 + block * 2 + col])
            scale, shift = norm[block]
            act0[row, :, :, block * LANES : (block + 1) * LANES] = activate(
                frames_of(row, block), scale, shift
            )

    @pl.when(z == 0)
    def _():
        act0[0] = jnp.zeros(act0.shape[1:], BF)

    @pl.when(z == nz - 1)
    def _():
        act0[2] = jnp.zeros(act0.shape[1:], BF)

    @pl.when(c == 0)
    def _():
        act0[:, 0:2] = jnp.zeros((3, 2, *act0.shape[2:]), BF)

    loads[0].wait()
    y = jnp.zeros((half * 16, 3 * LANES), F32)
    for dt in range(3):
        for di in range(3):
            y = y + dot(flat(act0[di, dt : dt + half]), taps(w0, dt, di))
    mixed = column_sum(y.reshape(half, 16, 3 * LANES))
    rest = frames_of(1, x)[2:10]
    value = (rest + mixed + c0[...].reshape(1, 1, LANES)).astype(BF)
    middle[...] = value
    plane_src[1] = packed_sums(flat(value.astype(F32)), x)
    plane_start(1)

    def spread(act):
        for j in range(half):
            for later in range(2):
                to_z = lax.rem(half * c + j + later, nz)
                fr = 1 - later
                for case in range(2):
                    if case == 0:
                        to_c = z // half
                        wanted = to_z >= 0
                    else:
                        to_c = 1 - z // half
                        wanted = (z == half - 1) | (z == half)
                    slot = z - half * to_c + 1
                    itself = (to_z == z) & (to_c == c)
                    act(j, fr, case, to_z, to_c, slot, wanted, itself)

    def a_copy(j, fr, case, to_z, to_c, slot):
        return remote(
            middle.at[j],
            x1.at[(x * 10 + slot) * 2 + fr],
            a_s.at[(j * 2 + fr) * 2 + case],
            a_r.at[slot * 2 + fr],
            {"seq": to_z, "ch": x, "col": to_c},
        )

    def a_start(j, fr, case, to_z, to_c, slot, wanted, itself):
        @pl.when(wanted & jnp.logical_not(itself))
        def _():
            a_copy(j, fr, case, to_z, to_c, slot).start()

        @pl.when(wanted & itself)
        def _():
            x1[(x * 10 + slot) * 2 + fr] = middle[j]

    def a_sent(j, fr, case, to_z, to_c, slot, wanted, itself):
        @pl.when(wanted & jnp.logical_not(itself))
        def _():
            a_copy(j, fr, case, to_z, to_c, slot).wait_send()

    spread(a_start)
    line_start(1)

    first = 1 - c
    for part in range(3):
        for i in range(3):
            slot = first + part * 3 + i
            source_row = half * c - 1 + slot
            for fr in range(2):
                source_c = lax.rem(z - 1 + fr + nz, nz) // half

                @pl.when(jnp.logical_not((source_row == z) & (source_c == c)))
                def _():
                    landed(x1.at[(x * 10 + slot) * 2 + fr], a_r.at[slot * 2 + fr])

        tiles = pl.ds((x * 10 + first + part * 3) * 2, 6)
        for dx in (2, 1, 3):
            remote(
                x1.at[tiles], x1.at[tiles], x1_s, x1_r.at[x * 3 + part], peer(0, dx, c)
            ).start()

    norm = affine(line_total(1), samples, params, 1, nx)
    for block in range(nx):
        @pl.when(block != x)
        def _():
            for part in range(3):
                landed(
                    x1.at[pl.ds((block * 10 + first + part * 3) * 2, 6)],
                    x1_r.at[block * 3 + part],
                )

        scale, shift = norm[block]
        v = x1[block * 20 : (block + 1) * 20].astype(F32).reshape(10, 2, 16, LANES)
        v = activate(v, scale, shift)
        for fr in range(2):
            act1[fr, :, :, block * LANES : (block + 1) * LANES] = v[:, fr]

    zero_row1 = jnp.zeros((2, 16, nx * LANES), BF)

    @pl.when(c == 0)
    def _():
        act1[:, 0] = zero_row1

    @pl.when(c == 1)
    def _():
        act1[:, 9] = zero_row1

    @pl.when(z == 0)
    def _():
        act1[0] = jnp.zeros(act1.shape[1:], BF)

    loads[1].wait()
    shared = jnp.zeros((half * 16, 3 * LANES), F32)
    apart = jnp.zeros((2 * half * 16, 3 * LANES), F32)
    for di in range(3):
        rows = act1[:, di : di + half]
        shared = shared + dot(flat(rows[0]), taps(w1, 0, di))
        shared = shared + dot(flat(rows[1]), taps(w1, 2, di))
    for di in range(3):
        apart = apart + dot(flat(act1[:, di : di + half]), taps(w1, 1, di))
    y = apart.reshape(2, half, 16, 3 * LANES) + shared.reshape(1, half, 16, 3 * LANES)
    mixed = column_sum(y.reshape(2 * half, 16, 3 * LANES))
    value = (mixed + c1[...].reshape(1, 1, LANES)).astype(BF)
    plane_src[2] = packed_sums(flat(value.astype(F32)), x)
    value = value.reshape(2, half, 16, LANES)
    for fr in range(2):
        for row in range(half):
            hidden[row * 2 + fr] = value[fr, row]
    plane_start(2)

    x2[pl.ds((x * 2 + 1) * 20 + 2, 2 * half)] = hidden[...]
    edge_at = pl.ds((2 * half - 2) * (1 - c), 2)
    edge_slot = pl.ds(18 * c, 2)
    for dz in (1, 0):
        for dx in (2, 1, 3, 0):
            if not (dz == 0 and dx == 0):
                remote(
                    hidden,
                    x2.at[pl.ds((x * 2 + 1 - dz) * 20 + 2, 2 * half)],
                    x2_s,
                    x2_r.at[(1 - dz) * nx + x],
                    peer(dz, dx, c),
                ).start()
            slot = pl.ds((x * 2 + 1 - dz) * 20 + 18 * c, 2)
            remote(
                hidden.at[edge_at], x2.at[slot], e2_s, e2_r.at[(1 - dz) * nx + x], peer(dz, dx, 1 - c)
            ).start()
    line_start(2)
    norm = affine(line_total(2), 2.0 * samples, params, 2, nx)

    for block in range(nx):
        for own_frames in (1, 0):
            sem = own_frames * nx + block
            at = (block * 2 + own_frames) * 20
            if own_frames:
                @pl.when(block != x)
                def _():
                    landed(x2.at[pl.ds(at + 2, 2 * half)], x2_r.at[sem])
            else:
                landed(x2.at[pl.ds(at + 2, 2 * half)], x2_r.at[sem])
            landed(x2.at[pl.ds(at + 18 * (1 - c), 2)], e2_r.at[sem])
            scale, shift = norm[block]
            v = x2[at : at + 20].astype(F32).reshape(10, 2, 16, LANES)
            v = activate(v, scale, shift)
            for fr in range(2):
                act2[2 * own_frames + fr, :, :, block * LANES : (block + 1) * LANES] = v[:, fr]

    zero_row2 = jnp.zeros((4, 16, nx * LANES), BF)

    @pl.when(c == 0)
    def _():
        act2[:, 0] = zero_row2

    @pl.when(c == 1)
    def _():
        act2[:, 9] = zero_row2

    @pl.when(z == 0)
    def _():
        act2[0:2] = jnp.zeros((2, *act2.shape[1:]), BF)

    loads[2].wait()
    y = jnp.zeros((2 * half * 16, 3 * LANES), F32)
    for dt in range(3):
        for di in range(3):
            y = y + dot(flat(act2[dt : dt + 2, di : di + half]), taps(w2, dt, di))
    mixed = column_sum(y.reshape(2 * half, 16, 3 * LANES)).reshape(2, half, 16, LANES)
    doubled = x1[pl.ds(x * 20 + 2, 2 * half)].astype(F32).reshape(half, 2, 16, LANES)[:, 1]
    final = doubled[None] + mixed + c2[...].reshape(1, 1, 1, LANES)

    sides = [
        final[:, :, 8 * side : 8 * side + 8].reshape(2, half // 2, 16, LANES).astype(BF)
        for side in range(2)
    ]

    @pl.when(c == 0)
    def _():
        give[...] = sides[1]
        out[:, pl.ds(0, half // 2)] = sides[0]

    @pl.when(c == 1)
    def _():
        give[...] = sides[0]
        out[:, pl.ds(half // 2, half // 2)] = sides[1]

    last = remote(give, take, o_s, o_r, peer(0, 0, 1 - c))
    last.start()

    for stage in range(3):
        landed(plane_in.at[pl.ds(8 * stage, 2 * nx - 1)], plane_s.at[stage])
        landed(line_in.at[pl.ds(stage * nz, nz - 1)], line_s.at[stage])
    landed(params.at[pl.ds(0, nx - 1)], par_s)
    landed(r0.at[pl.ds(0, 5 * (2 * nx - 1))], x0_s)
    landed(r0.at[pl.ds(0, 5 * 4 * nx)], z0_s)
    spread(a_sent)
    landed(x1.at[pl.ds(0, 3 * 3 * 6)], x1_s)
    landed(x2.at[pl.ds(0, 2 * half * (2 * nx - 1))], x2_s)
    landed(x2.at[pl.ds(0, 2 * 2 * nx)], e2_s)
    last.wait()

    @pl.when(c == 0)
    def _():
        out[:, pl.ds(half // 2, half // 2)] = take[...]

    @pl.when(c == 1)
    def _():
        out[:, pl.ds(0, half // 2)] = take[...]


def body(nz, nx, *args):
    latent = args[0]
    frames = latent.shape[0]
    half = nz // 2
    channels = nx * LANES
    operands = [latent.reshape(frames // 2, 16, LANES)]
    vmem = pl.BlockSpec(memory_space=pltpu.VMEM)
    specs = [vmem]
    for a in args[1:]:
        if a.ndim == 1:
            operands.append(a.reshape(1, LANES))
            specs.append(vmem)
        else:
            operands.append(a.reshape(27, channels, LANES))
            specs.append(pl.BlockSpec(memory_space=pl.ANY))
    weight = pltpu.VMEM((27, channels, LANES), BF)
    dma = pltpu.SemaphoreType.DMA
    result = pl.pallas_call(
        functools.partial(kernel, nz, nx),
        out_shape=jax.ShapeDtypeStruct((2, half, 16, LANES), BF),
        in_specs=specs,
        out_specs=vmem,
        scratch_shapes=[
            weight,
            weight,
            weight,
            pltpu.VMEM((nx, 8, LANES), F32),
            pltpu.VMEM((3 * nx * 2 * 6, 16, LANES), BF),
            pltpu.VMEM((nx * 10 * 2, 16, LANES), BF),
            pltpu.VMEM((nx * 2 * 10 * 2, 16, LANES), BF),
            pltpu.VMEM((3, half + 2, 16, channels), BF),
            pltpu.VMEM((2, half + 2, 16, channels), BF),
            pltpu.VMEM((4, half + 2, 16, channels), BF),
            pltpu.VMEM((half, 16, LANES), BF),
            pltpu.VMEM((2 * half, 16, LANES), BF),
            pltpu.VMEM((2, half // 2, 16, LANES), BF),
            pltpu.VMEM((2, half // 2, 16, LANES), BF),
            pltpu.VMEM((3, 1, LANES), F32),
            pltpu.VMEM((3 * 8, 1, LANES), F32),
            pltpu.VMEM((3, 1, LANES), F32),
            pltpu.VMEM((3 * nz, 1, LANES), F32),
            dma((3,)),
            dma,
            dma,
            dma((3,)),
            dma((3,)),
            dma((3,)),
            dma((3,)),
            dma,
            dma((2 * nx,)),
            dma,
            dma((4 * nx,)),
            dma((half * 4,)),
            dma((20,)),
            dma,
            dma((3 * nx,)),
            dma,
            dma((2 * nx,)),
            dma,
            dma((2 * nx,)),
            dma,
            dma,
        ],
        compiler_params=pltpu.CompilerParams(collective_id=0, has_side_effects=True),
    )(*operands)
    return result.reshape(2, nz, 8, LANES)


def solution(mesh):
    nz, nx = mesh.shape["seq"], mesh.shape["ch"]
    in_specs = (
        P("grp", "seq", "col", "ch"),
        *(P("ch"), P("ch"), P(None, None, None, None, "ch"), P("ch")) * 3,
    )
    out_specs = P(("grp", "seq"), None, "col", "ch")
    return jax.shard_map(
        functools.partial(body, nz, nx),
        mesh=mesh,
        in_specs=in_specs,
        out_specs=out_specs,
        check_vma=False,
    )
```

```python
import functools

import jax
import jax.numpy as jnp
from jax import lax
from jax.experimental import pallas as pl
from jax.experimental.pallas import tpu as pltpu
from jax.sharding import PartitionSpec as P

MESH = pl.DeviceIdType.MESH
GROUP = 16
LANES = 128
EPS = 0.01
BF = jnp.bfloat16
F32 = jnp.float32


def lane_ids():
    return lax.broadcasted_iota(jnp.int32, (8, LANES), 1)


def row_ids():
    return lax.broadcasted_iota(jnp.int32, (8, LANES), 0)


def group_total(v):
    lane = lane_ids()
    step = GROUP // 2
    while step:
        from_below = pltpu.roll(v, step, 1)
        from_above = pltpu.roll(v, LANES - step, 1)
        v = v + jnp.where((lane & step) != 0, from_below, from_above)
        step //= 2
    return v


def packed_sums(values, x):
    total = jnp.sum(values, axis=0, keepdims=True)
    square = jnp.sum(values * values, axis=0, keepdims=True)
    total = group_total(jnp.broadcast_to(total, (8, LANES)))
    square = group_total(jnp.broadcast_to(square, (8, LANES)))
    slot = lane_ids() & 7
    row = jnp.where(slot == 2 * x, total, jnp.where(slot == 2 * x + 1, square, 0.0))
    return row[0:1]


def affine(row, samples, params, which, nx):
    spread_rows = jnp.broadcast_to(row, (8, LANES))
    picked = jnp.where((lane_ids() & (GROUP - 1)) == row_ids(), spread_rows, 0.0)
    sums = group_total(picked) * (1.0 / samples)
    out = []
    for block in range(nx):
        mean = sums[2 * block : 2 * block + 1]
        square = sums[2 * block + 1 : 2 * block + 2]
        inverse = 1.0 / jnp.sqrt(square - mean * mean + EPS)
        gain = params[block, 2 * which : 2 * which + 1]
        bias = params[block, 2 * which + 1 : 2 * which + 2]
        scale = inverse * gain
        out.append((scale, bias - mean * scale))
    return out


def activate(values, scale, shift):
    u = values * scale.reshape((1,) * (values.ndim - 1) + (LANES,)) + shift.reshape(
        (1,) * (values.ndim - 1) + (LANES,)
    )
    half = 0.5 * u
    return (half + half * jnp.tanh(half)).astype(BF)


def column_sum(y):
    n, cols = y.shape[0], y.shape[1]
    left, mid, right = (y[:, :, i * LANES : (i + 1) * LANES] for i in range(3))
    col = lax.broadcasted_iota(jnp.int32, (n, cols, LANES), 1)
    left = jnp.where(col == 0, 0.0, pltpu.roll(left, 1, 1))
    right = jnp.where(col == cols - 1, 0.0, pltpu.roll(right, cols - 1, 1))
    return left + mid + right


def taps(weight, dt, di):
    base = dt * 9 + di * 3
    return jnp.concatenate([weight[base + dj] for dj in range(3)], axis=1)


def dot(a, b):
    return jnp.dot(a, b, preferred_element_type=F32)


def flat(v):
    return v.reshape(-1, v.shape[-1])


def kernel(
    nz,
    nx,
    lat_hbm,
    g0,
    b0,
    w0_hbm,
    c0,
    g1,
    b1,
    w1_hbm,
    c1,
    g2,
    b2,
    w2_hbm,
    c2,
    out,
    lat,
    vectors,
    w0,
    w1,
    w2,
    params,
    r0,
    x1,
    x2,
    act0,
    act1,
    act2,
    middle,
    hidden,
    give,
    take,
    plane_src,
    plane_in,
    line_src,
    line_in,
    i_sem,
    w_sem,
    par_s,
    par_r,
    plane_s,
    plane_r,
    line_s,
    line_r,
    x0_s,
    x0_r,
    z0_s,
    z0_r,
    a_s,
    a_r,
    x1_s,
    x1_r,
    x2_s,
    x2_r,
    h2_r,
    e2_s,
    e2_r,
    o_s,
    o_r,
):
    z = lax.axis_index("seq")
    x = lax.axis_index("ch")
    c = lax.axis_index("col")
    half = nz // 2
    samples = float(nz * nz * 16 * GROUP)

    def peer(dz, dx, col):
        return {"seq": lax.rem(z + dz + nz, nz), "ch": lax.rem(x + dx, nx), "col": col}

    def remote(src, dst, s_sem, r_sem, to):
        return pltpu.make_async_remote_copy(
            src_ref=src,
            dst_ref=dst,
            send_sem=s_sem,
            recv_sem=r_sem,
            device_id=to,
            device_id_type=MESH,
        )

    def landed(ref, sem):
        pltpu.make_async_copy(ref, ref, sem).wait()

    inputs = [pltpu.make_async_copy(lat_hbm, lat, i_sem.at[9])]
    for i, ref in enumerate((g0, b0, g1, b1, g2, b2, c0, c1, c2)):
        inputs.append(pltpu.make_async_copy(ref, vectors.at[i], i_sem.at[i]))
    loads = [
        pltpu.make_async_copy(a, b, w_sem.at[i])
        for i, (a, b) in enumerate(((w0_hbm, w0), (w1_hbm, w1), (w2_hbm, w2)))
    ]
    for copy in inputs:
        copy.start()

    barrier = pltpu.get_barrier_semaphore()
    greeted = []
    for dz in range(nz):
        greeted.append((dz, 0, 1 - c))
        if dz:
            greeted.append((dz, 0, c))
    for dz in (0, 1, nz - 1):
        for dx in range(1, nx):
            greeted.append((dz, dx, c))
            greeted.append((dz, dx, 1 - c))
    greeted.sort(key=lambda g: -min(g[0], nz - g[0]))
    for dz, dx, col in greeted:
        pl.semaphore_signal(barrier, inc=1, device_id=peer(dz, dx, col), device_id_type=MESH)

    for copy in inputs:
        copy.wait()
    for load in loads:
        load.start()
    for i in range(6):
        params[x, i : i + 1, :] = vectors[i]
    own = lat[...].astype(F32)
    plane_src[0] = packed_sums(flat(own), x)
    own_at = ((nx + x) * 2 + c) * 6
    r0[pl.ds(own_at + 1 - c, 5)] = lat[pl.ds(3 * c, 5)]

    pl.semaphore_wait(barrier, len(greeted))

    def plane_start(stage):
        place = 8 * stage + 2 * x + c
        plane_in[place] = plane_src[stage]
        for dx in range(nx):
            for other in (0, 1):
                if dx == 0 and other == 0:
                    continue
                remote(
                    plane_src.at[stage],
                    plane_in.at[place],
                    plane_s.at[stage],
                    plane_r.at[stage],
                    peer(0, dx, c if other == 0 else 1 - c),
                ).start()

    def line_start(stage):
        landed(plane_in.at[pl.ds(8 * stage, 2 * nx - 1)], plane_r.at[stage])
        row = jnp.sum(plane_in[8 * stage : 8 * stage + 2 * nx], axis=0)
        line_src[stage] = row
        line_in[stage * nz + z] = row
        order = sorted(range(1, nz), key=lambda dz: -min(dz, nz - dz))
        for dz in order:
            remote(
                line_src.at[stage],
                line_in.at[stage * nz + z],
                line_s.at[stage],
                line_r.at[stage],
                peer(dz, 0, c),
            ).start()

    def line_total(stage):
        landed(line_in.at[pl.ds(stage * nz, nz - 1)], line_r.at[stage])
        return jnp.sum(line_in[stage * nz : (stage + 1) * nz], axis=0)

    plane_start(0)
    for dx in range(1, nx):
        remote(params.at[x], params.at[x], par_s, par_r, peer(0, dx, c)).start()

    for dx in (2, 1, 3, 0):
        for other in (0, 1):
            if dx == 0 and other == 0:
                continue
            to_col = c if other == 0 else 1 - c
            remote(
                lat.at[pl.ds(3 * to_col, 5)],
                r0.at[pl.ds(own_at + 1 - to_col, 5)],
                x0_s,
                x0_r.at[x * 2 + c],
                peer(0, dx, to_col),
            ).start()

    line_start(0)

    for dx in (0, 1, 3, 2):
        for other in (0, 1):
            from_x = lax.rem(x + dx, nx)
            from_c = c if other == 0 else 1 - c
            at = (from_x * 2 + from_c) * 6
            if not (dx == 0 and other == 0):
                landed(r0.at[pl.ds(nx * 12 + at + 1 - c, 5)], x0_r.at[from_x * 2 + from_c])
            for row, dz in ((0, 1), (2, nz - 1)):
                remote(
                    r0.at[pl.ds(nx * 12 + at, 5)],
                    r0.at[pl.ds(row * nx * 12 + at, 5)],
                    z0_s,
                    z0_r.at[(row // 2) * 8 + from_x * 2 + from_c],
                    peer(dz, 0, c),
                ).start()

    landed(params.at[pl.ds(0, nx - 1)], par_r)
    norm = affine(line_total(0), samples, params, 0, nx)

    def frames_of(row, block):
        at = (row * nx + block) * 12
        parts = []
        for col in range(2):
            v = r0[pl.ds(at + 6 * col, 5)].astype(F32)
            parts.append(v.reshape(10, 8, LANES))
        return jnp.concatenate(parts, axis=1)

    for row in (1, 0, 2):
        for block in range(nx):
            if row != 1:
                for col in range(2):
                    at = (row * nx + block) * 12 + 6 * col
                    landed(r0.at[pl.ds(at, 5)], z0_r.at[(row // 2) * 8 + block * 2 + col])
            scale, shift = norm[block]
            act0[row, :, :, block * LANES : (block + 1) * LANES] = activate(
                frames_of(row, block), scale, shift
            )

    @pl.when(z == 0)
    def _():
        act0[0] = jnp.zeros(act0.shape[1:], BF)

    @pl.when(z == nz - 1)
    def _():
        act0[2] = jnp.zeros(act0.shape[1:], BF)

    @pl.when(c == 0)
    def _():
        act0[:, 0:2] = jnp.zeros((3, 2, *act0.shape[2:]), BF)

    loads[0].wait()
    y = jnp.zeros((half * 16, 3 * LANES), F32)
    for dt in range(3):
        for di in range(3):
            y = y + dot(flat(act0[di, dt : dt + half]), taps(w0, dt, di))
    mixed = column_sum(y.reshape(half, 16, 3 * LANES))
    rest = frames_of(1, x)[2:10]
    value = (rest + mixed + vectors[6].reshape(1, 1, LANES)).astype(BF)
    middle[...] = value
    plane_src[1] = packed_sums(flat(value.astype(F32)), x)
    plane_start(1)

    low, high = lax.rem(z - half * c + nz, nz), lax.rem(z - half * c - half + 1 + nz, nz)
    ascending = jnp.minimum(low, nz - low) <= jnp.minimum(high, nz - high)
    def spread(act):
        for turn in range(half + 1):
            j = jnp.where(ascending, half - turn, turn)
            to_z = lax.rem(half * c + j, nz)
            source = jnp.maximum(j - 1, 0)
            tiles = 2 if 0 < turn < half else 1
            fr = 0 if 0 < turn < half else jnp.where(j == 0, 1, 0)
            for case in range(2):
                if case == 0:
                    to_c = z // half
                    wanted = to_z >= 0
                else:
                    to_c = 1 - z // half
                    wanted = (z == half - 1) | (z == half)
                slot = z - half * to_c + 1
                at = (x * 10 + slot) * 2 + fr
                copy = remote(
                    middle.at[pl.ds(source, tiles)],
                    x1.at[pl.ds(at, tiles)],
                    a_s.at[2 * turn + case],
                    a_r.at[slot],
                    {"seq": to_z, "ch": x, "col": to_c},
                )
                act(copy, source, tiles, at, wanted, (to_z == z) & (to_c == c))

    def a_start(copy, source, tiles, at, wanted, itself):
        @pl.when(wanted & jnp.logical_not(itself))
        def _():
            copy.start()

        @pl.when(wanted & itself)
        def _():
            x1[pl.ds(at, tiles)] = middle[pl.ds(source, tiles)]

    def a_sent(copy, source, tiles, at, wanted, itself):
        @pl.when(wanted & jnp.logical_not(itself))
        def _():
            copy.wait_send()

    spread(a_start)
    line_start(1)

    first = 1 - c
    previous_c = lax.rem(z - 1 + nz, nz) // half
    for turn in range(9):
        slot = first + jnp.where(ascending, turn, 8 - turn)
        mine = half * c - 1 + slot == z
        at = (x * 10 + slot) * 2
        lost_old = mine & (previous_c == c)
        lost_new = mine & (z // half == c)

        @pl.when(jnp.logical_not(lost_old | lost_new))
        def _():
            landed(x1.at[pl.ds(at, 2)], a_r.at[slot])

        @pl.when(lost_old ^ lost_new)
        def _():
            landed(x1.at[pl.ds(at, 1)], a_r.at[slot])

        for dx in (2, 1, 3):
            remote(
                x1.at[pl.ds(at, 2)], x1.at[pl.ds(at, 2)], x1_s, x1_r.at[x], peer(0, dx, c)
            ).start()

    norm = affine(line_total(1), samples, params, 1, nx)
    for block in range(nx):
        @pl.when(block != x)
        def _():
            landed(x1.at[pl.ds((block * 10 + first) * 2, 18)], x1_r.at[block])

        scale, shift = norm[block]
        v = x1[block * 20 : (block + 1) * 20].astype(F32).reshape(10, 2, 16, LANES)
        v = activate(v, scale, shift)
        for fr in range(2):
            act1[fr, :, :, block * LANES : (block + 1) * LANES] = v[:, fr]

    zero_row1 = jnp.zeros((2, 16, nx * LANES), BF)

    @pl.when(c == 0)
    def _():
        act1[:, 0] = zero_row1

    @pl.when(c == 1)
    def _():
        act1[:, 9] = zero_row1

    @pl.when(z == 0)
    def _():
        act1[0] = jnp.zeros(act1.shape[1:], BF)

    loads[1].wait()
    shared = jnp.zeros((half * 16, 3 * LANES), F32)
    apart = jnp.zeros((2 * half * 16, 3 * LANES), F32)
    for di in range(3):
        rows = act1[:, di : di + half]
        shared = shared + dot(flat(rows[0]), taps(w1, 0, di))
        shared = shared + dot(flat(rows[1]), taps(w1, 2, di))
    for di in range(3):
        apart = apart + dot(flat(act1[:, di : di + half]), taps(w1, 1, di))
    y = apart.reshape(2, half, 16, 3 * LANES) + shared.reshape(1, half, 16, 3 * LANES)
    mixed = column_sum(y.reshape(2 * half, 16, 3 * LANES))
    value = (mixed + vectors[7].reshape(1, 1, LANES)).astype(BF)
    plane_src[2] = packed_sums(flat(value.astype(F32)), x)
    value = value.reshape(2, half, 16, LANES)
    for fr in range(2):
        for row in range(half):
            hidden[row * 2 + fr] = value[fr, row]
    plane_start(2)

    x2[pl.ds((x * 2 + 1) * 20 + 2, 2 * half)] = hidden[...]
    edge_at = pl.ds((2 * half - 2) * (1 - c), 2)
    edge_slot = pl.ds(18 * c, 2)
    def x2_block(block, own_frames):
        return pl.ds((block * 2 + own_frames) * 20 + 2, 2 * half)

    def history(part):
        return x2.at[pl.ds(x * 40 + 2 + part * half, half)]

    for part in range(2):
        remote(
            hidden.at[pl.ds(part * half, half)], history(part), x2_s, h2_r.at[part], peer(1, 0, c)
        ).start()
    for dx in (2, 1, 3):
        remote(hidden, x2.at[x2_block(x, 1)], x2_s, x2_r.at[nx + x], peer(0, dx, c)).start()
    for dz in (1, 0):
        for dx in (2, 1, 3, 0):
            slot = pl.ds((x * 2 + 1 - dz) * 20 + 18 * c, 2)
            remote(
                hidden.at[edge_at], x2.at[slot], e2_s, e2_r.at[(1 - dz) * nx + x], peer(dz, dx, 1 - c)
            ).start()
    line_start(2)
    for part in range(2):
        landed(history(part), h2_r.at[part])
        for dx in (2, 1, 3):
            remote(history(part), history(part), x2_s, x2_r.at[x], peer(0, dx, c)).start()
    norm = affine(line_total(2), 2.0 * samples, params, 2, nx)

    for own_frames in (1, 0):
        for block in range(nx):
            sem = own_frames * nx + block
            at = (block * 2 + own_frames) * 20

            @pl.when(block != x)
            def _():
                landed(x2.at[x2_block(block, own_frames)], x2_r.at[sem])

            landed(x2.at[pl.ds(at + 18 * (1 - c), 2)], e2_r.at[sem])
            scale, shift = norm[block]
            v = x2[at : at + 20].astype(F32).reshape(10, 2, 16, LANES)
            v = activate(v, scale, shift)
            for fr in range(2):
                act2[2 * own_frames + fr, :, :, block * LANES : (block + 1) * LANES] = v[:, fr]

    zero_row2 = jnp.zeros((4, 16, nx * LANES), BF)

    @pl.when(c == 0)
    def _():
        act2[:, 0] = zero_row2

    @pl.when(c == 1)
    def _():
        act2[:, 9] = zero_row2

    @pl.when(z == 0)
    def _():
        act2[0:2] = jnp.zeros((2, *act2.shape[1:]), BF)

    loads[2].wait()
    y = jnp.zeros((2 * half * 16, 3 * LANES), F32)
    for dt in range(3):
        for di in range(3):
            y = y + dot(flat(act2[dt : dt + 2, di : di + half]), taps(w2, dt, di))
    mixed = column_sum(y.reshape(2 * half, 16, 3 * LANES)).reshape(2, half, 16, LANES)
    doubled = x1[pl.ds(x * 20 + 2, 2 * half)].astype(F32).reshape(half, 2, 16, LANES)[:, 1]
    final = doubled[None] + mixed + vectors[8].reshape(1, 1, 1, LANES)

    sides = [
        final[:, :, 8 * side : 8 * side + 8].reshape(2, half // 2, 16, LANES).astype(BF)
        for side in range(2)
    ]

    @pl.when(c == 0)
    def _():
        give[...] = sides[1]
        out[:, pl.ds(0, half // 2)] = sides[0]

    @pl.when(c == 1)
    def _():
        give[...] = sides[0]
        out[:, pl.ds(half // 2, half // 2)] = sides[1]

    last = remote(give, take, o_s, o_r, peer(0, 0, 1 - c))
    last.start()

    for stage in range(3):
        landed(plane_in.at[pl.ds(8 * stage, 2 * nx - 1)], plane_s.at[stage])
        landed(line_in.at[pl.ds(stage * nz, nz - 1)], line_s.at[stage])
    landed(params.at[pl.ds(0, nx - 1)], par_s)
    landed(r0.at[pl.ds(0, 5 * (2 * nx - 1))], x0_s)
    landed(r0.at[pl.ds(0, 5 * 4 * nx)], z0_s)
    spread(a_sent)
    landed(x1.at[pl.ds(0, 3 * 3 * 6)], x1_s)
    landed(x2.at[pl.ds(0, 2 * half * (2 * nx - 1))], x2_s)
    landed(x2.at[pl.ds(0, 2 * 2 * nx)], e2_s)
    last.wait()

    @pl.when(c == 0)
    def _():
        out[:, pl.ds(half // 2, half // 2)] = take[...]

    @pl.when(c == 1)
    def _():
        out[:, pl.ds(0, half // 2)] = take[...]


def body(nz, nx, *args):
    latent = args[0]
    frames = latent.shape[0]
    half = nz // 2
    channels = nx * LANES
    operands = [latent.reshape(frames // 2, 16, LANES)]
    for a in args[1:]:
        operands.append(a.reshape((1, LANES) if a.ndim == 1 else (27, channels, LANES)))
    weight = pltpu.VMEM((27, channels, LANES), BF)
    dma = pltpu.SemaphoreType.DMA
    result = pl.pallas_call(
        functools.partial(kernel, nz, nx),
        out_shape=jax.ShapeDtypeStruct((2, half, 16, LANES), BF),
        in_specs=[pl.BlockSpec(memory_space=pl.ANY)] * len(operands),
        out_specs=pl.BlockSpec(memory_space=pltpu.VMEM),
        scratch_shapes=[
            pltpu.VMEM((frames // 2, 16, LANES), BF),
            pltpu.VMEM((9, 1, LANES), F32),
            weight,
            weight,
            weight,
            pltpu.VMEM((nx, 8, LANES), F32),
            pltpu.VMEM((3 * nx * 2 * 6, 16, LANES), BF),
            pltpu.VMEM((nx * 10 * 2, 16, LANES), BF),
            pltpu.VMEM((nx * 2 * 10 * 2, 16, LANES), BF),
            pltpu.VMEM((3, half + 2, 16, channels), BF),
            pltpu.VMEM((2, half + 2, 16, channels), BF),
            pltpu.VMEM((4, half + 2, 16, channels), BF),
            pltpu.VMEM((half, 16, LANES), BF),
            pltpu.VMEM((2 * half, 16, LANES), BF),
            pltpu.VMEM((2, half // 2, 16, LANES), BF),
            pltpu.VMEM((2, half // 2, 16, LANES), BF),
            pltpu.VMEM((3, 1, LANES), F32),
            pltpu.VMEM((3 * 8, 1, LANES), F32),
            pltpu.VMEM((3, 1, LANES), F32),
            pltpu.VMEM((3 * nz, 1, LANES), F32),
            dma((10,)),
            dma((3,)),
            dma,
            dma,
            dma((3,)),
            dma((3,)),
            dma((3,)),
            dma((3,)),
            dma,
            dma((2 * nx,)),
            dma,
            dma((4 * nx,)),
            dma((2 * half + 2,)),
            dma((10,)),
            dma,
            dma((nx,)),
            dma,
            dma((2 * nx,)),
            dma((2,)),
            dma,
            dma((2 * nx,)),
            dma,
            dma,
        ],
        compiler_params=pltpu.CompilerParams(collective_id=0, has_side_effects=True),
    )(*operands)
    return result.reshape(2, nz, 8, LANES)


def solution(mesh):
    nz, nx = mesh.shape["seq"], mesh.shape["ch"]
    in_specs = (
        P("grp", "seq", "col", "ch"),
        *(P("ch"), P("ch"), P(None, None, None, None, "ch"), P("ch")) * 3,
    )
    out_specs = P(("grp", "seq"), None, "col", "ch")
    return jax.shard_map(
        functools.partial(body, nz, nx),
        mesh=mesh,
        in_specs=in_specs,
        out_specs=out_specs,
        check_vma=False,
    )
```

```python
import functools

import jax
import jax.numpy as jnp
from jax import lax
from jax.experimental import pallas as pl
from jax.experimental.pallas import tpu as pltpu
from jax.sharding import PartitionSpec as P

MESH = pl.DeviceIdType.MESH
GROUP = 16
LANES = 128
EPS = 0.01
BF = jnp.bfloat16
F32 = jnp.float32


def lane_ids():
    return lax.broadcasted_iota(jnp.int32, (8, LANES), 1)


def row_ids():
    return lax.broadcasted_iota(jnp.int32, (8, LANES), 0)


def group_total(v):
    lane = lane_ids()
    step = GROUP // 2
    while step:
        from_below = pltpu.roll(v, step, 1)
        from_above = pltpu.roll(v, LANES - step, 1)
        v = v + jnp.where((lane & step) != 0, from_below, from_above)
        step //= 2
    return v


def packed_sums(values, x):
    total = jnp.sum(values, axis=0, keepdims=True)
    square = jnp.sum(values * values, axis=0, keepdims=True)
    total = group_total(jnp.broadcast_to(total, (8, LANES)))
    square = group_total(jnp.broadcast_to(square, (8, LANES)))
    slot = lane_ids() & 7
    row = jnp.where(slot == 2 * x, total, jnp.where(slot == 2 * x + 1, square, 0.0))
    return row[0:1]


def affine(row, samples, params, which, nx):
    spread_rows = jnp.broadcast_to(row, (8, LANES))
    picked = jnp.where((lane_ids() & (GROUP - 1)) == row_ids(), spread_rows, 0.0)
    sums = group_total(picked) * (1.0 / samples)
    out = []
    for block in range(nx):
        mean = sums[2 * block : 2 * block + 1]
        square = sums[2 * block + 1 : 2 * block + 2]
        inverse = 1.0 / jnp.sqrt(square - mean * mean + EPS)
        gain = params[block, 2 * which : 2 * which + 1]
        bias = params[block, 2 * which + 1 : 2 * which + 2]
        scale = inverse * gain
        out.append((scale, bias - mean * scale))
    return out


def activate(values, scale, shift):
    u = values * scale.reshape((1,) * (values.ndim - 1) + (LANES,)) + shift.reshape(
        (1,) * (values.ndim - 1) + (LANES,)
    )
    half = 0.5 * u
    return (half + half * jnp.tanh(half)).astype(BF)


def column_sum(y):
    n, cols = y.shape[0], y.shape[1]
    left, mid, right = (y[:, :, i * LANES : (i + 1) * LANES] for i in range(3))
    col = lax.broadcasted_iota(jnp.int32, (n, cols, LANES), 1)
    left = jnp.where(col == 0, 0.0, pltpu.roll(left, 1, 1))
    right = jnp.where(col == cols - 1, 0.0, pltpu.roll(right, cols - 1, 1))
    return left + mid + right


def taps(weight, dt, di):
    base = dt * 9 + di * 3
    return jnp.concatenate([weight[base + dj] for dj in range(3)], axis=1)


def dot(a, b):
    return jnp.dot(a, b, preferred_element_type=F32)


def flat(v):
    return v.reshape(-1, v.shape[-1])


def kernel(
    nz,
    nx,
    lat_hbm,
    g0,
    b0,
    w0_hbm,
    c0,
    g1,
    b1,
    w1_hbm,
    c1,
    g2,
    b2,
    w2_hbm,
    c2,
    out,
    lat,
    vectors,
    w0,
    w1,
    w2,
    params,
    r0,
    x1,
    x2,
    act0,
    act1,
    act2,
    middle,
    hidden,
    give,
    take,
    plane_src,
    plane_in,
    line_src,
    line_in,
    i_sem,
    w_sem,
    par_s,
    par_r,
    plane_s,
    plane_r,
    line_s,
    line_r,
    x0_s,
    x0_r,
    z0_s,
    z0_r,
    a_s,
    a_r,
    x1_s,
    x1_r,
    x2_s,
    x2_r,
    h2_r,
    e2_s,
    e2_r,
    o_s,
    o_r,
):
    z = lax.axis_index("seq")
    x = lax.axis_index("ch")
    c = lax.axis_index("col")
    half = nz // 2
    samples = float(nz * nz * 16 * GROUP)

    def peer(dz, dx, col):
        return {"seq": lax.rem(z + dz + nz, nz), "ch": lax.rem(x + dx, nx), "col": col}

    def remote(src, dst, s_sem, r_sem, to):
        return pltpu.make_async_remote_copy(
            src_ref=src,
            dst_ref=dst,
            send_sem=s_sem,
            recv_sem=r_sem,
            device_id=to,
            device_id_type=MESH,
        )

    def landed(ref, sem):
        pltpu.make_async_copy(ref, ref, sem).wait()

    inputs = [pltpu.make_async_copy(lat_hbm, lat, i_sem.at[9])]
    for i, ref in enumerate((g0, b0, g1, b1, g2, b2, c0, c1, c2)):
        inputs.append(pltpu.make_async_copy(ref, vectors.at[i], i_sem.at[i]))
    loads = [
        pltpu.make_async_copy(a, b, w_sem.at[i])
        for i, (a, b) in enumerate(((w0_hbm, w0), (w1_hbm, w1), (w2_hbm, w2)))
    ]
    for copy in inputs:
        copy.start()

    barrier = pltpu.get_barrier_semaphore()
    greeted = [(dz, 0, c) for dz in range(1, nz)] + [(0, 0, 1 - c)]
    for dx in range(1, nx):
        greeted += [(0, dx, c), (0, dx, 1 - c)]
    greeted.sort(key=lambda g: -min(g[0], nz - g[0]))
    for dz, dx, col in greeted:
        pl.semaphore_signal(barrier, inc=1, device_id=peer(dz, dx, col), device_id_type=MESH)

    for copy in inputs:
        copy.wait()
    for load in loads:
        load.start()
    for i in range(6):
        params[x, i : i + 1, :] = vectors[i]
    own = lat[...].astype(F32)
    plane_src[0] = packed_sums(flat(own), x)
    own_at = ((nx + x) * 2 + c) * 6
    r0[pl.ds(own_at + 1 - c, 5)] = lat[pl.ds(3 * c, 5)]

    pl.semaphore_wait(barrier, len(greeted))

    def plane_start(stage):
        place = 8 * stage + 2 * x + c
        plane_in[place] = plane_src[stage]
        for dx in range(nx):
            for other in (0, 1):
                if dx == 0 and other == 0:
                    continue
                remote(
                    plane_src.at[stage],
                    plane_in.at[place],
                    plane_s.at[stage],
                    plane_r.at[stage],
                    peer(0, dx, c if other == 0 else 1 - c),
                ).start()

    def line_start(stage):
        landed(plane_in.at[pl.ds(8 * stage, 2 * nx - 1)], plane_r.at[stage])
        row = jnp.sum(plane_in[8 * stage : 8 * stage + 2 * nx], axis=0)
        line_src[stage] = row
        line_in[stage * nz + z] = row
        order = sorted(range(1, nz), key=lambda dz: -min(dz, nz - dz))
        for dz in order:
            remote(
                line_src.at[stage],
                line_in.at[stage * nz + z],
                line_s.at[stage],
                line_r.at[stage],
                peer(dz, 0, c),
            ).start()

    def line_total(stage):
        landed(line_in.at[pl.ds(stage * nz, nz - 1)], line_r.at[stage])
        return jnp.sum(line_in[stage * nz : (stage + 1) * nz], axis=0)

    plane_start(0)
    for dx in range(1, nx):
        remote(params.at[x], params.at[x], par_s, par_r, peer(0, dx, c)).start()

    for dx in (2, 1, 3, 0):
        for other in (0, 1):
            if dx == 0 and other == 0:
                continue
            to_col = c if other == 0 else 1 - c
            remote(
                lat.at[pl.ds(3 * to_col, 5)],
                r0.at[pl.ds(own_at + 1 - to_col, 5)],
                x0_s,
                x0_r.at[x * 2 + c],
                peer(0, dx, to_col),
            ).start()

    line_start(0)

    for dx in (0, 1, 3, 2):
        for other in (0, 1):
            from_x = lax.rem(x + dx, nx)
            from_c = c if other == 0 else 1 - c
            at = (from_x * 2 + from_c) * 6
            if not (dx == 0 and other == 0):
                landed(r0.at[pl.ds(nx * 12 + at + 1 - c, 5)], x0_r.at[from_x * 2 + from_c])
            for row, dz in ((0, 1), (2, nz - 1)):
                remote(
                    r0.at[pl.ds(nx * 12 + at, 5)],
                    r0.at[pl.ds(row * nx * 12 + at, 5)],
                    z0_s,
                    z0_r.at[(row // 2) * 8 + from_x * 2 + from_c],
                    peer(dz, 0, c),
                ).start()

    landed(params.at[pl.ds(0, nx - 1)], par_r)
    norm = affine(line_total(0), samples, params, 0, nx)

    def frames_of(row, block):
        at = (row * nx + block) * 12
        parts = []
        for col in range(2):
            v = r0[pl.ds(at + 6 * col, 5)].astype(F32)
            parts.append(v.reshape(10, 8, LANES))
        return jnp.concatenate(parts, axis=1)

    for row in (1, 0, 2):
        for block in range(nx):
            if row != 1:
                for col in range(2):
                    at = (row * nx + block) * 12 + 6 * col
                    landed(r0.at[pl.ds(at, 5)], z0_r.at[(row // 2) * 8 + block * 2 + col])
            scale, shift = norm[block]
            act0[row, :, :, block * LANES : (block + 1) * LANES] = activate(
                frames_of(row, block), scale, shift
            )

    @pl.when(z == 0)
    def _():
        act0[0] = jnp.zeros(act0.shape[1:], BF)

    @pl.when(z == nz - 1)
    def _():
        act0[2] = jnp.zeros(act0.shape[1:], BF)

    @pl.when(c == 0)
    def _():
        act0[:, 0:2] = jnp.zeros((3, 2, *act0.shape[2:]), BF)

    loads[0].wait()
    y = jnp.zeros((half * 16, 3 * LANES), F32)
    for dt in range(3):
        for di in range(3):
            y = y + dot(flat(act0[di, dt : dt + half]), taps(w0, dt, di))
    mixed = column_sum(y.reshape(half, 16, 3 * LANES))
    rest = frames_of(1, x)[2:10]
    value = (rest + mixed + vectors[6].reshape(1, 1, LANES)).astype(BF)
    middle[...] = value
    plane_src[1] = packed_sums(flat(value.astype(F32)), x)
    plane_start(1)

    low, high = lax.rem(z - half * c + nz, nz), lax.rem(z - half * c - half + 1 + nz, nz)
    ascending = jnp.minimum(low, nz - low) <= jnp.minimum(high, nz - high)
    def spread(act):
        for turn in range(half + 1):
            j = jnp.where(ascending, half - turn, turn)
            to_z = lax.rem(half * c + j, nz)
            source = jnp.maximum(j - 1, 0)
            tiles = 2 if 0 < turn < half else 1
            fr = 0 if 0 < turn < half else jnp.where(j == 0, 1, 0)
            for case in range(2):
                if case == 0:
                    to_c = z // half
                    wanted = to_z >= 0
                else:
                    to_c = 1 - z // half
                    wanted = (z == half - 1) | (z == half)
                slot = z - half * to_c + 1
                at = (x * 10 + slot) * 2 + fr
                copy = remote(
                    middle.at[pl.ds(source, tiles)],
                    x1.at[pl.ds(at, tiles)],
                    a_s.at[2 * turn + case],
                    a_r.at[slot],
                    {"seq": to_z, "ch": x, "col": to_c},
                )
                act(copy, source, tiles, at, wanted, (to_z == z) & (to_c == c))

    def a_start(copy, source, tiles, at, wanted, itself):
        @pl.when(wanted & jnp.logical_not(itself))
        def _():
            copy.start()

        @pl.when(wanted & itself)
        def _():
            x1[pl.ds(at, tiles)] = middle[pl.ds(source, tiles)]

    def a_sent(copy, source, tiles, at, wanted, itself):
        @pl.when(wanted & jnp.logical_not(itself))
        def _():
            copy.wait_send()

    spread(a_start)
    line_start(1)

    first = 1 - c
    previous_c = lax.rem(z - 1 + nz, nz) // half
    for turn in range(9):
        slot = first + jnp.where(ascending, turn, 8 - turn)
        mine = half * c - 1 + slot == z
        at = (x * 10 + slot) * 2
        lost_old = mine & (previous_c == c)
        lost_new = mine & (z // half == c)

        @pl.when(jnp.logical_not(lost_old | lost_new))
        def _():
            landed(x1.at[pl.ds(at, 2)], a_r.at[slot])

        @pl.when(lost_old ^ lost_new)
        def _():
            landed(x1.at[pl.ds(at, 1)], a_r.at[slot])

        for dx in (2, 1, 3):
            remote(
                x1.at[pl.ds(at, 2)], x1.at[pl.ds(at, 2)], x1_s, x1_r.at[x], peer(0, dx, c)
            ).start()

    norm = affine(line_total(1), samples, params, 1, nx)
    for block in range(nx):
        @pl.when(block != x)
        def _():
            landed(x1.at[pl.ds((block * 10 + first) * 2, 18)], x1_r.at[block])

        scale, shift = norm[block]
        v = x1[block * 20 : (block + 1) * 20].astype(F32).reshape(10, 2, 16, LANES)
        v = activate(v, scale, shift)
        for fr in range(2):
            act1[fr, :, :, block * LANES : (block + 1) * LANES] = v[:, fr]

    zero_row1 = jnp.zeros((2, 16, nx * LANES), BF)

    @pl.when(c == 0)
    def _():
        act1[:, 0] = zero_row1

    @pl.when(c == 1)
    def _():
        act1[:, 9] = zero_row1

    @pl.when(z == 0)
    def _():
        act1[0] = jnp.zeros(act1.shape[1:], BF)

    loads[1].wait()
    shared = jnp.zeros((half * 16, 3 * LANES), F32)
    apart = jnp.zeros((2 * half * 16, 3 * LANES), F32)
    for di in range(3):
        rows = act1[:, di : di + half]
        shared = shared + dot(flat(rows[0]), taps(w1, 0, di))
        shared = shared + dot(flat(rows[1]), taps(w1, 2, di))
    for di in range(3):
        apart = apart + dot(flat(act1[:, di : di + half]), taps(w1, 1, di))
    y = apart.reshape(2, half, 16, 3 * LANES) + shared.reshape(1, half, 16, 3 * LANES)
    mixed = column_sum(y.reshape(2 * half, 16, 3 * LANES))
    value = (mixed + vectors[7].reshape(1, 1, LANES)).astype(BF)
    plane_src[2] = packed_sums(flat(value.astype(F32)), x)
    value = value.reshape(2, half, 16, LANES)
    for fr in range(2):
        for row in range(half):
            hidden[row * 2 + fr] = value[fr, row]
    plane_start(2)

    x2[pl.ds((x * 2 + 1) * 20 + 2, 2 * half)] = hidden[...]
    edge_at = pl.ds((2 * half - 2) * (1 - c), 2)
    edge_slot = pl.ds(18 * c, 2)
    def x2_block(block, own_frames):
        return pl.ds((block * 2 + own_frames) * 20 + 2, 2 * half)

    def history(part):
        return x2.at[pl.ds(x * 40 + 2 + part * half, half)]

    for part in range(2):
        remote(
            hidden.at[pl.ds(part * half, half)], history(part), x2_s, h2_r.at[part], peer(1, 0, c)
        ).start()
    for dx in (2, 1, 3):
        remote(hidden, x2.at[x2_block(x, 1)], x2_s, x2_r.at[nx + x], peer(0, dx, c)).start()
    for dz in (1, 0):
        for dx in (2, 1, 3, 0):
            slot = pl.ds((x * 2 + 1 - dz) * 20 + 18 * c, 2)
            remote(
                hidden.at[edge_at], x2.at[slot], e2_s, e2_r.at[(1 - dz) * nx + x], peer(dz, dx, 1 - c)
            ).start()
    line_start(2)
    for part in range(2):
        landed(history(part), h2_r.at[part])
        for dx in (2, 1, 3):
            remote(history(part), history(part), x2_s, x2_r.at[x], peer(0, dx, c)).start()
    norm = affine(line_total(2), 2.0 * samples, params, 2, nx)

    for own_frames in (1, 0):
        for block in range(nx):
            sem = own_frames * nx + block
            at = (block * 2 + own_frames) * 20

            @pl.when(block != x)
            def _():
                landed(x2.at[x2_block(block, own_frames)], x2_r.at[sem])

            landed(x2.at[pl.ds(at + 18 * (1 - c), 2)], e2_r.at[sem])
            scale, shift = norm[block]
            v = x2[at : at + 20].astype(F32).reshape(10, 2, 16, LANES)
            v = activate(v, scale, shift)
            for fr in range(2):
                act2[2 * own_frames + fr, :, :, block * LANES : (block + 1) * LANES] = v[:, fr]

    zero_row2 = jnp.zeros((4, 16, nx * LANES), BF)

    @pl.when(c == 0)
    def _():
        act2[:, 0] = zero_row2

    @pl.when(c == 1)
    def _():
        act2[:, 9] = zero_row2

    @pl.when(z == 0)
    def _():
        act2[0:2] = jnp.zeros((2, *act2.shape[1:]), BF)

    loads[2].wait()
    y = jnp.zeros((2 * half * 16, 3 * LANES), F32)
    for dt in range(3):
        for di in range(3):
            y = y + dot(flat(act2[dt : dt + 2, di : di + half]), taps(w2, dt, di))
    mixed = column_sum(y.reshape(2 * half, 16, 3 * LANES)).reshape(2, half, 16, LANES)
    doubled = x1[pl.ds(x * 20 + 2, 2 * half)].astype(F32).reshape(half, 2, 16, LANES)[:, 1]
    final = doubled[None] + mixed + vectors[8].reshape(1, 1, 1, LANES)

    sides = [
        final[:, :, 8 * side : 8 * side + 8].reshape(2, half // 2, 16, LANES).astype(BF)
        for side in range(2)
    ]

    @pl.when(c == 0)
    def _():
        give[...] = sides[1]
        out[:, pl.ds(0, half // 2)] = sides[0]

    @pl.when(c == 1)
    def _():
        give[...] = sides[0]
        out[:, pl.ds(half // 2, half // 2)] = sides[1]

    last = remote(give, take, o_s, o_r, peer(0, 0, 1 - c))
    last.start()

    for stage in range(3):
        landed(plane_in.at[pl.ds(8 * stage, 2 * nx - 1)], plane_s.at[stage])
        landed(line_in.at[pl.ds(stage * nz, nz - 1)], line_s.at[stage])
    landed(params.at[pl.ds(0, nx - 1)], par_s)
    landed(r0.at[pl.ds(0, 5 * (2 * nx - 1))], x0_s)
    landed(r0.at[pl.ds(0, 5 * 4 * nx)], z0_s)
    spread(a_sent)
    landed(x1.at[pl.ds(0, 3 * 3 * 6)], x1_s)
    landed(x2.at[pl.ds(0, 2 * half * (2 * nx - 1))], x2_s)
    landed(x2.at[pl.ds(0, 2 * 2 * nx)], e2_s)
    last.wait()

    @pl.when(c == 0)
    def _():
        out[:, pl.ds(half // 2, half // 2)] = take[...]

    @pl.when(c == 1)
    def _():
        out[:, pl.ds(0, half // 2)] = take[...]


def body(nz, nx, *args):
    latent = args[0]
    frames = latent.shape[0]
    half = nz // 2
    channels = nx * LANES
    operands = [latent.reshape(frames // 2, 16, LANES)]
    for a in args[1:]:
        operands.append(a.reshape((1, LANES) if a.ndim == 1 else (27, channels, LANES)))
    weight = pltpu.VMEM((27, channels, LANES), BF)
    dma = pltpu.SemaphoreType.DMA
    result = pl.pallas_call(
        functools.partial(kernel, nz, nx),
        out_shape=jax.ShapeDtypeStruct((2, half, 16, LANES), BF),
        in_specs=[pl.BlockSpec(memory_space=pl.ANY)] * len(operands),
        out_specs=pl.BlockSpec(memory_space=pltpu.VMEM),
        scratch_shapes=[
            pltpu.VMEM((frames // 2, 16, LANES), BF),
            pltpu.VMEM((9, 1, LANES), F32),
            weight,
            weight,
            weight,
            pltpu.VMEM((nx, 8, LANES), F32),
            pltpu.VMEM((3 * nx * 2 * 6, 16, LANES), BF),
            pltpu.VMEM((nx * 10 * 2, 16, LANES), BF),
            pltpu.VMEM((nx * 2 * 10 * 2, 16, LANES), BF),
            pltpu.VMEM((3, half + 2, 16, channels), BF),
            pltpu.VMEM((2, half + 2, 16, channels), BF),
            pltpu.VMEM((4, half + 2, 16, channels), BF),
            pltpu.VMEM((half, 16, LANES), BF),
            pltpu.VMEM((2 * half, 16, LANES), BF),
            pltpu.VMEM((2, half // 2, 16, LANES), BF),
            pltpu.VMEM((2, half // 2, 16, LANES), BF),
            pltpu.VMEM((3, 1, LANES), F32),
            pltpu.VMEM((3 * 8, 1, LANES), F32),
            pltpu.VMEM((3, 1, LANES), F32),
            pltpu.VMEM((3 * nz, 1, LANES), F32),
            dma((10,)),
            dma((3,)),
            dma,
            dma,
            dma((3,)),
            dma((3,)),
            dma((3,)),
            dma((3,)),
            dma,
            dma((2 * nx,)),
            dma,
            dma((4 * nx,)),
            dma((2 * half + 2,)),
            dma((10,)),
            dma,
            dma((nx,)),
            dma,
            dma((2 * nx,)),
            dma((2,)),
            dma,
            dma((2 * nx,)),
            dma,
            dma,
        ],
        compiler_params=pltpu.CompilerParams(collective_id=0, has_side_effects=True, vmem_limit_bytes=50 * 2**20),
    )(*[pltpu.with_memory_space_constraint(a, pltpu.HBM) for a in operands])
    return result.reshape(2, nz, 8, LANES)


def solution(mesh):
    nz, nx = mesh.shape["seq"], mesh.shape["ch"]
    in_specs = (
        P("grp", "seq", "col", "ch"),
        *(P("ch"), P("ch"), P(None, None, None, None, "ch"), P("ch")) * 3,
    )
    out_specs = P(("grp", "seq"), None, "col", "ch")
    return jax.shard_map(
        functools.partial(body, nz, nx),
        mesh=mesh,
        in_specs=in_specs,
        out_specs=out_specs,
        check_vma=False,
    )
```

```python
import functools

import jax
import jax.numpy as jnp
from jax import lax
from jax.experimental import pallas as pl
from jax.experimental.pallas import tpu as pltpu
from jax.sharding import PartitionSpec as P

MESH = pl.DeviceIdType.MESH
GROUP = 16
LANES = 128
EPS = 0.01
BF = jnp.bfloat16
F32 = jnp.float32


def lane_ids():
    return lax.broadcasted_iota(jnp.int32, (8, LANES), 1)


def row_ids():
    return lax.broadcasted_iota(jnp.int32, (8, LANES), 0)


def group_total(v):
    lane = lane_ids()
    step = GROUP // 2
    while step:
        from_below = pltpu.roll(v, step, 1)
        from_above = pltpu.roll(v, LANES - step, 1)
        v = v + jnp.where((lane & step) != 0, from_below, from_above)
        step //= 2
    return v


def packed_sums(values, x):
    total = jnp.sum(values, axis=0, keepdims=True)
    square = jnp.sum(values * values, axis=0, keepdims=True)
    total = group_total(jnp.broadcast_to(total, (8, LANES)))
    square = group_total(jnp.broadcast_to(square, (8, LANES)))
    slot = lane_ids() & 7
    row = jnp.where(slot == 2 * x, total, jnp.where(slot == 2 * x + 1, square, 0.0))
    return row[0:1]


def affine(row, samples, params, which, nx):
    spread_rows = jnp.broadcast_to(row, (8, LANES))
    picked = jnp.where((lane_ids() & (GROUP - 1)) == row_ids(), spread_rows, 0.0)
    sums = group_total(picked) * (1.0 / samples)
    out = []
    for block in range(nx):
        mean = sums[2 * block : 2 * block + 1]
        square = sums[2 * block + 1 : 2 * block + 2]
        inverse = 1.0 / jnp.sqrt(square - mean * mean + EPS)
        gain = params[block, 2 * which : 2 * which + 1]
        bias = params[block, 2 * which + 1 : 2 * which + 2]
        scale = inverse * gain
        out.append((scale, bias - mean * scale))
    return out


def activate(values, scale, shift):
    u = values * scale.reshape((1,) * (values.ndim - 1) + (LANES,)) + shift.reshape(
        (1,) * (values.ndim - 1) + (LANES,)
    )
    half = 0.5 * u
    return (half + half * jnp.tanh(half)).astype(BF)


def column_sum(y):
    n, cols = y.shape[0], y.shape[1]
    left, mid, right = (y[:, :, i * LANES : (i + 1) * LANES] for i in range(3))
    col = lax.broadcasted_iota(jnp.int32, (n, cols, LANES), 1)
    left = jnp.where(col == 0, 0.0, pltpu.roll(left, 1, 1))
    right = jnp.where(col == cols - 1, 0.0, pltpu.roll(right, cols - 1, 1))
    return left + mid + right


def taps(weight, dt, di):
    base = dt * 9 + di * 3
    return jnp.concatenate([weight[base + dj] for dj in range(3)], axis=1)


def dot(a, b):
    return jnp.dot(a, b, preferred_element_type=F32)


def flat(v):
    return v.reshape(-1, v.shape[-1])


def kernel(
    nz,
    nx,
    lat_hbm,
    g0,
    b0,
    w0_hbm,
    c0,
    g1,
    b1,
    w1_hbm,
    c1,
    g2,
    b2,
    w2_hbm,
    c2,
    out,
    lat,
    vectors,
    w0,
    w1,
    w2,
    params,
    r0,
    x1,
    x2,
    act0,
    act1,
    act2,
    middle,
    hidden,
    give,
    take,
    plane_src,
    plane_in,
    line_src,
    line_in,
    hub_in,
    total_row,
    i_sem,
    w_sem,
    par_s,
    par_r,
    hub_s,
    hub_r,
    plane_s,
    plane_r,
    line_s,
    line_r,
    x0_s,
    x0_r,
    z0_s,
    z0_r,
    a_s,
    a_r,
    x1_s,
    x1_r,
    x2_s,
    x2_r,
    h2_r,
    e2_s,
    e2_r,
    o_s,
    o_r,
):
    z = lax.axis_index("seq")
    x = lax.axis_index("ch")
    c = lax.axis_index("col")
    half = nz // 2
    samples = float(nz * nz * 16 * GROUP)

    def peer(dz, dx, col):
        return {"seq": lax.rem(z + dz + nz, nz), "ch": lax.rem(x + dx, nx), "col": col}

    def remote(src, dst, s_sem, r_sem, to):
        return pltpu.make_async_remote_copy(
            src_ref=src,
            dst_ref=dst,
            send_sem=s_sem,
            recv_sem=r_sem,
            device_id=to,
            device_id_type=MESH,
        )

    def landed(ref, sem):
        pltpu.make_async_copy(ref, ref, sem).wait()

    inputs = [pltpu.make_async_copy(lat_hbm, lat, i_sem.at[9])]
    for i, ref in enumerate((g0, b0, g1, b1, g2, b2, c0, c1, c2)):
        inputs.append(pltpu.make_async_copy(ref, vectors.at[i], i_sem.at[i]))
    loads = [
        pltpu.make_async_copy(a, b, w_sem.at[i])
        for i, (a, b) in enumerate(((w0_hbm, w0), (w1_hbm, w1), (w2_hbm, w2)))
    ]
    for copy in inputs:
        copy.start()

    hub = 1
    barrier = pltpu.get_barrier_semaphore()

    def greet(dz, dx, col):
        pl.semaphore_signal(barrier, inc=1, device_id=peer(dz, dx, col), device_id_type=MESH)

    greet(1, 0, c)
    greet(nz - 1, 0, c)
    for dx in range(nx):
        greet(0, dx, 1 - c)
        if dx:
            greet(0, dx, c)

    @pl.when(z == hub)
    def _():
        def greet_all(dz, carry):
            for dx in range(nx):
                greet(dz, dx, 1 - c)
                if dx:
                    greet(dz, dx, c)
            return carry

        lax.fori_loop(1, nz, greet_all, 0)

        def greet_line(dz, carry):
            greet(dz, 0, c)
            return carry

        lax.fori_loop(2, nz - 1, greet_line, 0)

    near = (z == hub + 1) | (z == hub - 1)
    awaited = 2 * nx + 1 + jnp.where(z == hub, 0, jnp.where(near, 2 * nx - 1, 2 * nx))

    for copy in inputs:
        copy.wait()
    for load in loads:
        load.start()
    for i in range(6):
        params[x, i : i + 1, :] = vectors[i]
    own = lat[...].astype(F32)
    plane_src[0] = packed_sums(flat(own), x)
    own_at = ((nx + x) * 2 + c) * 6
    r0[pl.ds(own_at + 1 - c, 5)] = lat[pl.ds(3 * c, 5)]

    pl.semaphore_wait(barrier, awaited)

    def hub_start():
        place = (z * nx + x) * 2 + c

        @pl.when(z != hub)
        def _():
            for dx in (2, 1, 3, 0):
                for col in (c, 1 - c):
                    remote(
                        plane_src.at[0],
                        hub_in.at[place],
                        hub_s,
                        hub_r,
                        {"seq": hub, "ch": lax.rem(x + dx, nx), "col": col},
                    ).start()

        @pl.when(z == hub)
        def _():
            hub_in[place] = plane_src[0]
            for dx in (2, 1, 3, 0):
                for col in (c, 1 - c):
                    if dx == 0 and col is c:
                        continue
                    remote(
                        plane_src.at[0],
                        hub_in.at[place],
                        plane_s.at[0],
                        hub_r,
                        {"seq": hub, "ch": lax.rem(x + dx, nx), "col": col},
                    ).start()

    def hub_run():
        @pl.when(z == hub)
        def _():
            landed(hub_in.at[pl.ds(0, nz * nx * 2 - 1)], hub_r)
            total_row[0] = jnp.sum(hub_in[...], axis=0)

            def far_first(k, carry):
                step = (k + 1) // 2
                dz = half + step * (2 * lax.rem(k, 2) - 1)
                remote(
                    total_row.at[0], total_row.at[0], line_s.at[0], line_r.at[0], peer(dz, 0, c)
                ).start()
                return carry

            lax.fori_loop(0, nz - 1, far_first, 0)

    def hub_total():
        @pl.when(z != hub)
        def _():
            landed(total_row.at[0], line_r.at[0])

        return total_row[0]

    def plane_start(stage):
        place = 8 * stage + 2 * x + c
        plane_in[place] = plane_src[stage]
        for dx in range(nx):
            for other in (0, 1):
                if dx == 0 and other == 0:
                    continue
                remote(
                    plane_src.at[stage],
                    plane_in.at[place],
                    plane_s.at[stage],
                    plane_r.at[stage],
                    peer(0, dx, c if other == 0 else 1 - c),
                ).start()

    def line_start(stage):
        landed(plane_in.at[pl.ds(8 * stage, 2 * nx - 1)], plane_r.at[stage])
        row = jnp.sum(plane_in[8 * stage : 8 * stage + 2 * nx], axis=0)
        line_src[stage] = row
        line_in[stage * nz + z] = row
        order = sorted(range(1, nz), key=lambda dz: -min(dz, nz - dz))
        for dz in order:
            remote(
                line_src.at[stage],
                line_in.at[stage * nz + z],
                line_s.at[stage],
                line_r.at[stage],
                peer(dz, 0, c),
            ).start()

    def line_total(stage):
        landed(line_in.at[pl.ds(stage * nz, nz - 1)], line_r.at[stage])
        return jnp.sum(line_in[stage * nz : (stage + 1) * nz], axis=0)

    hub_start()
    for dx in range(1, nx):
        remote(params.at[x], params.at[x], par_s, par_r, peer(0, dx, c)).start()

    for dx in (2, 1, 3, 0):
        for other in (0, 1):
            if dx == 0 and other == 0:
                continue
            to_col = c if other == 0 else 1 - c
            remote(
                lat.at[pl.ds(3 * to_col, 5)],
                r0.at[pl.ds(own_at + 1 - to_col, 5)],
                x0_s,
                x0_r.at[x * 2 + c],
                peer(0, dx, to_col),
            ).start()

    for dx in (0, 1, 3, 2):
        for other in (0, 1):
            from_x = lax.rem(x + dx, nx)
            from_c = c if other == 0 else 1 - c
            at = (from_x * 2 + from_c) * 6
            if not (dx == 0 and other == 0):
                landed(r0.at[pl.ds(nx * 12 + at + 1 - c, 5)], x0_r.at[from_x * 2 + from_c])
            for row, dz in ((0, 1), (2, nz - 1)):
                remote(
                    r0.at[pl.ds(nx * 12 + at, 5)],
                    r0.at[pl.ds(row * nx * 12 + at, 5)],
                    z0_s,
                    z0_r.at[(row // 2) * 8 + from_x * 2 + from_c],
                    peer(dz, 0, c),
                ).start()

    hub_run()
    landed(params.at[pl.ds(0, nx - 1)], par_r)
    norm = affine(hub_total(), samples, params, 0, nx)

    def frames_of(row, block):
        at = (row * nx + block) * 12
        parts = []
        for col in range(2):
            v = r0[pl.ds(at + 6 * col, 5)].astype(F32)
            parts.append(v.reshape(10, 8, LANES))
        return jnp.concatenate(parts, axis=1)

    for row in (1, 0, 2):
        for block in range(nx):
            if row != 1:
                for col in range(2):
                    at = (row * nx + block) * 12 + 6 * col
                    landed(r0.at[pl.ds(at, 5)], z0_r.at[(row // 2) * 8 + block * 2 + col])
            scale, shift = norm[block]
            act0[row, :, :, block * LANES : (block + 1) * LANES] = activate(
                frames_of(row, block), scale, shift
            )

    @pl.when(z == 0)
    def _():
        act0[0] = jnp.zeros(act0.shape[1:], BF)

    @pl.when(z == nz - 1)
    def _():
        act0[2] = jnp.zeros(act0.shape[1:], BF)

    @pl.when(c == 0)
    def _():
        act0[:, 0:2] = jnp.zeros((3, 2, *act0.shape[2:]), BF)

    loads[0].wait()
    y = jnp.zeros((half * 16, 3 * LANES), F32)
    for dt in range(3):
        for di in range(3):
            y = y + dot(flat(act0[di, dt : dt + half]), taps(w0, dt, di))
    mixed = column_sum(y.reshape(half, 16, 3 * LANES))
    rest = frames_of(1, x)[2:10]
    value = (rest + mixed + vectors[6].reshape(1, 1, LANES)).astype(BF)
    plane_src[1] = packed_sums(flat(value.astype(F32)), x)
    plane_start(1)
    middle[...] = value

    low, high = lax.rem(z - half * c + nz, nz), lax.rem(z - half * c - half + nz, nz)
    low_near = jnp.minimum(low, nz - low) <= jnp.minimum(high, nz - high)

    boundary = (z == half - 1) | (z == half)

    def spread(act, case):
        to_c = z // half if case == 0 else 1 - z // half
        slot = z - half * to_c + 1
        for turn in range(half + 1):
            j = jnp.where(low_near, half - turn, turn)
            to_z = lax.rem(half * c + j, nz)
            source = jnp.maximum(j - 1, 0)
            tiles = 2 if 0 < turn < half else 1
            fr = 0 if 0 < turn < half else jnp.where(j == 0, 1, 0)
            at = (x * 10 + slot) * 2 + fr
            copy = remote(
                middle.at[pl.ds(source, tiles)],
                x1.at[pl.ds(at, tiles)],
                a_s.at[2 * turn + case],
                a_r.at[slot],
                {"seq": to_z, "ch": x, "col": to_c},
            )
            act(copy, source, tiles, at, (to_z == z) & (to_c == c))

    def a_start(copy, source, tiles, at, itself):
        @pl.when(jnp.logical_not(itself))
        def _():
            copy.start()

    def a_keep(copy, source, tiles, at, itself):
        @pl.when(itself)
        def _():
            x1[pl.ds(at, tiles)] = middle[pl.ds(source, tiles)]

    def a_sent(copy, source, tiles, at, itself):
        @pl.when(jnp.logical_not(itself))
        def _():
            copy.wait_send()

    spread(a_start, 0)

    @pl.when(boundary)
    def _():
        spread(a_start, 1)
        spread(a_keep, 1)

    @pl.when(z // half == c)
    def _():
        spread(a_keep, 0)

    first = 1 - c
    previous_c = lax.rem(z - 1 + nz, nz) // half
    whole_own = (previous_c == c) & (z // half == c)

    def row_over_ch(slot):
        tiles = pl.ds((x * 10 + slot) * 2, 2)
        for dx in (2, 1, 3):
            remote(
                x1.at[tiles], x1.at[tiles], x1_s, x1_r.at[x], peer(0, dx, c)
            ).start()

    @pl.when(whole_own)
    def _():
        row_over_ch(z - half * c + 1)

    line_start(1)

    for turn in range(9):
        slot = first + jnp.where(c == 0, turn, 8 - turn)
        mine = half * c - 1 + slot == z
        at = (x * 10 + slot) * 2
        lost_old = mine & (previous_c == c)
        lost_new = mine & (z // half == c)

        @pl.when(jnp.logical_not(lost_old | lost_new))
        def _():
            landed(x1.at[pl.ds(at, 2)], a_r.at[slot])

        @pl.when(lost_old ^ lost_new)
        def _():
            landed(x1.at[pl.ds(at, 1)], a_r.at[slot])

        @pl.when(jnp.logical_not(mine & whole_own))
        def _():
            row_over_ch(slot)

    norm = affine(line_total(1), samples, params, 1, nx)
    for block in range(nx):
        @pl.when(block != x)
        def _():
            landed(x1.at[pl.ds((block * 10 + first) * 2, 18)], x1_r.at[block])

        scale, shift = norm[block]
        v = x1[block * 20 : (block + 1) * 20].astype(F32).reshape(10, 2, 16, LANES)
        v = activate(v, scale, shift)
        for fr in range(2):
            act1[fr, :, :, block * LANES : (block + 1) * LANES] = v[:, fr]

    zero_row1 = jnp.zeros((2, 16, nx * LANES), BF)

    @pl.when(c == 0)
    def _():
        act1[:, 0] = zero_row1

    @pl.when(c == 1)
    def _():
        act1[:, 9] = zero_row1

    @pl.when(z == 0)
    def _():
        act1[0] = jnp.zeros(act1.shape[1:], BF)

    loads[1].wait()
    shared = jnp.zeros((half * 16, 3 * LANES), F32)
    apart = jnp.zeros((2 * half * 16, 3 * LANES), F32)
    for di in range(3):
        rows = act1[:, di : di + half]
        shared = shared + dot(flat(rows[0]), taps(w1, 0, di))
        shared = shared + dot(flat(rows[1]), taps(w1, 2, di))
    for di in range(3):
        apart = apart + dot(flat(act1[:, di : di + half]), taps(w1, 1, di))
    y = apart.reshape(2, half, 16, 3 * LANES) + shared.reshape(1, half, 16, 3 * LANES)
    mixed = column_sum(y.reshape(2 * half, 16, 3 * LANES))
    value = (mixed + vectors[7].reshape(1, 1, LANES)).astype(BF)
    plane_src[2] = packed_sums(flat(value.astype(F32)), x)
    plane_start(2)
    value = value.reshape(2, half, 16, LANES)
    for fr in range(2):
        for row in range(half):
            hidden[row * 2 + fr] = value[fr, row]

    edge_at = pl.ds((2 * half - 2) * (1 - c), 2)
    edge_slot = pl.ds(18 * c, 2)
    def x2_block(block, own_frames):
        return pl.ds((block * 2 + own_frames) * 20 + 2, 2 * half)

    def history(part):
        return x2.at[pl.ds(x * 40 + 2 + part * half, half)]

    for part in range(2):
        remote(
            hidden.at[pl.ds(part * half, half)], history(part), x2_s, h2_r.at[part], peer(1, 0, c)
        ).start()
    for dx in (2, 1, 3):
        remote(hidden, x2.at[x2_block(x, 1)], x2_s, x2_r.at[nx + x], peer(0, dx, c)).start()
    for dz in (1, 0):
        for dx in (2, 1, 3, 0):
            slot = pl.ds((x * 2 + 1 - dz) * 20 + 18 * c, 2)
            remote(
                hidden.at[edge_at], x2.at[slot], e2_s, e2_r.at[(1 - dz) * nx + x], peer(dz, dx, 1 - c)
            ).start()
    x2[pl.ds((x * 2 + 1) * 20 + 2, 2 * half)] = hidden[...]
    line_start(2)
    for part in range(2):
        landed(history(part), h2_r.at[part])
        for dx in (2, 1, 3):
            remote(history(part), history(part), x2_s, x2_r.at[x], peer(0, dx, c)).start()
    norm = affine(line_total(2), 2.0 * samples, params, 2, nx)

    for own_frames in (1, 0):
        for block in range(nx):
            sem = own_frames * nx + block
            at = (block * 2 + own_frames) * 20

            @pl.when(block != x)
            def _():
                landed(x2.at[x2_block(block, own_frames)], x2_r.at[sem])

            landed(x2.at[pl.ds(at + 18 * (1 - c), 2)], e2_r.at[sem])
            scale, shift = norm[block]
            v = x2[at : at + 20].astype(F32).reshape(10, 2, 16, LANES)
            v = activate(v, scale, shift)
            for fr in range(2):
                act2[2 * own_frames + fr, :, :, block * LANES : (block + 1) * LANES] = v[:, fr]

    zero_row2 = jnp.zeros((4, 16, nx * LANES), BF)

    @pl.when(c == 0)
    def _():
        act2[:, 0] = zero_row2

    @pl.when(c == 1)
    def _():
        act2[:, 9] = zero_row2

    @pl.when(z == 0)
    def _():
        act2[0:2] = jnp.zeros((2, *act2.shape[1:]), BF)

    loads[2].wait()
    y = jnp.zeros((2 * half * 16, 3 * LANES), F32)
    for dt in range(3):
        for di in range(3):
            y = y + dot(flat(act2[dt : dt + 2, di : di + half]), taps(w2, dt, di))
    mixed = column_sum(y.reshape(2 * half, 16, 3 * LANES)).reshape(2, half, 16, LANES)
    doubled = x1[pl.ds(x * 20 + 2, 2 * half)].astype(F32).reshape(half, 2, 16, LANES)[:, 1]
    final = doubled[None] + mixed + vectors[8].reshape(1, 1, 1, LANES)

    sides = [
        final[:, :, 8 * side : 8 * side + 8].reshape(2, half // 2, 16, LANES).astype(BF)
        for side in range(2)
    ]

    @pl.when(c == 0)
    def _():
        give[...] = sides[1]
        out[:, pl.ds(0, half // 2)] = sides[0]

    @pl.when(c == 1)
    def _():
        give[...] = sides[0]
        out[:, pl.ds(half // 2, half // 2)] = sides[1]

    last = remote(give, take, o_s, o_r, peer(0, 0, 1 - c))
    last.start()

    @pl.when(z != hub)
    def _():
        landed(hub_in.at[pl.ds(0, 2 * nx)], hub_s)

    @pl.when(z == hub)
    def _():
        landed(hub_in.at[pl.ds(0, 2 * nx - 1)], plane_s.at[0])
        landed(hub_in.at[pl.ds(0, nz - 1)], line_s.at[0])

    for stage in (1, 2):
        landed(plane_in.at[pl.ds(8 * stage, 2 * nx - 1)], plane_s.at[stage])
        landed(line_in.at[pl.ds(stage * nz, nz - 1)], line_s.at[stage])
    landed(params.at[pl.ds(0, nx - 1)], par_s)
    landed(r0.at[pl.ds(0, 5 * (2 * nx - 1))], x0_s)
    landed(r0.at[pl.ds(0, 5 * 4 * nx)], z0_s)
    spread(a_sent, 0)

    @pl.when(boundary)
    def _():
        spread(a_sent, 1)

    landed(x1.at[pl.ds(0, 3 * 3 * 6)], x1_s)
    landed(x2.at[pl.ds(0, 2 * half * (2 * nx - 1))], x2_s)
    landed(x2.at[pl.ds(0, 2 * 2 * nx)], e2_s)
    last.wait()

    @pl.when(c == 0)
    def _():
        out[:, pl.ds(half // 2, half // 2)] = take[...]

    @pl.when(c == 1)
    def _():
        out[:, pl.ds(0, half // 2)] = take[...]


def body(nz, nx, *args):
    latent = args[0]
    frames = latent.shape[0]
    half = nz // 2
    channels = nx * LANES
    operands = [latent.reshape(frames // 2, 16, LANES)]
    for a in args[1:]:
        operands.append(a.reshape((1, LANES) if a.ndim == 1 else (27, channels, LANES)))
    weight = pltpu.VMEM((27, channels, LANES), BF)
    dma = pltpu.SemaphoreType.DMA
    result = pl.pallas_call(
        functools.partial(kernel, nz, nx),
        out_shape=jax.ShapeDtypeStruct((2, half, 16, LANES), BF),
        in_specs=[pl.BlockSpec(memory_space=pl.ANY)] * len(operands),
        out_specs=pl.BlockSpec(memory_space=pltpu.VMEM),
        scratch_shapes=[
            pltpu.VMEM((frames // 2, 16, LANES), BF),
            pltpu.VMEM((9, 1, LANES), F32),
            weight,
            weight,
            weight,
            pltpu.VMEM((nx, 8, LANES), F32),
            pltpu.VMEM((3 * nx * 2 * 6, 16, LANES), BF),
            pltpu.VMEM((nx * 10 * 2, 16, LANES), BF),
            pltpu.VMEM((nx * 2 * 10 * 2, 16, LANES), BF),
            pltpu.VMEM((3, half + 2, 16, channels), BF),
            pltpu.VMEM((2, half + 2, 16, channels), BF),
            pltpu.VMEM((4, half + 2, 16, channels), BF),
            pltpu.VMEM((half, 16, LANES), BF),
            pltpu.VMEM((2 * half, 16, LANES), BF),
            pltpu.VMEM((2, half // 2, 16, LANES), BF),
            pltpu.VMEM((2, half // 2, 16, LANES), BF),
            pltpu.VMEM((3, 1, LANES), F32),
            pltpu.VMEM((3 * 8, 1, LANES), F32),
            pltpu.VMEM((3, 1, LANES), F32),
            pltpu.VMEM((3 * nz, 1, LANES), F32),
            pltpu.VMEM((nz * nx * 2, 1, LANES), F32),
            pltpu.VMEM((1, 1, LANES), F32),
            dma((10,)),
            dma((3,)),
            dma,
            dma,
            dma,
            dma,
            dma((3,)),
            dma((3,)),
            dma((3,)),
            dma((3,)),
            dma,
            dma((2 * nx,)),
            dma,
            dma((4 * nx,)),
            dma((2 * half + 2,)),
            dma((10,)),
            dma,
            dma((nx,)),
            dma,
            dma((2 * nx,)),
            dma((2,)),
            dma,
            dma((2 * nx,)),
            dma,
            dma,
        ],
        compiler_params=pltpu.CompilerParams(collective_id=0, has_side_effects=True, vmem_limit_bytes=50 * 2**20),
    )(*[pltpu.with_memory_space_constraint(a, pltpu.HBM) for a in operands])
    return result.reshape(2, nz, 8, LANES)


def solution(mesh):
    nz, nx = mesh.shape["seq"], mesh.shape["ch"]
    in_specs = (
        P("grp", "seq", "col", "ch"),
        *(P("ch"), P("ch"), P(None, None, None, None, "ch"), P("ch")) * 3,
    )
    out_specs = P(("grp", "seq"), None, "col", "ch")
    return jax.shard_map(
        functools.partial(body, nz, nx),
        mesh=mesh,
        in_specs=in_specs,
        out_specs=out_specs,
        check_vma=False,
    )
```

```python
import functools

import jax
import jax.numpy as jnp
from jax import lax
from jax.experimental import pallas as pl
from jax.experimental.pallas import tpu as pltpu
from jax.sharding import PartitionSpec as P

MESH = pl.DeviceIdType.MESH
GROUP = 16
LANES = 128
EPS = 0.01
BF = jnp.bfloat16
F32 = jnp.float32


def lane_ids():
    return lax.broadcasted_iota(jnp.int32, (8, LANES), 1)


def row_ids():
    return lax.broadcasted_iota(jnp.int32, (8, LANES), 0)


def group_total(v):
    lane = lane_ids()
    step = GROUP // 2
    while step:
        from_below = pltpu.roll(v, step, 1)
        from_above = pltpu.roll(v, LANES - step, 1)
        v = v + jnp.where((lane & step) != 0, from_below, from_above)
        step //= 2
    return v


def packed_sums(values, x):
    total = jnp.sum(values, axis=0, keepdims=True)
    square = jnp.sum(values * values, axis=0, keepdims=True)
    total = group_total(jnp.broadcast_to(total, (8, LANES)))
    square = group_total(jnp.broadcast_to(square, (8, LANES)))
    slot = lane_ids() & 7
    row = jnp.where(slot == 2 * x, total, jnp.where(slot == 2 * x + 1, square, 0.0))
    return row[0:1]


def affine(row, samples, params, which, nx):
    spread_rows = jnp.broadcast_to(row, (8, LANES))
    picked = jnp.where((lane_ids() & (GROUP - 1)) == row_ids(), spread_rows, 0.0)
    sums = group_total(picked) * (1.0 / samples)
    out = []
    for block in range(nx):
        mean = sums[2 * block : 2 * block + 1]
        square = sums[2 * block + 1 : 2 * block + 2]
        inverse = 1.0 / jnp.sqrt(square - mean * mean + EPS)
        gain = params[block, 2 * which : 2 * which + 1]
        bias = params[block, 2 * which + 1 : 2 * which + 2]
        scale = inverse * gain
        out.append((scale, bias - mean * scale))
    return out


def activate(values, scale, shift):
    u = values * scale.reshape((1,) * (values.ndim - 1) + (LANES,)) + shift.reshape(
        (1,) * (values.ndim - 1) + (LANES,)
    )
    half = 0.5 * u
    return (half + half * jnp.tanh(half)).astype(BF)


def column_sum(y):
    n, cols = y.shape[0], y.shape[1]
    left, mid, right = (y[:, :, i * LANES : (i + 1) * LANES] for i in range(3))
    col = lax.broadcasted_iota(jnp.int32, (n, cols, LANES), 1)
    left = jnp.where(col == 0, 0.0, pltpu.roll(left, 1, 1))
    right = jnp.where(col == cols - 1, 0.0, pltpu.roll(right, cols - 1, 1))
    return left + mid + right


def taps(weight, dt, di, blocks):
    base = dt * 9 + di * 3
    rows = [pl.ds(pl.multiple_of(block * LANES, LANES), LANES) for block in blocks]
    return jnp.concatenate(
        [jnp.concatenate([weight[base + dj, r] for r in rows], axis=0) for dj in range(3)], axis=1
    )


def dot(a, b):
    return jnp.dot(a, b, preferred_element_type=F32)


def flat(v):
    return v.reshape(-1, v.shape[-1])


def kernel(
    nz,
    nx,
    lat_hbm,
    g0,
    b0,
    w0_hbm,
    c0,
    g1,
    b1,
    w1_hbm,
    c1,
    g2,
    b2,
    w2_hbm,
    c2,
    out,
    lat,
    vectors,
    w0,
    w1,
    w2,
    params,
    r0,
    x1,
    x2,
    act0,
    act1,
    act2,
    scales,
    middle,
    hidden,
    give,
    take,
    plane_src,
    plane_in,
    line_src,
    line_in,
    hub_in,
    total_row,
    i_sem,
    w_sem,
    par_s,
    par_r,
    hub_s,
    hub_r,
    plane_s,
    plane_r,
    line_s,
    line_r,
    x0_s,
    x0_r,
    z0_s,
    z0_r,
    a_s,
    a_r,
    x1_s,
    x1_r,
    x2_s,
    x2_r,
    h2_r,
    e2_s,
    e2_r,
    o_s,
    o_r,
):
    z = lax.axis_index("seq")
    x = lax.axis_index("ch")
    c = lax.axis_index("col")
    half = nz // 2
    samples = float(nz * nz * 16 * GROUP)

    def peer(dz, dx, col):
        return {"seq": lax.rem(z + dz + nz, nz), "ch": lax.rem(x + dx, nx), "col": col}

    def remote(src, dst, s_sem, r_sem, to):
        return pltpu.make_async_remote_copy(
            src_ref=src,
            dst_ref=dst,
            send_sem=s_sem,
            recv_sem=r_sem,
            device_id=to,
            device_id_type=MESH,
        )

    def landed(ref, sem):
        pltpu.make_async_copy(ref, ref, sem).wait()

    inputs = [pltpu.make_async_copy(lat_hbm, lat, i_sem.at[9])]
    for i, ref in enumerate((g0, b0, g1, b1, g2, b2, c0, c1, c2)):
        inputs.append(pltpu.make_async_copy(ref, vectors.at[i], i_sem.at[i]))
    loads = [
        pltpu.make_async_copy(a, b, w_sem.at[i])
        for i, (a, b) in enumerate(((w0_hbm, w0), (w1_hbm, w1), (w2_hbm, w2)))
    ]
    for copy in inputs:
        copy.start()

    hub = 1
    barrier = pltpu.get_barrier_semaphore()

    def greet(dz, dx, col):
        pl.semaphore_signal(barrier, inc=1, device_id=peer(dz, dx, col), device_id_type=MESH)

    greet(1, 0, c)
    greet(nz - 1, 0, c)
    for dx in range(nx):
        greet(0, dx, 1 - c)
        if dx:
            greet(0, dx, c)

    @pl.when(z == hub)
    def _():
        def greet_all(dz, carry):
            for dx in range(nx):
                greet(dz, dx, 1 - c)
                if dx:
                    greet(dz, dx, c)
            return carry

        lax.fori_loop(1, nz, greet_all, 0)

        def greet_line(dz, carry):
            greet(dz, 0, c)
            return carry

        lax.fori_loop(2, nz - 1, greet_line, 0)

    near = (z == hub + 1) | (z == hub - 1)
    awaited = 2 * nx + 1 + jnp.where(z == hub, 0, jnp.where(near, 2 * nx - 1, 2 * nx))

    for copy in inputs:
        copy.wait()
    for load in loads:
        load.start()
    for i in range(6):
        params[x, i : i + 1, :] = vectors[i]
    own = lat[...].astype(F32)
    plane_src[0] = packed_sums(flat(own), x)
    own_at = ((nx + x) * 2 + c) * 6
    r0[pl.ds(own_at + 1 - c, 5)] = lat[pl.ds(3 * c, 5)]

    pl.semaphore_wait(barrier, awaited)

    def hub_start():
        place = (z * nx + x) * 2 + c

        @pl.when(z != hub)
        def _():
            for dx in (2, 1, 3, 0):
                for col in (c, 1 - c):
                    remote(
                        plane_src.at[0],
                        hub_in.at[place],
                        hub_s,
                        hub_r,
                        {"seq": hub, "ch": lax.rem(x + dx, nx), "col": col},
                    ).start()

        @pl.when(z == hub)
        def _():
            hub_in[place] = plane_src[0]
            for dx in (2, 1, 3, 0):
                for col in (c, 1 - c):
                    if dx == 0 and col is c:
                        continue
                    remote(
                        plane_src.at[0],
                        hub_in.at[place],
                        plane_s.at[0],
                        hub_r,
                        {"seq": hub, "ch": lax.rem(x + dx, nx), "col": col},
                    ).start()

    def hub_run():
        @pl.when(z == hub)
        def _():
            landed(hub_in.at[pl.ds(0, nz * nx * 2 - 1)], hub_r)
            total_row[0] = jnp.sum(hub_in[...], axis=0)

            def far_first(k, carry):
                step = (k + 1) // 2
                dz = half + step * (2 * lax.rem(k, 2) - 1)
                remote(
                    total_row.at[0], total_row.at[0], line_s.at[0], line_r.at[0], peer(dz, 0, c)
                ).start()
                return carry

            lax.fori_loop(0, nz - 1, far_first, 0)

    def hub_total():
        @pl.when(z != hub)
        def _():
            landed(total_row.at[0], line_r.at[0])

        return total_row[0]

    def plane_start(stage):
        place = 8 * stage + 2 * x + c
        plane_in[place] = plane_src[stage]
        for dx in range(nx):
            for other in (0, 1):
                if dx == 0 and other == 0:
                    continue
                remote(
                    plane_src.at[stage],
                    plane_in.at[place],
                    plane_s.at[stage],
                    plane_r.at[stage],
                    peer(0, dx, c if other == 0 else 1 - c),
                ).start()

    def line_start(stage):
        landed(plane_in.at[pl.ds(8 * stage, 2 * nx - 1)], plane_r.at[stage])
        row = jnp.sum(plane_in[8 * stage : 8 * stage + 2 * nx], axis=0)
        line_src[stage] = row
        line_in[stage * nz + z] = row
        order = sorted(range(1, nz), key=lambda dz: -min(dz, nz - dz))
        for dz in order:
            remote(
                line_src.at[stage],
                line_in.at[stage * nz + z],
                line_s.at[stage],
                line_r.at[stage],
                peer(dz, 0, c),
            ).start()

    def line_total(stage):
        landed(line_in.at[pl.ds(stage * nz, nz - 1)], line_r.at[stage])
        return jnp.sum(line_in[stage * nz : (stage + 1) * nz], axis=0)

    hub_start()
    for dx in range(1, nx):
        remote(params.at[x], params.at[x], par_s, par_r, peer(0, dx, c)).start()

    for dx in (2, 1, 3, 0):
        for other in (0, 1):
            if dx == 0 and other == 0:
                continue
            to_col = c if other == 0 else 1 - c
            remote(
                lat.at[pl.ds(3 * to_col, 5)],
                r0.at[pl.ds(own_at + 1 - to_col, 5)],
                x0_s,
                x0_r.at[x * 2 + c],
                peer(0, dx, to_col),
            ).start()

    @pl.when(c == 0)
    def _():
        for i in range(2 * nx):
            r0[nx * 12 + 6 * i] = jnp.zeros((16, LANES), BF)

    for block in range(nx):
        x1[pl.ds((block * 10 + 9 * c) * 2, 2)] = jnp.zeros((2, 16, LANES), BF)
    for block in range(2 * nx):
        x2[pl.ds((block * 10 + 9 * c) * 2, 2)] = jnp.zeros((2, 16, LANES), BF)

    for dx in (0, 1, 3, 2):
        for other in (0, 1):
            from_x = lax.rem(x + dx, nx)
            from_c = c if other == 0 else 1 - c
            at = (from_x * 2 + from_c) * 6
            if not (dx == 0 and other == 0):
                landed(r0.at[pl.ds(nx * 12 + at + 1 - c, 5)], x0_r.at[from_x * 2 + from_c])
            for row, dz in ((0, 1), (2, nz - 1)):
                remote(
                    r0.at[pl.ds(nx * 12 + at, 5)],
                    r0.at[pl.ds(row * nx * 12 + at, 5)],
                    z0_s,
                    z0_r.at[(row // 2) * 8 + from_x * 2 + from_c],
                    peer(dz, 0, c),
                ).start()

    hub_run()
    landed(params.at[pl.ds(0, nx - 1)], par_r)
    norm = affine(hub_total(), samples, params, 0, nx)

    def frames_of(row, block):
        at = (row * nx + block) * 12
        parts = []
        for col in range(2):
            v = r0[pl.ds(at + 6 * col, 5)].astype(F32)
            parts.append(v.reshape(10, 8, LANES))
        return jnp.concatenate(parts, axis=1)

    for row in (0, 2):
        for block in range(nx):
            for col in range(2):
                at = (row * nx + block) * 12 + 6 * col
                landed(r0.at[pl.ds(at, 5)], z0_r.at[(row // 2) * 8 + block * 2 + col])
    loads[0].wait()

    def inside(condition):
        return jnp.where(condition, 1.0, 0.0).astype(F32)

    in_row = (inside(z > 0), 1.0, inside(z < nz - 1))
    in_core = (inside(c > 0), inside(c < 1))
    in_time = inside(z > 0)

    y = jnp.zeros((half * 16, 3 * LANES), F32)
    for pair in range(nx // 2):
        for k in range(2):
            scale, shift = norm[2 * pair + k]
            lanes = slice(k * LANES, (k + 1) * LANES)
            for row in range(3):
                v = frames_of(row, 2 * pair + k)
                keep = in_row[row] * in_core[0]
                act0[pair, row, 0:2, :, lanes] = activate(v[0:2], scale * keep, shift * keep)
                keep = in_row[row]
                act0[pair, row, 2:, :, lanes] = activate(v[2:], scale * keep, shift * keep)
        for di in range(3):
            for dt in range(3):
                y = y + dot(
                    flat(act0[pair, di, dt : dt + half]), taps(w0, dt, di, (2 * pair, 2 * pair + 1))
                )
    mixed = column_sum(y.reshape(half, 16, 3 * LANES))
    rest = frames_of(1, x)[2:10]
    value = (rest + mixed + vectors[6].reshape(1, 1, LANES)).astype(BF)
    plane_src[1] = packed_sums(flat(value.astype(F32)), x)
    plane_start(1)
    middle[...] = value

    low, high = lax.rem(z - half * c + nz, nz), lax.rem(z - half * c - half + nz, nz)
    low_near = jnp.minimum(low, nz - low) <= jnp.minimum(high, nz - high)

    boundary = (z == half - 1) | (z == half)

    def spread(act, case):
        to_c = z // half if case == 0 else 1 - z // half
        slot = z - half * to_c + 1
        for turn in range(half + 1):
            j = jnp.where(low_near, half - turn, turn)
            to_z = lax.rem(half * c + j, nz)
            source = jnp.maximum(j - 1, 0)
            tiles = 2 if 0 < turn < half else 1
            fr = 0 if 0 < turn < half else jnp.where(j == 0, 1, 0)
            at = (x * 10 + slot) * 2 + fr
            copy = remote(
                middle.at[pl.ds(source, tiles)],
                x1.at[pl.ds(at, tiles)],
                a_s.at[2 * turn + case],
                a_r.at[slot],
                {"seq": to_z, "ch": x, "col": to_c},
            )
            act(copy, source, tiles, at, (to_z == z) & (to_c == c))

    def a_start(copy, source, tiles, at, itself):
        @pl.when(jnp.logical_not(itself))
        def _():
            copy.start()

    def a_keep(copy, source, tiles, at, itself):
        @pl.when(itself)
        def _():
            x1[pl.ds(at, tiles)] = middle[pl.ds(source, tiles)]

    def a_sent(copy, source, tiles, at, itself):
        @pl.when(jnp.logical_not(itself))
        def _():
            copy.wait_send()

    spread(a_start, 0)

    @pl.when(boundary)
    def _():
        spread(a_start, 1)
        spread(a_keep, 1)

    @pl.when(z // half == c)
    def _():
        spread(a_keep, 0)

    first = 1 - c
    previous_c = lax.rem(z - 1 + nz, nz) // half
    whole_own = (previous_c == c) & (z // half == c)

    def row_over_ch(slot):
        tiles = pl.ds((x * 10 + slot) * 2, 2)
        for dx in (2, 1, 3):
            remote(
                x1.at[tiles], x1.at[tiles], x1_s, x1_r.at[x], peer(0, dx, c)
            ).start()

    @pl.when(whole_own)
    def _():
        row_over_ch(z - half * c + 1)

    line_start(1)

    for turn in range(9):
        slot = first + jnp.where(c == 0, turn, 8 - turn)
        mine = half * c - 1 + slot == z
        at = (x * 10 + slot) * 2
        lost_old = mine & (previous_c == c)
        lost_new = mine & (z // half == c)

        @pl.when(jnp.logical_not(lost_old | lost_new))
        def _():
            landed(x1.at[pl.ds(at, 2)], a_r.at[slot])

        @pl.when(lost_old ^ lost_new)
        def _():
            landed(x1.at[pl.ds(at, 1)], a_r.at[slot])

        @pl.when(jnp.logical_not(mine & whole_own))
        def _():
            row_over_ch(slot)

    norm = affine(line_total(1), samples, params, 1, nx)
    for block in range(nx):
        scales[2 * block] = norm[block][0]
        scales[2 * block + 1] = norm[block][1]
    loads[1].wait()
    bands = ((0, 1, in_core[0]), (1, half + 1, 1.0), (half + 1, half + 2, in_core[1]))

    shared = jnp.zeros((half * 16, 3 * LANES), F32)
    apart = jnp.zeros((2 * half * 16, 3 * LANES), F32)
    for pair, steps in enumerate(((0, 1), (3, 2))):
        blocks = [lax.rem(x + step, nx) for step in steps]
        for block, step in zip(blocks, steps):
            if step:
                landed(x1.at[pl.ds((block * 10 + first) * 2, 18)], x1_r.at[block])
        for k, block in enumerate(blocks):
            scale, shift = scales[2 * block], scales[2 * block + 1]
            v = x1[pl.ds(block * 20, 20)].astype(F32).reshape(half + 2, 2, 16, LANES)
            for fr in range(2):
                for lo, hi, keep in bands:
                    keep = keep * in_time if fr == 0 else keep
                    act1[pair, fr, lo:hi, :, k * LANES : (k + 1) * LANES] = activate(
                        v[lo:hi, fr], scale * keep, shift * keep
                    )
        for di in range(3):
            rows = act1[pair, :, di : di + half]
            shared = shared + dot(flat(rows[0]), taps(w1, 0, di, blocks))
            shared = shared + dot(flat(rows[1]), taps(w1, 2, di, blocks))
            apart = apart + dot(flat(rows), taps(w1, 1, di, blocks))
    y = apart.reshape(2, half, 16, 3 * LANES) + shared.reshape(1, half, 16, 3 * LANES)
    mixed = column_sum(y.reshape(2 * half, 16, 3 * LANES))
    value = (mixed + vectors[7].reshape(1, 1, LANES)).astype(BF)
    plane_src[2] = packed_sums(flat(value.astype(F32)), x)
    plane_start(2)
    value = value.reshape(2, half, 16, LANES)
    for fr in range(2):
        for row in range(half):
            hidden[row * 2 + fr] = value[fr, row]

    edge_at = pl.ds((2 * half - 2) * (1 - c), 2)
    edge_slot = pl.ds(18 * c, 2)
    def x2_block(block, own_frames):
        return pl.ds((block * 2 + own_frames) * 20 + 2, 2 * half)

    def history(part):
        return x2.at[pl.ds(x * 40 + 2 + part * half, half)]

    for part in range(2):
        remote(
            hidden.at[pl.ds(part * half, half)], history(part), x2_s, h2_r.at[part], peer(1, 0, c)
        ).start()
    for dx in (2, 1, 3):
        remote(hidden, x2.at[x2_block(x, 1)], x2_s, x2_r.at[nx + x], peer(0, dx, c)).start()
    for dz in (1, 0):
        for dx in (2, 1, 3, 0):
            slot = pl.ds((x * 2 + 1 - dz) * 20 + 18 * c, 2)
            remote(
                hidden.at[edge_at], x2.at[slot], e2_s, e2_r.at[(1 - dz) * nx + x], peer(dz, dx, 1 - c)
            ).start()
    x2[pl.ds((x * 2 + 1) * 20 + 2, 2 * half)] = hidden[...]
    line_start(2)
    for part in range(2):
        landed(history(part), h2_r.at[part])
        for dx in (2, 1, 3):
            remote(history(part), history(part), x2_s, x2_r.at[x], peer(0, dx, c)).start()
    norm = affine(line_total(2), 2.0 * samples, params, 2, nx)

    for own_frames in (1, 0):
        for block in range(nx):
            sem = own_frames * nx + block
            at = (block * 2 + own_frames) * 20

            @pl.when(block != x)
            def _():
                landed(x2.at[x2_block(block, own_frames)], x2_r.at[sem])

            landed(x2.at[pl.ds(at + 18 * (1 - c), 2)], e2_r.at[sem])
    loads[2].wait()

    y = jnp.zeros((2 * half * 16, 3 * LANES), F32)
    for pair in range(nx // 2):
        for k in range(2):
            block = 2 * pair + k
            scale, shift = norm[block]
            for own_frames in range(2):
                at = (block * 2 + own_frames) * 20
                v = x2[at : at + 20].astype(F32).reshape(half + 2, 2, 16, LANES)
                for lo, hi, keep in bands:
                    keep = keep if own_frames else keep * in_time
                    part = activate(v[lo:hi], scale * keep, shift * keep)
                    for fr in range(2):
                        act2[pair, 2 * own_frames + fr, lo:hi, :, k * LANES : (k + 1) * LANES] = part[:, fr]
        for di in range(3):
            for dt in range(3):
                y = y + dot(
                    flat(act2[pair, dt : dt + 2, di : di + half]),
                    taps(w2, dt, di, (2 * pair, 2 * pair + 1)),
                )
    mixed = column_sum(y.reshape(2 * half, 16, 3 * LANES)).reshape(2, half, 16, LANES)
    doubled = x1[pl.ds(x * 20 + 2, 2 * half)].astype(F32).reshape(half, 2, 16, LANES)[:, 1]
    final = doubled[None] + mixed + vectors[8].reshape(1, 1, 1, LANES)

    sides = [
        final[:, :, 8 * side : 8 * side + 8].reshape(2, half // 2, 16, LANES).astype(BF)
        for side in range(2)
    ]

    @pl.when(c == 0)
    def _():
        give[...] = sides[1]
        out[:, pl.ds(0, half // 2)] = sides[0]

    @pl.when(c == 1)
    def _():
        give[...] = sides[0]
        out[:, pl.ds(half // 2, half // 2)] = sides[1]

    last = remote(give, take, o_s, o_r, peer(0, 0, 1 - c))
    last.start()

    @pl.when(z != hub)
    def _():
        landed(hub_in.at[pl.ds(0, 2 * nx)], hub_s)

    @pl.when(z == hub)
    def _():
        landed(hub_in.at[pl.ds(0, 2 * nx - 1)], plane_s.at[0])
        landed(hub_in.at[pl.ds(0, nz - 1)], line_s.at[0])

    for stage in (1, 2):
        landed(plane_in.at[pl.ds(8 * stage, 2 * nx - 1)], plane_s.at[stage])
        landed(line_in.at[pl.ds(stage * nz, nz - 1)], line_s.at[stage])
    landed(params.at[pl.ds(0, nx - 1)], par_s)
    landed(r0.at[pl.ds(0, 5 * (2 * nx - 1))], x0_s)
    landed(r0.at[pl.ds(0, 5 * 4 * nx)], z0_s)
    spread(a_sent, 0)

    @pl.when(boundary)
    def _():
        spread(a_sent, 1)

    landed(x1.at[pl.ds(0, 3 * 3 * 6)], x1_s)
    landed(x2.at[pl.ds(0, 2 * half * (2 * nx - 1))], x2_s)
    landed(x2.at[pl.ds(0, 2 * 2 * nx)], e2_s)
    last.wait()

    @pl.when(c == 0)
    def _():
        out[:, pl.ds(half // 2, half // 2)] = take[...]

    @pl.when(c == 1)
    def _():
        out[:, pl.ds(0, half // 2)] = take[...]


def body(nz, nx, *args):
    latent = args[0]
    frames = latent.shape[0]
    half = nz // 2
    channels = nx * LANES
    operands = [latent.reshape(frames // 2, 16, LANES)]
    for a in args[1:]:
        operands.append(a.reshape((1, LANES) if a.ndim == 1 else (27, channels, LANES)))
    weight = pltpu.VMEM((27, channels, LANES), BF)
    dma = pltpu.SemaphoreType.DMA
    result = pl.pallas_call(
        functools.partial(kernel, nz, nx),
        out_shape=jax.ShapeDtypeStruct((2, half, 16, LANES), BF),
        in_specs=[pl.BlockSpec(memory_space=pl.ANY)] * len(operands),
        out_specs=pl.BlockSpec(memory_space=pltpu.VMEM),
        scratch_shapes=[
            pltpu.VMEM((frames // 2, 16, LANES), BF),
            pltpu.VMEM((9, 1, LANES), F32),
            weight,
            weight,
            weight,
            pltpu.VMEM((nx, 8, LANES), F32),
            pltpu.VMEM((3 * nx * 2 * 6, 16, LANES), BF),
            pltpu.VMEM((nx * 10 * 2, 16, LANES), BF),
            pltpu.VMEM((nx * 2 * 10 * 2, 16, LANES), BF),
            pltpu.VMEM((nx // 2, 3, half + 2, 16, 2 * LANES), BF),
            pltpu.VMEM((nx // 2, 2, half + 2, 16, 2 * LANES), BF),
            pltpu.VMEM((nx // 2, 4, half + 2, 16, 2 * LANES), BF),
            pltpu.VMEM((2 * nx, 1, LANES), F32),
            pltpu.VMEM((half, 16, LANES), BF),
            pltpu.VMEM((2 * half, 16, LANES), BF),
            pltpu.VMEM((2, half // 2, 16, LANES), BF),
            pltpu.VMEM((2, half // 2, 16, LANES), BF),
            pltpu.VMEM((3, 1, LANES), F32),
            pltpu.VMEM((3 * 8, 1, LANES), F32),
            pltpu.VMEM((3, 1, LANES), F32),
            pltpu.VMEM((3 * nz, 1, LANES), F32),
            pltpu.VMEM((nz * nx * 2, 1, LANES), F32),
            pltpu.VMEM((1, 1, LANES), F32),
            dma((10,)),
            dma((3,)),
            dma,
            dma,
            dma,
            dma,
            dma((3,)),
            dma((3,)),
            dma((3,)),
            dma((3,)),
            dma,
            dma((2 * nx,)),
            dma,
            dma((4 * nx,)),
            dma((2 * half + 2,)),
            dma((10,)),
            dma,
            dma((nx,)),
            dma,
            dma((2 * nx,)),
            dma((2,)),
            dma,
            dma((2 * nx,)),
            dma,
            dma,
        ],
        compiler_params=pltpu.CompilerParams(collective_id=0, has_side_effects=True, vmem_limit_bytes=50 * 2**20),
    )(*[pltpu.with_memory_space_constraint(a, pltpu.HBM) for a in operands])
    return result.reshape(2, nz, 8, LANES)


def solution(mesh):
    nz, nx = mesh.shape["seq"], mesh.shape["ch"]
    in_specs = (
        P("grp", "seq", "col", "ch"),
        *(P("ch"), P("ch"), P(None, None, None, None, "ch"), P("ch")) * 3,
    )
    out_specs = P(("grp", "seq"), None, "col", "ch")
    return jax.shard_map(
        functools.partial(body, nz, nx),
        mesh=mesh,
        in_specs=in_specs,
        out_specs=out_specs,
        check_vma=False,
    )
```

```python
import functools

import jax
import jax.numpy as jnp
from jax import lax
from jax.experimental import pallas as pl
from jax.experimental.pallas import tpu as pltpu
from jax.sharding import PartitionSpec as P

MESH = pl.DeviceIdType.MESH
GROUP = 16
LANES = 128
EPS = 0.01
BF = jnp.bfloat16
F32 = jnp.float32


def lane_ids():
    return lax.broadcasted_iota(jnp.int32, (8, LANES), 1)


def row_ids():
    return lax.broadcasted_iota(jnp.int32, (8, LANES), 0)


def group_total(v):
    lane = lane_ids()
    step = GROUP // 2
    while step:
        from_below = pltpu.roll(v, step, 1)
        from_above = pltpu.roll(v, LANES - step, 1)
        v = v + jnp.where((lane & step) != 0, from_below, from_above)
        step //= 2
    return v


def packed_sums(values, x):
    total = jnp.sum(values, axis=0, keepdims=True)
    square = jnp.sum(values * values, axis=0, keepdims=True)
    total = group_total(jnp.broadcast_to(total, (8, LANES)))
    square = group_total(jnp.broadcast_to(square, (8, LANES)))
    slot = lane_ids() & 7
    row = jnp.where(slot == 2 * x, total, jnp.where(slot == 2 * x + 1, square, 0.0))
    return row[0:1]


def affine(row, samples, params, which, nx):
    spread_rows = jnp.broadcast_to(row, (8, LANES))
    picked = jnp.where((lane_ids() & (GROUP - 1)) == row_ids(), spread_rows, 0.0)
    sums = group_total(picked) * (1.0 / samples)
    out = []
    for block in range(nx):
        mean = sums[2 * block : 2 * block + 1]
        square = sums[2 * block + 1 : 2 * block + 2]
        inverse = 1.0 / jnp.sqrt(square - mean * mean + EPS)
        gain = params[block, 2 * which : 2 * which + 1]
        bias = params[block, 2 * which + 1 : 2 * which + 2]
        scale = inverse * gain
        out.append((scale, bias - mean * scale))
    return out


def activate(values, scale, shift):
    u = values * scale.reshape((1,) * (values.ndim - 1) + (LANES,)) + shift.reshape(
        (1,) * (values.ndim - 1) + (LANES,)
    )
    half = 0.5 * u
    return (half + half * jnp.tanh(half)).astype(BF)


def column_sum(y):
    n, cols = y.shape[0], y.shape[1]
    left, mid, right = (y[:, :, i * LANES : (i + 1) * LANES] for i in range(3))
    col = lax.broadcasted_iota(jnp.int32, (n, cols, LANES), 1)
    left = jnp.where(col == 0, 0.0, pltpu.roll(left, 1, 1))
    right = jnp.where(col == cols - 1, 0.0, pltpu.roll(right, cols - 1, 1))
    return left + mid + right


def taps(weight, dt, di, blocks):
    base = dt * 9 + di * 3
    rows = [pl.ds(pl.multiple_of(block * LANES, LANES), LANES) for block in blocks]
    return jnp.concatenate(
        [jnp.concatenate([weight[base + dj, r] for r in rows], axis=0) for dj in range(3)], axis=1
    )


def dot(a, b):
    return jnp.dot(a, b, preferred_element_type=F32)


def flat(v):
    return v.reshape(-1, v.shape[-1])


def kernel(
    nz,
    nx,
    lat_hbm,
    g0,
    b0,
    w0_hbm,
    c0,
    g1,
    b1,
    w1_hbm,
    c1,
    g2,
    b2,
    w2_hbm,
    c2,
    out,
    lat,
    vectors,
    w0,
    w1,
    w2,
    params,
    r0,
    x1,
    x2,
    act0,
    act1,
    act2,
    scales,
    middle,
    hidden,
    give,
    take,
    plane_src,
    plane_in,
    line_src,
    line_in,
    hub_in,
    total_row,
    far_in,
    i_sem,
    w_sem,
    par_s,
    par_r,
    hub_s,
    hub_r,
    plane_s,
    plane_r,
    line_s,
    line_r,
    far_s,
    far_r,
    x0_s,
    x0_r,
    z0_s,
    z0_r,
    a_s,
    a_r,
    x1_s,
    x1_r,
    x2_s,
    x2_r,
    h2_r,
    e2_s,
    e2_r,
    o_s,
    o_r,
):
    z = lax.axis_index("seq")
    x = lax.axis_index("ch")
    c = lax.axis_index("col")
    half = nz // 2
    samples = float(nz * nz * 16 * GROUP)

    def peer(dz, dx, col):
        return {"seq": lax.rem(z + dz + nz, nz), "ch": lax.rem(x + dx, nx), "col": col}

    def remote(src, dst, s_sem, r_sem, to):
        return pltpu.make_async_remote_copy(
            src_ref=src,
            dst_ref=dst,
            send_sem=s_sem,
            recv_sem=r_sem,
            device_id=to,
            device_id_type=MESH,
        )

    def landed(ref, sem):
        pltpu.make_async_copy(ref, ref, sem).wait()

    inputs = [pltpu.make_async_copy(lat_hbm, lat, i_sem.at[9])]
    for i, ref in enumerate((g0, b0, g1, b1, g2, b2, c0, c1, c2)):
        inputs.append(pltpu.make_async_copy(ref, vectors.at[i], i_sem.at[i]))
    loads = [
        pltpu.make_async_copy(a, b, w_sem.at[i])
        for i, (a, b) in enumerate(((w0_hbm, w0), (w1_hbm, w1), (w2_hbm, w2)))
    ]
    for copy in inputs:
        copy.start()

    hub = 1
    barrier = pltpu.get_barrier_semaphore()

    def greet(dz, dx, col):
        pl.semaphore_signal(barrier, inc=1, device_id=peer(dz, dx, col), device_id_type=MESH)

    @pl.when(z < nz - 1)
    def _():
        greet(1, 0, c)

    @pl.when(z > 0)
    def _():
        greet(nz - 1, 0, c)

    for dx in range(nx):
        greet(0, dx, 1 - c)
        if dx:
            greet(0, dx, c)

    @pl.when(z == hub)
    def _():
        def greet_all(dz, carry):
            for dx in range(nx):
                greet(dz, dx, 1 - c)
                if dx:
                    greet(dz, dx, c)
            return carry

        lax.fori_loop(1, nz, greet_all, 0)

        def greet_line(dz, carry):
            greet(dz, 0, c)
            return carry

        lax.fori_loop(2, nz - 1, greet_line, 0)

    near = (z == hub + 1) | (z == hub - 1)
    awaited = 2 * nx + 1 + jnp.where(z == hub, 0, jnp.where(near, 2 * nx - 1, 2 * nx))
    awaited = awaited - jnp.where((z == 0) | (z == nz - 1), 1, 0)

    for copy in inputs:
        copy.wait()
    for load in loads:
        load.start()
    for i in range(6):
        params[x, i : i + 1, :] = vectors[i]
    own = lat[...].astype(F32)
    plane_src[0] = packed_sums(flat(own), x)
    own_at = ((nx + x) * 2 + c) * 6
    r0[pl.ds(own_at + 1 - c, 5)] = lat[pl.ds(3 * c, 5)]

    pl.semaphore_wait(barrier, awaited)

    def hub_start():
        place = (z * nx + x) * 2 + c

        @pl.when(z != hub)
        def _():
            for dx in (2, 1, 3, 0):
                for col in (c, 1 - c):
                    remote(
                        plane_src.at[0],
                        hub_in.at[place],
                        hub_s,
                        hub_r,
                        {"seq": hub, "ch": lax.rem(x + dx, nx), "col": col},
                    ).start()

        @pl.when(z == hub)
        def _():
            hub_in[place] = plane_src[0]
            for dx in (2, 1, 3, 0):
                for col in (c, 1 - c):
                    if dx == 0 and col is c:
                        continue
                    remote(
                        plane_src.at[0],
                        hub_in.at[place],
                        plane_s.at[0],
                        hub_r,
                        {"seq": hub, "ch": lax.rem(x + dx, nx), "col": col},
                    ).start()

    def hub_run():
        @pl.when(z == hub)
        def _():
            landed(hub_in.at[pl.ds(0, nz * nx * 2 - 1)], hub_r)
            total_row[0] = jnp.sum(hub_in[...], axis=0)

            def far_first(k, carry):
                step = (k + 1) // 2
                dz = half + step * (2 * lax.rem(k, 2) - 1)
                remote(
                    total_row.at[0], total_row.at[0], line_s.at[0], line_r.at[0], peer(dz, 0, c)
                ).start()
                return carry

            lax.fori_loop(0, nz - 1, far_first, 0)

    def hub_total():
        @pl.when(z != hub)
        def _():
            landed(total_row.at[0], line_r.at[0])

        return total_row[0]

    def plane_start(stage):
        place = 8 * stage + 2 * x + c
        plane_in[place] = plane_src[stage]
        for dx in range(nx):
            for other in (0, 1):
                if dx == 0 and other == 0:
                    continue
                remote(
                    plane_src.at[stage],
                    plane_in.at[place],
                    plane_s.at[stage],
                    plane_r.at[stage],
                    peer(0, dx, c if other == 0 else 1 - c),
                ).start()

    across = (half, half - 1, half + 1)

    def far_start():
        for k, dz in enumerate(across):
            for dx in (2, 1, 3, 0):
                for col in (c, 1 - c):
                    remote(
                        plane_src.at[2],
                        far_in.at[8 * k + 2 * x + c],
                        far_s,
                        far_r,
                        peer(dz, dx, col),
                    ).start()

    def line_steps(stage):
        steps = sorted(range(1, nz), key=lambda dz: -min(dz, nz - dz))
        return [dz for dz in steps if stage == 1 or dz not in across]

    def line_start(stage):
        landed(plane_in.at[pl.ds(8 * stage, 2 * nx - 1)], plane_r.at[stage])
        row = jnp.sum(plane_in[8 * stage : 8 * stage + 2 * nx], axis=0)
        line_src[stage] = row
        line_in[stage * nz] = row
        for dz in line_steps(stage):
            remote(
                line_src.at[stage],
                line_in.at[stage * nz + nz - dz],
                line_s.at[stage],
                line_r.at[stage],
                peer(dz, 0, c),
            ).start()

    def line_total(stage):
        landed(line_in.at[pl.ds(stage * nz, len(line_steps(stage)))], line_r.at[stage])
        if stage == 1:
            return jnp.sum(line_in[nz : 2 * nz], axis=0)
        landed(far_in, far_r)
        total = jnp.sum(line_in[stage * nz : stage * nz + half - 1], axis=0)
        total = total + jnp.sum(line_in[stage * nz + half + 2 : (stage + 1) * nz], axis=0)
        return total + jnp.sum(far_in[...], axis=0)

    hub_start()
    for dx in range(1, nx):
        remote(params.at[x], params.at[x], par_s, par_r, peer(0, dx, c)).start()

    for dx in (2, 1, 3, 0):
        for other in (0, 1):
            if dx == 0 and other == 0:
                continue
            to_col = c if other == 0 else 1 - c
            remote(
                lat.at[pl.ds(3 * to_col, 5)],
                r0.at[pl.ds(own_at + 1 - to_col, 5)],
                x0_s,
                x0_r.at[x * 2 + c],
                peer(0, dx, to_col),
            ).start()

    @pl.when(c == 0)
    def _():
        for i in range(2 * nx):
            r0[nx * 12 + 6 * i] = jnp.zeros((16, LANES), BF)

    for row, outside in ((0, z == 0), (2, z == nz - 1)):
        @pl.when(outside)
        def _():
            r0[row * nx * 12 : (row + 1) * nx * 12] = jnp.zeros((nx * 12, 16, LANES), BF)

    @pl.when(z == 0)
    def _():
        for block in range(nx):
            x2[block * 40 : block * 40 + 20] = jnp.zeros((20, 16, LANES), BF)

    for block in range(nx):
        x1[pl.ds((block * 10 + 9 * c) * 2, 2)] = jnp.zeros((2, 16, LANES), BF)
    for block in range(2 * nx):
        x2[pl.ds((block * 10 + 9 * c) * 2, 2)] = jnp.zeros((2, 16, LANES), BF)

    for dx in (0, 1, 3, 2):
        for other in (0, 1):
            from_x = lax.rem(x + dx, nx)
            from_c = c if other == 0 else 1 - c
            at = (from_x * 2 + from_c) * 6
            if not (dx == 0 and other == 0):
                landed(r0.at[pl.ds(nx * 12 + at + 1 - c, 5)], x0_r.at[from_x * 2 + from_c])
            for row, dz, there in ((0, 1, z < nz - 1), (2, nz - 1, z > 0)):
                @pl.when(there)
                def _():
                    remote(
                        r0.at[pl.ds(nx * 12 + at, 5)],
                        r0.at[pl.ds(row * nx * 12 + at, 5)],
                        z0_s.at[row // 2],
                        z0_r.at[(row // 2) * 8 + from_x * 2 + from_c],
                        peer(dz, 0, c),
                    ).start()


    hub_run()
    landed(params.at[pl.ds(0, nx - 1)], par_r)
    norm = affine(hub_total(), samples, params, 0, nx)

    def frames_of(row, block):
        at = (row * nx + block) * 12
        parts = []
        for col in range(2):
            v = r0[pl.ds(at + 6 * col, 5)].astype(F32)
            parts.append(v.reshape(10, 8, LANES))
        return jnp.concatenate(parts, axis=1)

    for row, there in ((0, z > 0), (2, z < nz - 1)):
        @pl.when(there)
        def _():
            for block in range(nx):
                for col in range(2):
                    at = (row * nx + block) * 12 + 6 * col
                    landed(r0.at[pl.ds(at, 5)], z0_r.at[(row // 2) * 8 + block * 2 + col])

    loads[0].wait()

    def inside(condition):
        return jnp.where(condition, 1.0, 0.0).astype(F32)

    in_row = (inside(z > 0), 1.0, inside(z < nz - 1))
    in_core = (inside(c > 0), inside(c < 1))
    in_time = inside(z > 0)

    y = jnp.zeros((half * 16, 3 * LANES), F32)
    for pair in range(nx // 2):
        for k in range(2):
            scale, shift = norm[2 * pair + k]
            lanes = slice(k * LANES, (k + 1) * LANES)
            for row in range(3):
                v = frames_of(row, 2 * pair + k)
                keep = in_row[row] * in_core[0]
                act0[pair, row, 0:2, :, lanes] = activate(v[0:2], scale * keep, shift * keep)
                keep = in_row[row]
                act0[pair, row, 2:, :, lanes] = activate(v[2:], scale * keep, shift * keep)
        for di in range(3):
            for dt in range(3):
                y = y + dot(
                    flat(act0[pair, di, dt : dt + half]), taps(w0, dt, di, (2 * pair, 2 * pair + 1))
                )
    mixed = column_sum(y.reshape(half, 16, 3 * LANES))
    rest = frames_of(1, x)[2:10]
    value = (rest + mixed + vectors[6].reshape(1, 1, LANES)).astype(BF)
    plane_src[1] = packed_sums(flat(value.astype(F32)), x)
    plane_start(1)
    middle[...] = value

    low, high = lax.rem(z - half * c + nz, nz), lax.rem(z - half * c - half + nz, nz)
    low_near = jnp.minimum(low, nz - low) <= jnp.minimum(high, nz - high)

    boundary = (z == half - 1) | (z == half)

    def spread(act, case):
        to_c = z // half if case == 0 else 1 - z // half
        slot = z - half * to_c + 1
        for turn in range(half + 1):
            j = jnp.where(low_near, half - turn, turn)
            to_z = lax.rem(half * c + j, nz)
            source = jnp.maximum(j - 1, 0)
            tiles = 2 if 0 < turn < half else 1
            fr = 0 if 0 < turn < half else jnp.where(j == 0, 1, 0)
            at = (x * 10 + slot) * 2 + fr
            copy = remote(
                middle.at[pl.ds(source, tiles)],
                x1.at[pl.ds(at, tiles)],
                a_s.at[2 * turn + case],
                a_r.at[slot],
                {"seq": to_z, "ch": x, "col": to_c},
            )
            act(copy, source, tiles, at, (to_z == z) & (to_c == c))

    def a_start(copy, source, tiles, at, itself):
        @pl.when(jnp.logical_not(itself))
        def _():
            copy.start()

    def a_keep(copy, source, tiles, at, itself):
        @pl.when(itself)
        def _():
            x1[pl.ds(at, tiles)] = middle[pl.ds(source, tiles)]

    def a_sent(copy, source, tiles, at, itself):
        @pl.when(jnp.logical_not(itself))
        def _():
            copy.wait_send()

    spread(a_start, 0)

    @pl.when(boundary)
    def _():
        spread(a_start, 1)
        spread(a_keep, 1)

    @pl.when(z // half == c)
    def _():
        spread(a_keep, 0)

    first = 1 - c
    previous_c = lax.rem(z - 1 + nz, nz) // half
    whole_own = (previous_c == c) & (z // half == c)

    def row_over_ch(slot):
        tiles = pl.ds((x * 10 + slot) * 2, 2)
        for dx in (2, 1, 3):
            remote(
                x1.at[tiles], x1.at[tiles], x1_s, x1_r.at[x], peer(0, dx, c)
            ).start()

    @pl.when(whole_own)
    def _():
        row_over_ch(z - half * c + 1)

    line_start(1)

    for turn in range(9):
        slot = first + jnp.where(c == 0, turn, 8 - turn)
        mine = half * c - 1 + slot == z
        at = (x * 10 + slot) * 2
        lost_old = mine & (previous_c == c)
        lost_new = mine & (z // half == c)

        @pl.when(jnp.logical_not(lost_old | lost_new))
        def _():
            landed(x1.at[pl.ds(at, 2)], a_r.at[slot])

        @pl.when(lost_old ^ lost_new)
        def _():
            landed(x1.at[pl.ds(at, 1)], a_r.at[slot])

        @pl.when(jnp.logical_not(mine & whole_own))
        def _():
            row_over_ch(slot)

    norm = affine(line_total(1), samples, params, 1, nx)
    for block in range(nx):
        scales[2 * block] = norm[block][0]
        scales[2 * block + 1] = norm[block][1]
    loads[1].wait()
    bands = ((0, 1, in_core[0]), (1, half + 1, 1.0), (half + 1, half + 2, in_core[1]))

    shared = jnp.zeros((half * 16, 3 * LANES), F32)
    apart = jnp.zeros((2 * half * 16, 3 * LANES), F32)
    for pair, steps in enumerate(((0, 1), (3, 2))):
        blocks = [lax.rem(x + step, nx) for step in steps]
        for block, step in zip(blocks, steps):
            if step:
                landed(x1.at[pl.ds((block * 10 + first) * 2, 18)], x1_r.at[block])
        for k, block in enumerate(blocks):
            scale, shift = scales[2 * block], scales[2 * block + 1]
            v = x1[pl.ds(block * 20, 20)].astype(F32).reshape(half + 2, 2, 16, LANES)
            for fr in range(2):
                for lo, hi, keep in bands:
                    keep = keep * in_time if fr == 0 else keep
                    act1[pair, fr, lo:hi, :, k * LANES : (k + 1) * LANES] = activate(
                        v[lo:hi, fr], scale * keep, shift * keep
                    )
        for di in range(3):
            rows = act1[pair, :, di : di + half]
            shared = shared + dot(flat(rows[0]), taps(w1, 0, di, blocks))
            shared = shared + dot(flat(rows[1]), taps(w1, 2, di, blocks))
            apart = apart + dot(flat(rows), taps(w1, 1, di, blocks))
    y = apart.reshape(2, half, 16, 3 * LANES) + shared.reshape(1, half, 16, 3 * LANES)
    mixed = column_sum(y.reshape(2 * half, 16, 3 * LANES))
    value = (mixed + vectors[7].reshape(1, 1, LANES)).astype(BF)
    plane_src[2] = packed_sums(flat(value.astype(F32)), x)
    plane_start(2)
    far_start()
    value = value.reshape(2, half, 16, LANES)
    for fr in range(2):
        for row in range(half):
            hidden[row * 2 + fr] = value[fr, row]

    edge_at = pl.ds((2 * half - 2) * (1 - c), 2)
    edge_slot = pl.ds(18 * c, 2)
    def x2_block(block, own_frames):
        return pl.ds((block * 2 + own_frames) * 20 + 2, 2 * half)

    def history(part):
        return x2.at[pl.ds(x * 40 + 2 + part * half, half)]

    has_next, has_past = z < nz - 1, z > 0

    def edges(dz):
        for dx in (2, 1, 3, 0):
            slot = pl.ds((x * 2 + 1 - dz) * 20 + 18 * c, 2)
            remote(
                hidden.at[edge_at],
                x2.at[slot],
                e2_s.at[dz],
                e2_r.at[(1 - dz) * nx + x],
                peer(dz, dx, 1 - c),
            ).start()

    @pl.when(has_next)
    def _():
        for part in range(2):
            remote(
                hidden.at[pl.ds(part * half, half)],
                history(part),
                x2_s.at[1],
                h2_r.at[part],
                peer(1, 0, c),
            ).start()

    for dx in (2, 1, 3):
        remote(
            hidden, x2.at[x2_block(x, 1)], x2_s.at[0], x2_r.at[nx + x], peer(0, dx, c)
        ).start()
    edges(0)

    @pl.when(has_next)
    def _():
        edges(1)

    x2[pl.ds((x * 2 + 1) * 20 + 2, 2 * half)] = hidden[...]
    line_start(2)
    @pl.when(has_past)
    def _():
        for part in range(2):
            landed(history(part), h2_r.at[part])
            for dx in (2, 1, 3):
                remote(
                    history(part), history(part), x2_s.at[2], x2_r.at[x], peer(0, dx, c)
                ).start()

    norm = affine(line_total(2), 2.0 * samples, params, 2, nx)

    def arrived(own_frames):
        for block in range(nx):
            sem = own_frames * nx + block
            at = (block * 2 + own_frames) * 20

            @pl.when(block != x)
            def _():
                landed(x2.at[x2_block(block, own_frames)], x2_r.at[sem])

            landed(x2.at[pl.ds(at + 18 * (1 - c), 2)], e2_r.at[sem])

    arrived(1)

    @pl.when(has_past)
    def _():
        arrived(0)

    loads[2].wait()

    y = jnp.zeros((2 * half * 16, 3 * LANES), F32)
    for pair in range(nx // 2):
        for k in range(2):
            block = 2 * pair + k
            scale, shift = norm[block]
            for own_frames in range(2):
                at = (block * 2 + own_frames) * 20
                v = x2[at : at + 20].astype(F32).reshape(half + 2, 2, 16, LANES)
                for lo, hi, keep in bands:
                    keep = keep if own_frames else keep * in_time
                    part = activate(v[lo:hi], scale * keep, shift * keep)
                    for fr in range(2):
                        act2[pair, 2 * own_frames + fr, lo:hi, :, k * LANES : (k + 1) * LANES] = part[:, fr]
        for di in range(3):
            for dt in range(3):
                y = y + dot(
                    flat(act2[pair, dt : dt + 2, di : di + half]),
                    taps(w2, dt, di, (2 * pair, 2 * pair + 1)),
                )
    mixed = column_sum(y.reshape(2 * half, 16, 3 * LANES)).reshape(2, half, 16, LANES)
    doubled = x1[pl.ds(x * 20 + 2, 2 * half)].astype(F32).reshape(half, 2, 16, LANES)[:, 1]
    final = doubled[None] + mixed + vectors[8].reshape(1, 1, 1, LANES)

    sides = [
        final[:, :, 8 * side : 8 * side + 8].reshape(2, half // 2, 16, LANES).astype(BF)
        for side in range(2)
    ]

    @pl.when(c == 0)
    def _():
        give[...] = sides[1]
        out[:, pl.ds(0, half // 2)] = sides[0]

    @pl.when(c == 1)
    def _():
        give[...] = sides[0]
        out[:, pl.ds(half // 2, half // 2)] = sides[1]

    last = remote(give, take, o_s, o_r, peer(0, 0, 1 - c))
    last.start()

    @pl.when(z != hub)
    def _():
        landed(hub_in.at[pl.ds(0, 2 * nx)], hub_s)

    @pl.when(z == hub)
    def _():
        landed(hub_in.at[pl.ds(0, 2 * nx - 1)], plane_s.at[0])
        landed(hub_in.at[pl.ds(0, nz - 1)], line_s.at[0])

    for stage in (1, 2):
        landed(plane_in.at[pl.ds(8 * stage, 2 * nx - 1)], plane_s.at[stage])
        landed(line_in.at[pl.ds(stage * nz, len(line_steps(stage)))], line_s.at[stage])

    landed(far_in, far_s)
    landed(params.at[pl.ds(0, nx - 1)], par_s)
    landed(r0.at[pl.ds(0, 5 * (2 * nx - 1))], x0_s)
    for row, there in ((0, z < nz - 1), (1, z > 0)):
        @pl.when(there)
        def _():
            landed(r0.at[pl.ds(0, 5 * 2 * nx)], z0_s.at[row])

    spread(a_sent, 0)

    @pl.when(boundary)
    def _():
        spread(a_sent, 1)

    landed(x1.at[pl.ds(0, 3 * 3 * 6)], x1_s)
    landed(x2.at[pl.ds(0, 2 * half * (nx - 1))], x2_s.at[0])
    landed(x2.at[pl.ds(0, 2 * nx)], e2_s.at[0])

    @pl.when(has_next)
    def _():
        landed(x2.at[pl.ds(0, 2 * half)], x2_s.at[1])
        landed(x2.at[pl.ds(0, 2 * nx)], e2_s.at[1])

    @pl.when(has_past)
    def _():
        landed(x2.at[pl.ds(0, 2 * half * (nx - 1))], x2_s.at[2])

    last.wait()

    @pl.when(c == 0)
    def _():
        out[:, pl.ds(half // 2, half // 2)] = take[...]

    @pl.when(c == 1)
    def _():
        out[:, pl.ds(0, half // 2)] = take[...]


def body(nz, nx, *args):
    latent = args[0]
    frames = latent.shape[0]
    half = nz // 2
    channels = nx * LANES
    operands = [latent.reshape(frames // 2, 16, LANES)]
    for a in args[1:]:
        operands.append(a.reshape((1, LANES) if a.ndim == 1 else (27, channels, LANES)))
    weight = pltpu.VMEM((27, channels, LANES), BF)
    dma = pltpu.SemaphoreType.DMA
    result = pl.pallas_call(
        functools.partial(kernel, nz, nx),
        out_shape=jax.ShapeDtypeStruct((2, half, 16, LANES), BF),
        in_specs=[pl.BlockSpec(memory_space=pl.ANY)] * len(operands),
        out_specs=pl.BlockSpec(memory_space=pltpu.VMEM),
        scratch_shapes=[
            pltpu.VMEM((frames // 2, 16, LANES), BF),
            pltpu.VMEM((9, 1, LANES), F32),
            weight,
            weight,
            weight,
            pltpu.VMEM((nx, 8, LANES), F32),
            pltpu.VMEM((3 * nx * 2 * 6, 16, LANES), BF),
            pltpu.VMEM((nx * 10 * 2, 16, LANES), BF),
            pltpu.VMEM((nx * 2 * 10 * 2, 16, LANES), BF),
            pltpu.VMEM((nx // 2, 3, half + 2, 16, 2 * LANES), BF),
            pltpu.VMEM((nx // 2, 2, half + 2, 16, 2 * LANES), BF),
            pltpu.VMEM((nx // 2, 4, half + 2, 16, 2 * LANES), BF),
            pltpu.VMEM((2 * nx, 1, LANES), F32),
            pltpu.VMEM((half, 16, LANES), BF),
            pltpu.VMEM((2 * half, 16, LANES), BF),
            pltpu.VMEM((2, half // 2, 16, LANES), BF),
            pltpu.VMEM((2, half // 2, 16, LANES), BF),
            pltpu.VMEM((3, 1, LANES), F32),
            pltpu.VMEM((3 * 8, 1, LANES), F32),
            pltpu.VMEM((3, 1, LANES), F32),
            pltpu.VMEM((3 * nz, 1, LANES), F32),
            pltpu.VMEM((nz * nx * 2, 1, LANES), F32),
            pltpu.VMEM((1, 1, LANES), F32),
            pltpu.VMEM((3 * 2 * nx, 1, LANES), F32),
            dma((10,)),
            dma((3,)),
            dma,
            dma,
            dma,
            dma,
            dma((3,)),
            dma((3,)),
            dma((3,)),
            dma((3,)),
            dma,
            dma,
            dma,
            dma((2 * nx,)),
            dma((2,)),
            dma((4 * nx,)),
            dma((2 * half + 2,)),
            dma((10,)),
            dma,
            dma((nx,)),
            dma((3,)),
            dma((2 * nx,)),
            dma((2,)),
            dma((2,)),
            dma((2 * nx,)),
            dma,
            dma,
        ],
        compiler_params=pltpu.CompilerParams(collective_id=0, has_side_effects=True, vmem_limit_bytes=50 * 2**20),
    )(*[pltpu.with_memory_space_constraint(a, pltpu.HBM) for a in operands])
    return result.reshape(2, nz, 8, LANES)


def solution(mesh):
    nz, nx = mesh.shape["seq"], mesh.shape["ch"]
    in_specs = (
        P("grp", "seq", "col", "ch"),
        *(P("ch"), P("ch"), P(None, None, None, None, "ch"), P("ch")) * 3,
    )
    out_specs = P(("grp", "seq"), None, "col", "ch")
    return jax.shard_map(
        functools.partial(body, nz, nx),
        mesh=mesh,
        in_specs=in_specs,
        out_specs=out_specs,
        check_vma=False,
    )
```

```python
import functools

import jax
import jax.numpy as jnp
from jax import lax
from jax.experimental import pallas as pl
from jax.experimental.pallas import tpu as pltpu
from jax.sharding import PartitionSpec as P

MESH = pl.DeviceIdType.MESH
GROUP = 16
LANES = 128
EPS = 0.01
BF = jnp.bfloat16
F32 = jnp.float32


def lane_ids():
    return lax.broadcasted_iota(jnp.int32, (8, LANES), 1)


def row_ids():
    return lax.broadcasted_iota(jnp.int32, (8, LANES), 0)


def group_total(v):
    lane = lane_ids()
    step = GROUP // 2
    while step:
        from_below = pltpu.roll(v, step, 1)
        from_above = pltpu.roll(v, LANES - step, 1)
        v = v + jnp.where((lane & step) != 0, from_below, from_above)
        step //= 2
    return v


def packed_sums(values, x):
    total = jnp.sum(values, axis=0, keepdims=True)
    square = jnp.sum(values * values, axis=0, keepdims=True)
    total = group_total(jnp.broadcast_to(total, (8, LANES)))
    square = group_total(jnp.broadcast_to(square, (8, LANES)))
    slot = lane_ids() & 7
    row = jnp.where(slot == 2 * x, total, jnp.where(slot == 2 * x + 1, square, 0.0))
    return row[0:1]


def affine(row, samples, params, which, nx):
    spread_rows = jnp.broadcast_to(row, (8, LANES))
    picked = jnp.where((lane_ids() & (GROUP - 1)) == row_ids(), spread_rows, 0.0)
    sums = group_total(picked) * (1.0 / samples)
    out = []
    for block in range(nx):
        mean = sums[2 * block : 2 * block + 1]
        square = sums[2 * block + 1 : 2 * block + 2]
        inverse = 1.0 / jnp.sqrt(square - mean * mean + EPS)
        gain = params[block, 2 * which : 2 * which + 1]
        bias = params[block, 2 * which + 1 : 2 * which + 2]
        scale = inverse * gain
        out.append((scale, bias - mean * scale))
    return out


def activate(values, scale, shift):
    u = values * scale.reshape((1,) * (values.ndim - 1) + (LANES,)) + shift.reshape(
        (1,) * (values.ndim - 1) + (LANES,)
    )
    half = 0.5 * u
    return (half + half * jnp.tanh(half)).astype(BF)


def column_sum(y):
    n, cols = y.shape[0], y.shape[1]
    left, mid, right = (y[:, :, i * LANES : (i + 1) * LANES] for i in range(3))
    col = lax.broadcasted_iota(jnp.int32, (n, cols, LANES), 1)
    left = jnp.where(col == 0, 0.0, pltpu.roll(left, 1, 1))
    right = jnp.where(col == cols - 1, 0.0, pltpu.roll(right, cols - 1, 1))
    return left + mid + right


def taps(weight, dt, di, blocks):
    base = dt * 9 + di * 3
    rows = [pl.ds(pl.multiple_of(block * LANES, LANES), LANES) for block in blocks]
    return jnp.concatenate(
        [jnp.concatenate([weight[base + dj, r] for r in rows], axis=0) for dj in range(3)], axis=1
    )


def dot(a, b):
    return jnp.dot(a, b, preferred_element_type=F32)


def flat(v):
    return v.reshape(-1, v.shape[-1])


def kernel(
    nz,
    nx,
    lat_hbm,
    g0,
    b0,
    w0_hbm,
    c0,
    g1,
    b1,
    w1_hbm,
    c1,
    g2,
    b2,
    w2_hbm,
    c2,
    out,
    lat,
    vectors,
    w0,
    w1,
    w2,
    params,
    r0,
    x1,
    x2,
    act0,
    act1,
    act2,
    scales,
    summed,
    middle,
    hidden,
    give,
    take,
    plane_src,
    plane_in,
    line_src,
    line_in,
    hub_in,
    total_row,
    far_in,
    i_sem,
    w_sem,
    par_s,
    par_r,
    hub_s,
    hub_r,
    plane_s,
    plane_r,
    line_s,
    line_r,
    far_s,
    far_r,
    x0_s,
    x0_r,
    z0_s,
    z0_r,
    a_s,
    a_r,
    x1_s,
    x1_r,
    x2_s,
    x2_r,
    h2_r,
    e2_s,
    e2_r,
    o_s,
    o_r,
):
    z = lax.axis_index("seq")
    x = lax.axis_index("ch")
    c = lax.axis_index("col")
    half = nz // 2
    samples = float(nz * nz * 16 * GROUP)

    def peer(dz, dx, col):
        return {"seq": lax.rem(z + dz + nz, nz), "ch": lax.rem(x + dx, nx), "col": col}

    def remote(src, dst, s_sem, r_sem, to):
        return pltpu.make_async_remote_copy(
            src_ref=src,
            dst_ref=dst,
            send_sem=s_sem,
            recv_sem=r_sem,
            device_id=to,
            device_id_type=MESH,
        )

    def landed(ref, sem):
        pltpu.make_async_copy(ref, ref, sem).wait()

    inputs = [pltpu.make_async_copy(lat_hbm, lat, i_sem.at[9])]
    for i, ref in enumerate((g0, b0, g1, b1, g2, b2, c0, c1, c2)):
        inputs.append(pltpu.make_async_copy(ref, vectors.at[i], i_sem.at[i]))
    loads = [
        pltpu.make_async_copy(a, b, w_sem.at[i])
        for i, (a, b) in enumerate(((w0_hbm, w0), (w1_hbm, w1), (w2_hbm, w2)))
    ]
    for copy in inputs:
        copy.start()

    hub = 1
    barrier = pltpu.get_barrier_semaphore()

    def greet(dz, dx, col):
        pl.semaphore_signal(barrier, inc=1, device_id=peer(dz, dx, col), device_id_type=MESH)

    @pl.when(z < nz - 1)
    def _():
        greet(1, 0, c)

    @pl.when(z > 0)
    def _():
        greet(nz - 1, 0, c)

    for dx in range(nx):
        greet(0, dx, 1 - c)
        if dx:
            greet(0, dx, c)

    @pl.when(z == hub)
    def _():
        def greet_all(dz, carry):
            for dx in range(nx):
                greet(dz, dx, 1 - c)
                if dx:
                    greet(dz, dx, c)
            return carry

        lax.fori_loop(1, nz, greet_all, 0)

        def greet_line(dz, carry):
            greet(dz, 0, c)
            return carry

        lax.fori_loop(2, nz - 1, greet_line, 0)

    near = (z == hub + 1) | (z == hub - 1)
    awaited = 2 * nx + 1 + jnp.where(z == hub, 0, jnp.where(near, 2 * nx - 1, 2 * nx))
    awaited = awaited - jnp.where((z == 0) | (z == nz - 1), 1, 0)

    for copy in inputs:
        copy.wait()
    for load in loads:
        load.start()
    for i in range(6):
        params[x, i : i + 1, :] = vectors[i]
    own = lat[...].astype(F32)
    plane_src[0] = packed_sums(flat(own), x)
    own_at = ((nx + x) * 2 + c) * 6
    r0[pl.ds(own_at + 1 - c, 5)] = lat[pl.ds(3 * c, 5)]

    pl.semaphore_wait(barrier, awaited)

    def hub_start():
        place = (z * nx + x) * 2 + c

        @pl.when(z != hub)
        def _():
            for dx in (2, 1, 3, 0):
                for col in (c, 1 - c):
                    remote(
                        plane_src.at[0],
                        hub_in.at[place],
                        hub_s,
                        hub_r,
                        {"seq": hub, "ch": lax.rem(x + dx, nx), "col": col},
                    ).start()

        @pl.when(z == hub)
        def _():
            hub_in[place] = plane_src[0]
            for dx in (2, 1, 3, 0):
                for col in (c, 1 - c):
                    if dx == 0 and col is c:
                        continue
                    remote(
                        plane_src.at[0],
                        hub_in.at[place],
                        plane_s.at[0],
                        hub_r,
                        {"seq": hub, "ch": lax.rem(x + dx, nx), "col": col},
                    ).start()

    def hub_run():
        @pl.when(z == hub)
        def _():
            landed(hub_in.at[pl.ds(0, nz * nx * 2 - 1)], hub_r)
            total_row[0] = jnp.sum(hub_in[...], axis=0)

            def send(dz):
                remote(
                    total_row.at[0], total_row.at[0], line_s.at[0], line_r.at[0], peer(dz, 0, c)
                ).start()

            send(nz - 1)
            send(1)

            def far_first(k, carry):
                step = (k + 1) // 2
                send(half + step * (2 * lax.rem(k, 2) - 1))
                return carry

            lax.fori_loop(0, nz - 3, far_first, 0)

    def hub_total():
        @pl.when(z != hub)
        def _():
            landed(total_row.at[0], line_r.at[0])

        return total_row[0]

    def plane_start(stage):
        place = 8 * stage + 2 * x + c
        plane_in[place] = plane_src[stage]
        for dx in range(nx):
            for other in (0, 1):
                if dx == 0 and other == 0:
                    continue
                remote(
                    plane_src.at[stage],
                    plane_in.at[place],
                    plane_s.at[stage],
                    plane_r.at[stage],
                    peer(0, dx, c if other == 0 else 1 - c),
                ).start()

    across = (half, half - 1, half + 1)

    def far_start():
        for k, dz in enumerate(across):
            for dx in (2, 1, 3, 0):
                for col in (c, 1 - c):
                    remote(
                        plane_src.at[2],
                        far_in.at[8 * k + 2 * x + c],
                        far_s,
                        far_r,
                        peer(dz, dx, col),
                    ).start()

    def line_steps(stage):
        steps = sorted(range(1, nz), key=lambda dz: -min(dz, nz - dz))
        return [dz for dz in steps if stage == 1 or dz not in across]

    def line_start(stage):
        landed(plane_in.at[pl.ds(8 * stage, 2 * nx - 1)], plane_r.at[stage])
        row = jnp.sum(plane_in[8 * stage : 8 * stage + 2 * nx], axis=0)
        line_src[stage] = row
        line_in[stage * nz] = row
        for dz in line_steps(stage):
            remote(
                line_src.at[stage],
                line_in.at[stage * nz + nz - dz],
                line_s.at[stage],
                line_r.at[stage],
                peer(dz, 0, c),
            ).start()

    def line_total(stage):
        landed(line_in.at[pl.ds(stage * nz, len(line_steps(stage)))], line_r.at[stage])
        if stage == 1:
            return jnp.sum(line_in[nz : 2 * nz], axis=0)
        landed(far_in, far_r)
        total = jnp.sum(line_in[stage * nz : stage * nz + half - 1], axis=0)
        total = total + jnp.sum(line_in[stage * nz + half + 2 : (stage + 1) * nz], axis=0)
        return total + jnp.sum(far_in[...], axis=0)

    hub_start()
    for dx in range(1, nx):
        remote(params.at[x], params.at[x], par_s, par_r, peer(0, dx, c)).start()

    for dx in (2, 1, 3, 0):
        for other in (0, 1):
            if dx == 0 and other == 0:
                continue
            to_col = c if other == 0 else 1 - c
            remote(
                lat.at[pl.ds(3 * to_col, 5)],
                r0.at[pl.ds(own_at + 1 - to_col, 5)],
                x0_s,
                x0_r.at[x * 2 + c],
                peer(0, dx, to_col),
            ).start()

    @pl.when(c == 0)
    def _():
        for i in range(2 * nx):
            r0[nx * 12 + 6 * i] = jnp.zeros((16, LANES), BF)

    for row, outside in ((0, z == 0), (2, z == nz - 1)):
        @pl.when(outside)
        def _():
            r0[row * nx * 12 : (row + 1) * nx * 12] = jnp.zeros((nx * 12, 16, LANES), BF)

    @pl.when(z == 0)
    def _():
        for block in range(nx):
            x2[block * 40 : block * 40 + 20] = jnp.zeros((20, 16, LANES), BF)

    for block in range(nx):
        x1[pl.ds((block * 10 + 9 * c) * 2, 2)] = jnp.zeros((2, 16, LANES), BF)
    for block in range(2 * nx):
        x2[pl.ds((block * 10 + 9 * c) * 2, 2)] = jnp.zeros((2, 16, LANES), BF)

    for dx in (0, 1, 3, 2):
        for other in (0, 1):
            from_x = lax.rem(x + dx, nx)
            from_c = c if other == 0 else 1 - c
            at = (from_x * 2 + from_c) * 6
            if not (dx == 0 and other == 0):
                landed(r0.at[pl.ds(nx * 12 + at + 1 - c, 5)], x0_r.at[from_x * 2 + from_c])
            for row, dz, there in ((0, 1, z < nz - 1), (2, nz - 1, z > 0)):
                @pl.when(there)
                def _():
                    remote(
                        r0.at[pl.ds(nx * 12 + at, 5)],
                        r0.at[pl.ds(row * nx * 12 + at, 5)],
                        z0_s.at[row // 2],
                        z0_r.at[(row // 2) * 8 + from_x * 2 + from_c],
                        peer(dz, 0, c),
                    ).start()


    hub_run()
    landed(params.at[pl.ds(0, nx - 1)], par_r)
    norm = affine(hub_total(), samples, params, 0, nx)

    def frames_of(row, block):
        at = (row * nx + block) * 12
        parts = []
        for col in range(2):
            v = r0[pl.ds(at + 6 * col, 5)].astype(F32)
            parts.append(v.reshape(10, 8, LANES))
        return jnp.concatenate(parts, axis=1)

    for row, there in ((0, z > 0), (2, z < nz - 1)):
        @pl.when(there)
        def _():
            for block in range(nx):
                for col in range(2):
                    at = (row * nx + block) * 12 + 6 * col
                    landed(r0.at[pl.ds(at, 5)], z0_r.at[(row // 2) * 8 + block * 2 + col])

    loads[0].wait()

    def inside(condition):
        return jnp.where(condition, 1.0, 0.0).astype(F32)

    in_row = (inside(z > 0), 1.0, inside(z < nz - 1))
    in_core = (inside(c > 0), inside(c < 1))
    in_time = inside(z > 0)

    y = jnp.zeros((half * 16, 3 * LANES), F32)
    for pair in range(nx // 2):
        for k in range(2):
            scale, shift = norm[2 * pair + k]
            lanes = slice(k * LANES, (k + 1) * LANES)
            for row in range(3):
                v = frames_of(row, 2 * pair + k)
                keep = in_row[row] * in_core[0]
                act0[pair, row, 0:2, :, lanes] = activate(v[0:2], scale * keep, shift * keep)
                keep = in_row[row]
                act0[pair, row, 2:, :, lanes] = activate(v[2:], scale * keep, shift * keep)
        for di in range(3):
            for dt in range(3):
                y = y + dot(
                    flat(act0[pair, di, dt : dt + half]), taps(w0, dt, di, (2 * pair, 2 * pair + 1))
                )
    mixed = column_sum(y.reshape(half, 16, 3 * LANES))
    rest = frames_of(1, x)[2:10]
    value = (rest + mixed + vectors[6].reshape(1, 1, LANES)).astype(BF)
    plane_src[1] = packed_sums(flat(value.astype(F32)), x)
    plane_start(1)
    middle[...] = value

    low, high = lax.rem(z - half * c + nz, nz), lax.rem(z - half * c - half + nz, nz)
    low_near = jnp.minimum(low, nz - low) <= jnp.minimum(high, nz - high)

    boundary = (z == half - 1) | (z == half)

    def spread(act, case):
        to_c = z // half if case == 0 else 1 - z // half
        slot = z - half * to_c + 1
        for turn in range(half + 1):
            j = jnp.where(low_near, half - turn, turn)
            to_z = lax.rem(half * c + j, nz)
            source = jnp.maximum(j - 1, 0)
            tiles = 2 if 0 < turn < half else 1
            fr = 0 if 0 < turn < half else jnp.where(j == 0, 1, 0)
            at = (x * 10 + slot) * 2 + fr
            copy = remote(
                middle.at[pl.ds(source, tiles)],
                x1.at[pl.ds(at, tiles)],
                a_s.at[2 * turn + case],
                a_r.at[slot],
                {"seq": to_z, "ch": x, "col": to_c},
            )
            act(copy, source, tiles, at, (to_z == z) & (to_c == c))

    def a_start(copy, source, tiles, at, itself):
        @pl.when(jnp.logical_not(itself))
        def _():
            copy.start()

    def a_keep(copy, source, tiles, at, itself):
        @pl.when(itself)
        def _():
            x1[pl.ds(at, tiles)] = middle[pl.ds(source, tiles)]

    def a_sent(copy, source, tiles, at, itself):
        @pl.when(jnp.logical_not(itself))
        def _():
            copy.wait_send()

    spread(a_start, 0)

    @pl.when(boundary)
    def _():
        spread(a_start, 1)
        spread(a_keep, 1)

    @pl.when(z // half == c)
    def _():
        spread(a_keep, 0)

    first = 1 - c
    previous_c = lax.rem(z - 1 + nz, nz) // half
    whole_own = (previous_c == c) & (z // half == c)

    def row_over_ch(slot):
        tiles = pl.ds((x * 10 + slot) * 2, 2)
        for dx in (2, 1, 3):
            remote(
                x1.at[tiles], x1.at[tiles], x1_s, x1_r.at[x], peer(0, dx, c)
            ).start()

    @pl.when(whole_own)
    def _():
        row_over_ch(z - half * c + 1)

    line_start(1)

    for turn in range(9):
        slot = first + jnp.where(c == 0, turn, 8 - turn)
        mine = half * c - 1 + slot == z
        at = (x * 10 + slot) * 2
        lost_old = mine & (previous_c == c)
        lost_new = mine & (z // half == c)

        @pl.when(jnp.logical_not(lost_old | lost_new))
        def _():
            landed(x1.at[pl.ds(at, 2)], a_r.at[slot])

        @pl.when(lost_old ^ lost_new)
        def _():
            landed(x1.at[pl.ds(at, 1)], a_r.at[slot])

        @pl.when(jnp.logical_not(mine & whole_own))
        def _():
            row_over_ch(slot)

    norm = affine(line_total(1), samples, params, 1, nx)
    for block in range(nx):
        scales[2 * block] = norm[block][0]
        scales[2 * block + 1] = norm[block][1]
    loads[1].wait()
    bands = ((0, 1, in_core[0]), (1, half + 1, 1.0), (half + 1, half + 2, in_core[1]))

    shared = jnp.zeros((half * 16, 3 * LANES), F32)
    apart = jnp.zeros((2 * half * 16, 3 * LANES), F32)
    for pair, steps in enumerate(((0, 1), (3, 2))):
        blocks = [lax.rem(x + step, nx) for step in steps]
        for block, step in zip(blocks, steps):
            if step:
                landed(x1.at[pl.ds((block * 10 + first) * 2, 18)], x1_r.at[block])
        for k, block in enumerate(blocks):
            scale, shift = scales[2 * block], scales[2 * block + 1]
            v = x1[pl.ds(block * 20, 20)].astype(F32).reshape(half + 2, 2, 16, LANES)
            for fr in range(2):
                for lo, hi, keep in bands:
                    keep = keep * in_time if fr == 0 else keep
                    act1[pair, fr, lo:hi, :, k * LANES : (k + 1) * LANES] = activate(
                        v[lo:hi, fr], scale * keep, shift * keep
                    )
        for di in range(3):
            rows = act1[pair, :, di : di + half]
            shared = shared + dot(flat(rows[0]), taps(w1, 0, di, blocks))
            shared = shared + dot(flat(rows[1]), taps(w1, 2, di, blocks))
            apart = apart + dot(flat(rows), taps(w1, 1, di, blocks))
    y = apart.reshape(2, half, 16, 3 * LANES) + shared.reshape(1, half, 16, 3 * LANES)
    mixed = column_sum(y.reshape(2 * half, 16, 3 * LANES))
    value = (mixed + vectors[7].reshape(1, 1, LANES)).astype(BF)
    plane_src[2] = packed_sums(flat(value.astype(F32)), x)
    plane_start(2)
    far_start()
    value = value.reshape(2, half, 16, LANES)
    for fr in range(2):
        for row in range(half):
            hidden[row * 2 + fr] = value[fr, row]

    edge_at = pl.ds((2 * half - 2) * (1 - c), 2)
    edge_slot = pl.ds(18 * c, 2)
    def x2_block(block, own_frames):
        return pl.ds((block * 2 + own_frames) * 20 + 2, 2 * half)

    def history(part):
        return x2.at[pl.ds(x * 40 + 2 + part * half, half)]

    has_next, has_past = z < nz - 1, z > 0

    def edges(dz):
        for dx in (2, 1, 3, 0):
            slot = pl.ds((x * 2 + 1 - dz) * 20 + 18 * c, 2)
            remote(
                hidden.at[edge_at],
                x2.at[slot],
                e2_s.at[dz],
                e2_r.at[(1 - dz) * nx + x],
                peer(dz, dx, 1 - c),
            ).start()

    @pl.when(has_next)
    def _():
        for part in range(2):
            remote(
                hidden.at[pl.ds(part * half, half)],
                history(part),
                x2_s.at[1],
                h2_r.at[part],
                peer(1, 0, c),
            ).start()

    for dx in (2, 1, 3):
        remote(
            hidden, x2.at[x2_block(x, 1)], x2_s.at[0], x2_r.at[nx + x], peer(0, dx, c)
        ).start()
    edges(0)

    @pl.when(has_next)
    def _():
        edges(1)

    x2[pl.ds((x * 2 + 1) * 20 + 2, 2 * half)] = hidden[...]
    line_start(2)
    @pl.when(has_past)
    def _():
        for part in range(2):
            landed(history(part), h2_r.at[part])
            for dx in (2, 1, 3):
                remote(
                    history(part), history(part), x2_s.at[2], x2_r.at[x], peer(0, dx, c)
                ).start()

    norm = affine(line_total(2), 2.0 * samples, params, 2, nx)

    def arrived(own_frames):
        for block in range(nx):
            sem = own_frames * nx + block
            at = (block * 2 + own_frames) * 20

            @pl.when(block != x)
            def _():
                landed(x2.at[x2_block(block, own_frames)], x2_r.at[sem])

            landed(x2.at[pl.ds(at + 18 * (1 - c), 2)], e2_r.at[sem])

    arrived(1)

    @pl.when(has_past)
    def _():
        arrived(0)

    loads[2].wait()

    y = jnp.zeros((2 * half * 16, 3 * LANES), F32)
    for pair in range(nx // 2):
        for k in range(2):
            block = 2 * pair + k
            scale, shift = norm[block]
            for own_frames in range(2):
                at = (block * 2 + own_frames) * 20
                v = x2[at : at + 20].astype(F32).reshape(half + 2, 2, 16, LANES)
                for lo, hi, keep in bands:
                    keep = keep if own_frames else keep * in_time
                    part = activate(v[lo:hi], scale * keep, shift * keep)
                    for fr in range(2):
                        act2[pair, 2 * own_frames + fr, lo:hi, :, k * LANES : (k + 1) * LANES] = part[:, fr]
        for di in range(3):
            for dt in (1, 2):
                y = y + dot(
                    flat(act2[pair, dt : dt + 2, di : di + half]),
                    taps(w2, dt, di, (2 * pair, 2 * pair + 1)),
                )
    summed[...] = y

    @pl.when(has_past)
    def _():
        y = summed[...]
        for pair in range(nx // 2):
            for di in range(3):
                y = y + dot(
                    flat(act2[pair, 0:2, di : di + half]),
                    taps(w2, 0, di, (2 * pair, 2 * pair + 1)),
                )
        summed[...] = y

    y = summed[...]
    mixed = column_sum(y.reshape(2 * half, 16, 3 * LANES)).reshape(2, half, 16, LANES)
    doubled = x1[pl.ds(x * 20 + 2, 2 * half)].astype(F32).reshape(half, 2, 16, LANES)[:, 1]
    final = doubled[None] + mixed + vectors[8].reshape(1, 1, 1, LANES)

    sides = [
        final[:, :, 8 * side : 8 * side + 8].reshape(2, half // 2, 16, LANES).astype(BF)
        for side in range(2)
    ]

    @pl.when(c == 0)
    def _():
        give[...] = sides[1]
        out[:, pl.ds(0, half // 2)] = sides[0]

    @pl.when(c == 1)
    def _():
        give[...] = sides[0]
        out[:, pl.ds(half // 2, half // 2)] = sides[1]

    last = remote(give, take, o_s, o_r, peer(0, 0, 1 - c))
    last.start()

    @pl.when(z != hub)
    def _():
        landed(hub_in.at[pl.ds(0, 2 * nx)], hub_s)

    @pl.when(z == hub)
    def _():
        landed(hub_in.at[pl.ds(0, 2 * nx - 1)], plane_s.at[0])
        landed(hub_in.at[pl.ds(0, nz - 1)], line_s.at[0])

    for stage in (1, 2):
        landed(plane_in.at[pl.ds(8 * stage, 2 * nx - 1)], plane_s.at[stage])
        landed(line_in.at[pl.ds(stage * nz, len(line_steps(stage)))], line_s.at[stage])

    landed(far_in, far_s)
    landed(params.at[pl.ds(0, nx - 1)], par_s)
    landed(r0.at[pl.ds(0, 5 * (2 * nx - 1))], x0_s)
    for row, there in ((0, z < nz - 1), (1, z > 0)):
        @pl.when(there)
        def _():
            landed(r0.at[pl.ds(0, 5 * 2 * nx)], z0_s.at[row])

    spread(a_sent, 0)

    @pl.when(boundary)
    def _():
        spread(a_sent, 1)

    landed(x1.at[pl.ds(0, 3 * 3 * 6)], x1_s)
    landed(x2.at[pl.ds(0, 2 * half * (nx - 1))], x2_s.at[0])
    landed(x2.at[pl.ds(0, 2 * nx)], e2_s.at[0])

    @pl.when(has_next)
    def _():
        landed(x2.at[pl.ds(0, 2 * half)], x2_s.at[1])
        landed(x2.at[pl.ds(0, 2 * nx)], e2_s.at[1])

    @pl.when(has_past)
    def _():
        landed(x2.at[pl.ds(0, 2 * half * (nx - 1))], x2_s.at[2])

    last.wait()

    @pl.when(c == 0)
    def _():
        out[:, pl.ds(half // 2, half // 2)] = take[...]

    @pl.when(c == 1)
    def _():
        out[:, pl.ds(0, half // 2)] = take[...]


def body(nz, nx, *args):
    latent = args[0]
    frames = latent.shape[0]
    half = nz // 2
    channels = nx * LANES
    operands = [latent.reshape(frames // 2, 16, LANES)]
    for a in args[1:]:
        operands.append(a.reshape((1, LANES) if a.ndim == 1 else (27, channels, LANES)))
    weight = pltpu.VMEM((27, channels, LANES), BF)
    dma = pltpu.SemaphoreType.DMA
    result = pl.pallas_call(
        functools.partial(kernel, nz, nx),
        out_shape=jax.ShapeDtypeStruct((2, half, 16, LANES), BF),
        in_specs=[pl.BlockSpec(memory_space=pl.ANY)] * len(operands),
        out_specs=pl.BlockSpec(memory_space=pltpu.VMEM),
        scratch_shapes=[
            pltpu.VMEM((frames // 2, 16, LANES), BF),
            pltpu.VMEM((9, 1, LANES), F32),
            weight,
            weight,
            weight,
            pltpu.VMEM((nx, 8, LANES), F32),
            pltpu.VMEM((3 * nx * 2 * 6, 16, LANES), BF),
            pltpu.VMEM((nx * 10 * 2, 16, LANES), BF),
            pltpu.VMEM((nx * 2 * 10 * 2, 16, LANES), BF),
            pltpu.VMEM((nx // 2, 3, half + 2, 16, 2 * LANES), BF),
            pltpu.VMEM((nx // 2, 2, half + 2, 16, 2 * LANES), BF),
            pltpu.VMEM((nx // 2, 4, half + 2, 16, 2 * LANES), BF),
            pltpu.VMEM((2 * nx, 1, LANES), F32),
            pltpu.VMEM((2 * half * 16, 3 * LANES), F32),
            pltpu.VMEM((half, 16, LANES), BF),
            pltpu.VMEM((2 * half, 16, LANES), BF),
            pltpu.VMEM((2, half // 2, 16, LANES), BF),
            pltpu.VMEM((2, half // 2, 16, LANES), BF),
            pltpu.VMEM((3, 1, LANES), F32),
            pltpu.VMEM((3 * 8, 1, LANES), F32),
            pltpu.VMEM((3, 1, LANES), F32),
            pltpu.VMEM((3 * nz, 1, LANES), F32),
            pltpu.VMEM((nz * nx * 2, 1, LANES), F32),
            pltpu.VMEM((1, 1, LANES), F32),
            pltpu.VMEM((3 * 2 * nx, 1, LANES), F32),
            dma((10,)),
            dma((3,)),
            dma,
            dma,
            dma,
            dma,
            dma((3,)),
            dma((3,)),
            dma((3,)),
            dma((3,)),
            dma,
            dma,
            dma,
            dma((2 * nx,)),
            dma((2,)),
            dma((4 * nx,)),
            dma((2 * half + 2,)),
            dma((10,)),
            dma,
            dma((nx,)),
            dma((3,)),
            dma((2 * nx,)),
            dma((2,)),
            dma((2,)),
            dma((2 * nx,)),
            dma,
            dma,
        ],
        compiler_params=pltpu.CompilerParams(collective_id=0, has_side_effects=True, vmem_limit_bytes=50 * 2**20),
    )(*[pltpu.with_memory_space_constraint(a, pltpu.HBM) for a in operands])
    return result.reshape(2, nz, 8, LANES)


def solution(mesh):
    nz, nx = mesh.shape["seq"], mesh.shape["ch"]
    in_specs = (
        P("grp", "seq", "col", "ch"),
        *(P("ch"), P("ch"), P(None, None, None, None, "ch"), P("ch")) * 3,
    )
    out_specs = P(("grp", "seq"), None, "col", "ch")
    return jax.shard_map(
        functools.partial(body, nz, nx),
        mesh=mesh,
        in_specs=in_specs,
        out_specs=out_specs,
        check_vma=False,
    )
```

```python
import functools

import jax
import jax.numpy as jnp
from jax import lax
from jax.experimental import pallas as pl
from jax.experimental.pallas import tpu as pltpu
from jax.sharding import PartitionSpec as P

MESH = pl.DeviceIdType.MESH
GROUP = 16
LANES = 128
EPS = 0.01
BF = jnp.bfloat16
F32 = jnp.float32


def lane_ids():
    return lax.broadcasted_iota(jnp.int32, (8, LANES), 1)


def row_ids():
    return lax.broadcasted_iota(jnp.int32, (8, LANES), 0)


def group_total(v):
    lane = lane_ids()
    step = GROUP // 2
    while step:
        from_below = pltpu.roll(v, step, 1)
        from_above = pltpu.roll(v, LANES - step, 1)
        v = v + jnp.where((lane & step) != 0, from_below, from_above)
        step //= 2
    return v


def packed_sums(values, x):
    total = jnp.sum(values, axis=0, keepdims=True)
    square = jnp.sum(values * values, axis=0, keepdims=True)
    total = group_total(jnp.broadcast_to(total, (8, LANES)))
    square = group_total(jnp.broadcast_to(square, (8, LANES)))
    slot = lane_ids() & 7
    row = jnp.where(slot == 2 * x, total, jnp.where(slot == 2 * x + 1, square, 0.0))
    return row[0:1]


def affine(row, samples, params, which, nx):
    spread_rows = jnp.broadcast_to(row, (8, LANES))
    picked = jnp.where((lane_ids() & (GROUP - 1)) == row_ids(), spread_rows, 0.0)
    sums = group_total(picked) * (1.0 / samples)
    out = []
    for block in range(nx):
        mean = sums[2 * block : 2 * block + 1]
        square = sums[2 * block + 1 : 2 * block + 2]
        inverse = 1.0 / jnp.sqrt(square - mean * mean + EPS)
        gain = params[block, 2 * which : 2 * which + 1]
        bias = params[block, 2 * which + 1 : 2 * which + 2]
        scale = inverse * gain
        out.append((scale, bias - mean * scale))
    return out


def activate(values, scale, shift):
    u = values * scale.reshape((1,) * (values.ndim - 1) + (LANES,)) + shift.reshape(
        (1,) * (values.ndim - 1) + (LANES,)
    )
    half = 0.5 * u
    return (half + half * jnp.tanh(half)).astype(BF)


def column_sum(y):
    n, cols = y.shape[0], y.shape[1]
    left, mid, right = (y[:, :, i * LANES : (i + 1) * LANES] for i in range(3))
    col = lax.broadcasted_iota(jnp.int32, (n, cols, LANES), 1)
    left = jnp.where(col == 0, 0.0, pltpu.roll(left, 1, 1))
    right = jnp.where(col == cols - 1, 0.0, pltpu.roll(right, cols - 1, 1))
    return left + mid + right


def taps(weight, dt, di, blocks):
    base = dt * 9 + di * 3
    rows = [pl.ds(pl.multiple_of(block * LANES, LANES), LANES) for block in blocks]
    return jnp.concatenate(
        [jnp.concatenate([weight[base + dj, r] for r in rows], axis=0) for dj in range(3)], axis=1
    )


def dot(a, b):
    return jnp.dot(a, b, preferred_element_type=F32)


def flat(v):
    return v.reshape(-1, v.shape[-1])


def kernel(
    nz,
    nx,
    lat_hbm,
    g0,
    b0,
    w0_hbm,
    c0,
    g1,
    b1,
    w1_hbm,
    c1,
    g2,
    b2,
    w2_hbm,
    c2,
    out,
    lat,
    vectors,
    w0,
    w1,
    w2,
    params,
    r0,
    x1,
    x2,
    act0,
    act1,
    act2,
    scales,
    summed,
    middle,
    hidden,
    give,
    take,
    plane_src,
    plane_in,
    line_src,
    line_in,
    hub_in,
    total_row,
    far_in,
    i_sem,
    w_sem,
    par_s,
    par_r,
    hub_s,
    hub_r,
    plane_s,
    plane_r,
    line_s,
    line_r,
    far_s,
    far_r,
    x0_s,
    x0_r,
    z0_s,
    z0_r,
    a_s,
    a_r,
    x1_s,
    x1_r,
    x2_s,
    x2_r,
    h2_r,
    e2_s,
    e2_r,
    o_s,
    o_r,
):
    z = lax.axis_index("seq")
    x = lax.axis_index("ch")
    c = lax.axis_index("col")
    half = nz // 2
    samples = float(nz * nz * 16 * GROUP)

    def peer(dz, dx, col):
        return {"seq": lax.rem(z + dz + nz, nz), "ch": lax.rem(x + dx, nx), "col": col}

    def remote(src, dst, s_sem, r_sem, to):
        return pltpu.make_async_remote_copy(
            src_ref=src,
            dst_ref=dst,
            send_sem=s_sem,
            recv_sem=r_sem,
            device_id=to,
            device_id_type=MESH,
        )

    def landed(ref, sem):
        pltpu.make_async_copy(ref, ref, sem).wait()

    inputs = [pltpu.make_async_copy(lat_hbm, lat, i_sem.at[9])]
    for i, ref in enumerate((g0, b0, g1, b1, g2, b2, c0, c1, c2)):
        inputs.append(pltpu.make_async_copy(ref, vectors.at[i], i_sem.at[i]))
    loads = [
        pltpu.make_async_copy(a, b, w_sem.at[i])
        for i, (a, b) in enumerate(((w0_hbm, w0), (w1_hbm, w1), (w2_hbm, w2)))
    ]
    for copy in inputs:
        copy.start()

    hub = 2
    barrier = pltpu.get_barrier_semaphore()

    def greet(dz, dx, col):
        pl.semaphore_signal(barrier, inc=1, device_id=peer(dz, dx, col), device_id_type=MESH)

    @pl.when(z < nz - 1)
    def _():
        greet(1, 0, c)

    @pl.when(z > 0)
    def _():
        greet(nz - 1, 0, c)

    for dx in range(nx):
        greet(0, dx, 1 - c)
        if dx:
            greet(0, dx, c)

    @pl.when(z == hub)
    def _():
        def greet_all(dz, carry):
            for dx in range(nx):
                greet(dz, dx, 1 - c)
                if dx:
                    greet(dz, dx, c)
            return carry

        lax.fori_loop(1, nz, greet_all, 0)

        def greet_line(dz, carry):
            greet(dz, 0, c)
            return carry

        lax.fori_loop(2, nz - 1, greet_line, 0)

    near = (z == hub + 1) | (z == hub - 1)
    awaited = 2 * nx + 1 + jnp.where(z == hub, 0, jnp.where(near, 2 * nx - 1, 2 * nx))
    awaited = awaited - jnp.where((z == 0) | (z == nz - 1), 1, 0)

    for copy in inputs:
        copy.wait()
    for load in loads:
        load.start()
    for i in range(6):
        params[x, i : i + 1, :] = vectors[i]
    own = lat[...].astype(F32)
    plane_src[0] = packed_sums(flat(own), x)
    own_at = ((nx + x) * 2 + c) * 6
    r0[pl.ds(own_at + 1 - c, 5)] = lat[pl.ds(3 * c, 5)]

    pl.semaphore_wait(barrier, awaited)

    def hub_start():
        place = (z * nx + x) * 2 + c

        @pl.when(z != hub)
        def _():
            for dx in (2, 1, 3, 0):
                for col in (c, 1 - c):
                    remote(
                        plane_src.at[0],
                        hub_in.at[place],
                        hub_s,
                        hub_r,
                        {"seq": hub, "ch": lax.rem(x + dx, nx), "col": col},
                    ).start()

        @pl.when(z == hub)
        def _():
            hub_in[place] = plane_src[0]
            for dx in (2, 1, 3, 0):
                for col in (c, 1 - c):
                    if dx == 0 and col is c:
                        continue
                    remote(
                        plane_src.at[0],
                        hub_in.at[place],
                        plane_s.at[0],
                        hub_r,
                        {"seq": hub, "ch": lax.rem(x + dx, nx), "col": col},
                    ).start()

    def hub_run():
        @pl.when(z == hub)
        def _():
            landed(hub_in.at[pl.ds(0, nz * nx * 2 - 1)], hub_r)
            total_row[0] = jnp.sum(hub_in[...], axis=0)

            def send(dz):
                remote(
                    total_row.at[0], total_row.at[0], line_s.at[0], line_r.at[0], peer(dz, 0, c)
                ).start()

            send(nz - 1)
            send(1)

            def far_first(k, carry):
                step = (k + 1) // 2
                send(half + step * (2 * lax.rem(k, 2) - 1))
                return carry

            lax.fori_loop(0, nz - 3, far_first, 0)

    def hub_total():
        @pl.when(z != hub)
        def _():
            landed(total_row.at[0], line_r.at[0])

        return total_row[0]

    def plane_start(stage):
        place = 8 * stage + 2 * x + c
        plane_in[place] = plane_src[stage]
        for dx in range(nx):
            for other in (0, 1):
                if dx == 0 and other == 0:
                    continue
                remote(
                    plane_src.at[stage],
                    plane_in.at[place],
                    plane_s.at[stage],
                    plane_r.at[stage],
                    peer(0, dx, c if other == 0 else 1 - c),
                ).start()

    across = (half, half - 1, half + 1)

    def far_start():
        for k, dz in enumerate(across):
            for dx in (2, 1, 3, 0):
                for col in (c, 1 - c):
                    remote(
                        plane_src.at[2],
                        far_in.at[8 * k + 2 * x + c],
                        far_s,
                        far_r,
                        peer(dz, dx, col),
                    ).start()

    def line_steps(stage):
        steps = sorted(range(1, nz), key=lambda dz: -min(dz, nz - dz))
        return [dz for dz in steps if stage == 1 or dz not in across]

    def line_start(stage):
        landed(plane_in.at[pl.ds(8 * stage, 2 * nx - 1)], plane_r.at[stage])
        row = jnp.sum(plane_in[8 * stage : 8 * stage + 2 * nx], axis=0)
        line_src[stage] = row
        line_in[stage * nz] = row
        for dz in line_steps(stage):
            remote(
                line_src.at[stage],
                line_in.at[stage * nz + nz - dz],
                line_s.at[stage],
                line_r.at[stage],
                peer(dz, 0, c),
            ).start()

    def line_total(stage):
        landed(line_in.at[pl.ds(stage * nz, len(line_steps(stage)))], line_r.at[stage])
        if stage == 1:
            return jnp.sum(line_in[nz : 2 * nz], axis=0)
        landed(far_in, far_r)
        total = jnp.sum(line_in[stage * nz : stage * nz + half - 1], axis=0)
        total = total + jnp.sum(line_in[stage * nz + half + 2 : (stage + 1) * nz], axis=0)
        return total + jnp.sum(far_in[...], axis=0)

    hub_start()
    for dx in range(1, nx):
        remote(params.at[x], params.at[x], par_s, par_r, peer(0, dx, c)).start()

    for dx in (2, 1, 3, 0):
        for other in (0, 1):
            if dx == 0 and other == 0:
                continue
            to_col = c if other == 0 else 1 - c
            remote(
                lat.at[pl.ds(3 * to_col, 5)],
                r0.at[pl.ds(own_at + 1 - to_col, 5)],
                x0_s,
                x0_r.at[x * 2 + c],
                peer(0, dx, to_col),
            ).start()

    @pl.when(c == 0)
    def _():
        for i in range(2 * nx):
            r0[nx * 12 + 6 * i] = jnp.zeros((16, LANES), BF)

    for row, outside in ((0, z == 0), (2, z == nz - 1)):
        @pl.when(outside)
        def _():
            r0[row * nx * 12 : (row + 1) * nx * 12] = jnp.zeros((nx * 12, 16, LANES), BF)

    @pl.when(z == 0)
    def _():
        for block in range(nx):
            x2[block * 40 : block * 40 + 20] = jnp.zeros((20, 16, LANES), BF)

    for block in range(nx):
        x1[pl.ds((block * 10 + 9 * c) * 2, 2)] = jnp.zeros((2, 16, LANES), BF)
    for block in range(2 * nx):
        x2[pl.ds((block * 10 + 9 * c) * 2, 2)] = jnp.zeros((2, 16, LANES), BF)

    for dx in (0, 1, 3, 2):
        for other in (0, 1):
            from_x = lax.rem(x + dx, nx)
            from_c = c if other == 0 else 1 - c
            at = (from_x * 2 + from_c) * 6
            if not (dx == 0 and other == 0):
                landed(r0.at[pl.ds(nx * 12 + at + 1 - c, 5)], x0_r.at[from_x * 2 + from_c])
            for row, dz, there in ((0, 1, z < nz - 1), (2, nz - 1, z > 0)):
                @pl.when(there)
                def _():
                    remote(
                        r0.at[pl.ds(nx * 12 + at, 5)],
                        r0.at[pl.ds(row * nx * 12 + at, 5)],
                        z0_s.at[row // 2],
                        z0_r.at[(row // 2) * 8 + from_x * 2 + from_c],
                        peer(dz, 0, c),
                    ).start()


    hub_run()
    landed(params.at[pl.ds(0, nx - 1)], par_r)
    norm = affine(hub_total(), samples, params, 0, nx)

    def frames_of(row, block):
        at = (row * nx + block) * 12
        parts = []
        for col in range(2):
            v = r0[pl.ds(at + 6 * col, 5)].astype(F32)
            parts.append(v.reshape(10, 8, LANES))
        return jnp.concatenate(parts, axis=1)

    for row, there in ((0, z > 0), (2, z < nz - 1)):
        @pl.when(there)
        def _():
            for block in range(nx):
                for col in range(2):
                    at = (row * nx + block) * 12 + 6 * col
                    landed(r0.at[pl.ds(at, 5)], z0_r.at[(row // 2) * 8 + block * 2 + col])

    loads[0].wait()

    def inside(condition):
        return jnp.where(condition, 1.0, 0.0).astype(F32)

    in_row = (inside(z > 0), 1.0, inside(z < nz - 1))
    in_core = (inside(c > 0), inside(c < 1))
    in_time = inside(z > 0)

    y = jnp.zeros((half * 16, 3 * LANES), F32)
    for pair in range(nx // 2):
        for k in range(2):
            scale, shift = norm[2 * pair + k]
            lanes = slice(k * LANES, (k + 1) * LANES)
            for row in range(3):
                v = frames_of(row, 2 * pair + k)
                keep = in_row[row] * in_core[0]
                act0[pair, row, 0:2, :, lanes] = activate(v[0:2], scale * keep, shift * keep)
                keep = in_row[row]
                act0[pair, row, 2:, :, lanes] = activate(v[2:], scale * keep, shift * keep)
        for di in range(3):
            for dt in range(3):
                y = y + dot(
                    flat(act0[pair, di, dt : dt + half]), taps(w0, dt, di, (2 * pair, 2 * pair + 1))
                )
    mixed = column_sum(y.reshape(half, 16, 3 * LANES))
    rest = frames_of(1, x)[2:10]
    value = (rest + mixed + vectors[6].reshape(1, 1, LANES)).astype(BF)
    plane_src[1] = packed_sums(flat(value.astype(F32)), x)
    plane_start(1)
    middle[...] = value

    low, high = lax.rem(z - half * c + nz, nz), lax.rem(z - half * c - half + nz, nz)
    low_near = jnp.minimum(low, nz - low) <= jnp.minimum(high, nz - high)

    boundary = (z == half - 1) | (z == half)

    def spread(act, case):
        to_c = z // half if case == 0 else 1 - z // half
        slot = z - half * to_c + 1
        for turn in range(half + 1):
            j = jnp.where(low_near, half - turn, turn)
            to_z = lax.rem(half * c + j, nz)
            source = jnp.maximum(j - 1, 0)
            tiles = 2 if 0 < turn < half else 1
            fr = 0 if 0 < turn < half else jnp.where(j == 0, 1, 0)
            at = (x * 10 + slot) * 2 + fr
            copy = remote(
                middle.at[pl.ds(source, tiles)],
                x1.at[pl.ds(at, tiles)],
                a_s.at[2 * turn + case],
                a_r.at[slot],
                {"seq": to_z, "ch": x, "col": to_c},
            )
            act(copy, source, tiles, at, (to_z == z) & (to_c == c))

    def a_start(copy, source, tiles, at, itself):
        @pl.when(jnp.logical_not(itself))
        def _():
            copy.start()

    def a_keep(copy, source, tiles, at, itself):
        @pl.when(itself)
        def _():
            x1[pl.ds(at, tiles)] = middle[pl.ds(source, tiles)]

    def a_sent(copy, source, tiles, at, itself):
        @pl.when(jnp.logical_not(itself))
        def _():
            copy.wait_send()

    spread(a_start, 0)

    @pl.when(boundary)
    def _():
        spread(a_start, 1)
        spread(a_keep, 1)

    @pl.when(z // half == c)
    def _():
        spread(a_keep, 0)

    first = 1 - c
    previous_c = lax.rem(z - 1 + nz, nz) // half
    whole_own = (previous_c == c) & (z // half == c)

    def row_over_ch(slot):
        tiles = pl.ds((x * 10 + slot) * 2, 2)
        for dx in (2, 1, 3):
            remote(
                x1.at[tiles], x1.at[tiles], x1_s, x1_r.at[x], peer(0, dx, c)
            ).start()

    @pl.when(whole_own)
    def _():
        row_over_ch(z - half * c + 1)

    line_start(1)

    for turn in range(9):
        slot = first + jnp.where(c == 0, turn, 8 - turn)
        mine = half * c - 1 + slot == z
        at = (x * 10 + slot) * 2
        lost_old = mine & (previous_c == c)
        lost_new = mine & (z // half == c)

        @pl.when(jnp.logical_not(lost_old | lost_new))
        def _():
            landed(x1.at[pl.ds(at, 2)], a_r.at[slot])

        @pl.when(lost_old ^ lost_new)
        def _():
            landed(x1.at[pl.ds(at, 1)], a_r.at[slot])

        @pl.when(jnp.logical_not(mine & whole_own))
        def _():
            row_over_ch(slot)

    norm = affine(line_total(1), samples, params, 1, nx)
    for block in range(nx):
        scales[2 * block] = norm[block][0]
        scales[2 * block + 1] = norm[block][1]
    loads[1].wait()
    bands = ((0, 1, in_core[0]), (1, half + 1, 1.0), (half + 1, half + 2, in_core[1]))

    shared = jnp.zeros((half * 16, 3 * LANES), F32)
    apart = jnp.zeros((2 * half * 16, 3 * LANES), F32)
    for pair, steps in enumerate(((0, 1), (3, 2))):
        blocks = [lax.rem(x + step, nx) for step in steps]
        for block, step in zip(blocks, steps):
            if step:
                landed(x1.at[pl.ds((block * 10 + first) * 2, 18)], x1_r.at[block])
        for k, block in enumerate(blocks):
            scale, shift = scales[2 * block], scales[2 * block + 1]
            v = x1[pl.ds(block * 20, 20)].astype(F32).reshape(half + 2, 2, 16, LANES)
            for fr in range(2):
                for lo, hi, keep in bands:
                    keep = keep * in_time if fr == 0 else keep
                    act1[pair, fr, lo:hi, :, k * LANES : (k + 1) * LANES] = activate(
                        v[lo:hi, fr], scale * keep, shift * keep
                    )
        for di in range(3):
            rows = act1[pair, :, di : di + half]
            shared = shared + dot(flat(rows[0]), taps(w1, 0, di, blocks))
            shared = shared + dot(flat(rows[1]), taps(w1, 2, di, blocks))
            apart = apart + dot(flat(rows), taps(w1, 1, di, blocks))
    y = apart.reshape(2, half, 16, 3 * LANES) + shared.reshape(1, half, 16, 3 * LANES)
    mixed = column_sum(y.reshape(2 * half, 16, 3 * LANES))
    value = (mixed + vectors[7].reshape(1, 1, LANES)).astype(BF)
    plane_src[2] = packed_sums(flat(value.astype(F32)), x)
    plane_start(2)
    far_start()
    value = value.reshape(2, half, 16, LANES)
    for fr in range(2):
        for row in range(half):
            hidden[row * 2 + fr] = value[fr, row]

    edge_at = pl.ds((2 * half - 2) * (1 - c), 2)
    edge_slot = pl.ds(18 * c, 2)
    def x2_block(block, own_frames):
        return pl.ds((block * 2 + own_frames) * 20 + 2, 2 * half)

    def history(part):
        return x2.at[pl.ds(x * 40 + 2 + part * half, half)]

    has_next, has_past = z < nz - 1, z > 0

    def edges(dz):
        for dx in (2, 1, 3, 0):
            slot = pl.ds((x * 2 + 1 - dz) * 20 + 18 * c, 2)
            remote(
                hidden.at[edge_at],
                x2.at[slot],
                e2_s.at[dz],
                e2_r.at[(1 - dz) * nx + x],
                peer(dz, dx, 1 - c),
            ).start()

    @pl.when(has_next)
    def _():
        for part in range(2):
            remote(
                hidden.at[pl.ds(part * half, half)],
                history(part),
                x2_s.at[1],
                h2_r.at[part],
                peer(1, 0, c),
            ).start()

    for dx in (2, 1, 3):
        remote(
            hidden, x2.at[x2_block(x, 1)], x2_s.at[0], x2_r.at[nx + x], peer(0, dx, c)
        ).start()
    edges(0)

    @pl.when(has_next)
    def _():
        edges(1)

    x2[pl.ds((x * 2 + 1) * 20 + 2, 2 * half)] = hidden[...]
    line_start(2)
    @pl.when(has_past)
    def _():
        for part in range(2):
            landed(history(part), h2_r.at[part])
            for dx in (2, 1, 3):
                remote(
                    history(part), history(part), x2_s.at[2], x2_r.at[x], peer(0, dx, c)
                ).start()

    norm = affine(line_total(2), 2.0 * samples, params, 2, nx)

    def arrived(own_frames):
        for block in range(nx):
            sem = own_frames * nx + block
            at = (block * 2 + own_frames) * 20

            @pl.when(block != x)
            def _():
                landed(x2.at[x2_block(block, own_frames)], x2_r.at[sem])

            landed(x2.at[pl.ds(at + 18 * (1 - c), 2)], e2_r.at[sem])

    arrived(1)

    @pl.when(has_past)
    def _():
        arrived(0)

    loads[2].wait()

    y = jnp.zeros((2 * half * 16, 3 * LANES), F32)
    for pair in range(nx // 2):
        for k in range(2):
            block = 2 * pair + k
            scale, shift = norm[block]
            for own_frames in range(2):
                at = (block * 2 + own_frames) * 20
                v = x2[at : at + 20].astype(F32).reshape(half + 2, 2, 16, LANES)
                for lo, hi, keep in bands:
                    keep = keep if own_frames else keep * in_time
                    part = activate(v[lo:hi], scale * keep, shift * keep)
                    for fr in range(2):
                        act2[pair, 2 * own_frames + fr, lo:hi, :, k * LANES : (k + 1) * LANES] = part[:, fr]
        for di in range(3):
            for dt in (1, 2):
                y = y + dot(
                    flat(act2[pair, dt : dt + 2, di : di + half]),
                    taps(w2, dt, di, (2 * pair, 2 * pair + 1)),
                )
    summed[...] = y

    @pl.when(has_past)
    def _():
        y = summed[...]
        for pair in range(nx // 2):
            for di in range(3):
                y = y + dot(
                    flat(act2[pair, 0:2, di : di + half]),
                    taps(w2, 0, di, (2 * pair, 2 * pair + 1)),
                )
        summed[...] = y

    y = summed[...]
    mixed = column_sum(y.reshape(2 * half, 16, 3 * LANES)).reshape(2, half, 16, LANES)
    doubled = x1[pl.ds(x * 20 + 2, 2 * half)].astype(F32).reshape(half, 2, 16, LANES)[:, 1]
    final = doubled[None] + mixed + vectors[8].reshape(1, 1, 1, LANES)

    sides = [
        final[:, :, 8 * side : 8 * side + 8].reshape(2, half // 2, 16, LANES).astype(BF)
        for side in range(2)
    ]

    @pl.when(c == 0)
    def _():
        give[...] = sides[1]
        out[:, pl.ds(0, half // 2)] = sides[0]

    @pl.when(c == 1)
    def _():
        give[...] = sides[0]
        out[:, pl.ds(half // 2, half // 2)] = sides[1]

    last = remote(give, take, o_s, o_r, peer(0, 0, 1 - c))
    last.start()

    @pl.when(z != hub)
    def _():
        landed(hub_in.at[pl.ds(0, 2 * nx)], hub_s)

    @pl.when(z == hub)
    def _():
        landed(hub_in.at[pl.ds(0, 2 * nx - 1)], plane_s.at[0])
        landed(hub_in.at[pl.ds(0, nz - 1)], line_s.at[0])

    for stage in (1, 2):
        landed(plane_in.at[pl.ds(8 * stage, 2 * nx - 1)], plane_s.at[stage])
        landed(line_in.at[pl.ds(stage * nz, len(line_steps(stage)))], line_s.at[stage])

    landed(far_in, far_s)
    landed(params.at[pl.ds(0, nx - 1)], par_s)
    landed(r0.at[pl.ds(0, 5 * (2 * nx - 1))], x0_s)
    for row, there in ((0, z < nz - 1), (1, z > 0)):
        @pl.when(there)
        def _():
            landed(r0.at[pl.ds(0, 5 * 2 * nx)], z0_s.at[row])

    spread(a_sent, 0)

    @pl.when(boundary)
    def _():
        spread(a_sent, 1)

    landed(x1.at[pl.ds(0, 3 * 3 * 6)], x1_s)
    landed(x2.at[pl.ds(0, 2 * half * (nx - 1))], x2_s.at[0])
    landed(x2.at[pl.ds(0, 2 * nx)], e2_s.at[0])

    @pl.when(has_next)
    def _():
        landed(x2.at[pl.ds(0, 2 * half)], x2_s.at[1])
        landed(x2.at[pl.ds(0, 2 * nx)], e2_s.at[1])

    @pl.when(has_past)
    def _():
        landed(x2.at[pl.ds(0, 2 * half * (nx - 1))], x2_s.at[2])

    last.wait()

    @pl.when(c == 0)
    def _():
        out[:, pl.ds(half // 2, half // 2)] = take[...]

    @pl.when(c == 1)
    def _():
        out[:, pl.ds(0, half // 2)] = take[...]


def body(nz, nx, *args):
    latent = args[0]
    frames = latent.shape[0]
    half = nz // 2
    channels = nx * LANES
    operands = [latent.reshape(frames // 2, 16, LANES)]
    for a in args[1:]:
        operands.append(a.reshape((1, LANES) if a.ndim == 1 else (27, channels, LANES)))
    weight = pltpu.VMEM((27, channels, LANES), BF)
    dma = pltpu.SemaphoreType.DMA
    result = pl.pallas_call(
        functools.partial(kernel, nz, nx),
        out_shape=jax.ShapeDtypeStruct((2, half, 16, LANES), BF),
        in_specs=[pl.BlockSpec(memory_space=pl.ANY)] * len(operands),
        out_specs=pl.BlockSpec(memory_space=pltpu.VMEM),
        scratch_shapes=[
            pltpu.VMEM((frames // 2, 16, LANES), BF),
            pltpu.VMEM((9, 1, LANES), F32),
            weight,
            weight,
            weight,
            pltpu.VMEM((nx, 8, LANES), F32),
            pltpu.VMEM((3 * nx * 2 * 6, 16, LANES), BF),
            pltpu.VMEM((nx * 10 * 2, 16, LANES), BF),
            pltpu.VMEM((nx * 2 * 10 * 2, 16, LANES), BF),
            pltpu.VMEM((nx // 2, 3, half + 2, 16, 2 * LANES), BF),
            pltpu.VMEM((nx // 2, 2, half + 2, 16, 2 * LANES), BF),
            pltpu.VMEM((nx // 2, 4, half + 2, 16, 2 * LANES), BF),
            pltpu.VMEM((2 * nx, 1, LANES), F32),
            pltpu.VMEM((2 * half * 16, 3 * LANES), F32),
            pltpu.VMEM((half, 16, LANES), BF),
            pltpu.VMEM((2 * half, 16, LANES), BF),
            pltpu.VMEM((2, half // 2, 16, LANES), BF),
            pltpu.VMEM((2, half // 2, 16, LANES), BF),
            pltpu.VMEM((3, 1, LANES), F32),
            pltpu.VMEM((3 * 8, 1, LANES), F32),
            pltpu.VMEM((3, 1, LANES), F32),
            pltpu.VMEM((3 * nz, 1, LANES), F32),
            pltpu.VMEM((nz * nx * 2, 1, LANES), F32),
            pltpu.VMEM((1, 1, LANES), F32),
            pltpu.VMEM((3 * 2 * nx, 1, LANES), F32),
            dma((10,)),
            dma((3,)),
            dma,
            dma,
            dma,
            dma,
            dma((3,)),
            dma((3,)),
            dma((3,)),
            dma((3,)),
            dma,
            dma,
            dma,
            dma((2 * nx,)),
            dma((2,)),
            dma((4 * nx,)),
            dma((2 * half + 2,)),
            dma((10,)),
            dma,
            dma((nx,)),
            dma((3,)),
            dma((2 * nx,)),
            dma((2,)),
            dma((2,)),
            dma((2 * nx,)),
            dma,
            dma,
        ],
        compiler_params=pltpu.CompilerParams(collective_id=0, has_side_effects=True, vmem_limit_bytes=50 * 2**20),
    )(*[pltpu.with_memory_space_constraint(a, pltpu.HBM) for a in operands])
    return result.reshape(2, nz, 8, LANES)


def solution(mesh):
    nz, nx = mesh.shape["seq"], mesh.shape["ch"]
    in_specs = (
        P("grp", "seq", "col", "ch"),
        *(P("ch"), P("ch"), P(None, None, None, None, "ch"), P("ch")) * 3,
    )
    out_specs = P(("grp", "seq"), None, "col", "ch")
    return jax.shard_map(
        functools.partial(body, nz, nx),
        mesh=mesh,
        in_specs=in_specs,
        out_specs=out_specs,
        check_vma=False,
    )
```
